8 devices in a mesh: col: 2 (over z, y), row: 2 (over x), depth: 2 (over core).
Axes of the slice: x: 2, y: 2, z: 1, core: 2. Of those that a mesh axis runs over, the one named last changes fastest.
Arguments:
- a_mat: bfloat16 [8192, 16384], P(('depth', 'row', 'col'))
- b_mat: bfloat16 [16384, 10240], P(('depth', 'row', 'col'))
Outputs:
- output: bfloat16 [8192, 10240], P(('depth', 'row', 'col'))
All inputs are finite; a program needn't handle non-finite values.
Results may differ from the reference program's by a relative error of at most 0.001.
Values are sent between devices in bfloat16 or wider.
A program may use at most 1 GiB of HBM per device.

```python
import jax
import jax.numpy as jnp

D = 8192
F = 10240
TOKENS = 16384


def setup_inputs(seed: int = 0) -> dict:
    key_a, key_b = jax.random.split(jax.random.key(seed))
    a_vals = jax.random.normal(key_a, (D, TOKENS), jnp.float32)
    b_vals = jax.random.normal(key_b, (TOKENS, F), jnp.float32) * (TOKENS ** -0.5)
    return {"a_mat": a_vals.astype(jnp.bfloat16), "b_mat": b_vals.astype(jnp.bfloat16)}


def reference(a_mat, b_mat):
    product = jnp.dot(a_mat, b_mat, preferred_element_type=jnp.float32)
    return product.astype(jnp.bfloat16)
```

```python
import functools

import jax
import jax.numpy as jnp
from jax import lax
from jax.experimental import pallas as pl
from jax.experimental.pallas import tpu as pltpu
from jax.sharding import PartitionSpec as P

MESH = pl.DeviceIdType.MESH
BLOCK = 512
TILES = 4
AHEAD = 4
SLOTS = 2


def kernel(
    n_blocks, tile, a_ref, b_ref, c_ref, b_got, r_got,
    a_buf, b_buf, p_buf, q_buf, r_buf, c_buf,
    a_own_sem, a_send, a_recv, b_send, b_recv, b_load_sem, p_send, r_recv, r_load_sem, c_sem,
):
    col, row, core = lax.axis_index("col"), lax.axis_index("row"), lax.axis_index("depth")
    neighbour, partner, sibling = {"col": 1 - col}, {"row": 1 - row}, {"depth": 1 - core}
    depth, block = b_ref.shape[0], b_buf.shape[2]

    def rows_of(m):
        return pl.ds(pl.multiple_of(m * tile, tile), tile)

    def cols_of(t):
        return pl.ds(pl.multiple_of(t * block, block), block)

    def a_cols(h, r):
        return pl.ds(pl.multiple_of((h * 4 + r * 2) * depth, depth), 2 * depth)

    def a_half(h):
        return pl.ds(h * 2 * depth, 2 * depth)

    def own_a(h):
        return pltpu.make_async_copy(a_ref.at[:, a_cols(h, row)], a_buf.at[0, :, a_half(h)], a_own_sem.at[h])

    def send_a(m, h):
        return pltpu.make_async_remote_copy(
            src_ref=a_ref.at[rows_of(m), a_cols(h, 1 - row)], dst_ref=a_buf.at[1, rows_of(m), a_half(h)],
            send_sem=a_send.at[m, h], recv_sem=a_recv.at[m, h], device_id=partner, device_id_type=MESH)

    def send_b(way, t):
        return pltpu.make_async_remote_copy(
            src_ref=b_got.at[0, t] if way == 2 else b_ref.at[:, cols_of(t)], dst_ref=b_got.at[way, t],
            send_sem=b_send.at[way, t], recv_sem=b_recv.at[way, t],
            device_id=neighbour if way == 0 else sibling, device_id_type=MESH)

    def load_b(t, slot):
        places = (core * 2 + col, core * 2 + 1 - col, (1 - core) * 2 + col, (1 - core) * 2 + 1 - col)
        return [
            pltpu.make_async_copy(
                b_ref.at[:, cols_of(t)] if i == 0 else b_got.at[i - 1, t],
                b_buf.at[slot, pl.ds(pl.multiple_of(place * depth, depth), depth), :], b_load_sem.at[slot, i])
            for i, place in enumerate(places)
        ]

    def send_p(s, m):
        return pltpu.make_async_remote_copy(
            src_ref=p_buf.at[lax.rem(s, SLOTS), rows_of(m)], dst_ref=r_got.at[s, rows_of(m)],
            send_sem=p_send.at[s, m], recv_sem=r_recv.at[s, m], device_id=partner, device_id_type=MESH)

    def load_r(q, m):
        return pltpu.make_async_copy(r_got.at[q, rows_of(m)], r_buf.at[m], r_load_sem.at[m])

    def store_c(q, m):
        return pltpu.make_async_copy(c_buf.at[m], c_ref.at[rows_of(m), cols_of(q)], c_sem.at[m])

    def product(whose, m, slot):
        return jnp.dot(a_buf[whose, rows_of(m), :], b_buf[slot], preferred_element_type=jnp.float32)

    def pass_on(t):
        send_b(0, t).wait_recv()
        send_b(2, t).start()
        send_b(1, t).start()

        @pl.when(t + AHEAD < n_blocks)
        def _():
            send_b(0, t + AHEAD).start()

    def start_load_first(t):
        send_b(1, t).wait_recv()
        send_b(2, t).wait_recv()
        for copy in load_b(t, 0):
            copy.start()

    barrier = pltpu.get_barrier_semaphore()
    for other in (neighbour, partner, sibling):
        pl.semaphore_signal(barrier, inc=1, device_id=other, device_id_type=MESH)
    pl.semaphore_wait(barrier, 3)

    for m in range(TILES):
        for h in range(2):
            send_a(m, h).start()
        if m == 0:
            for t in range(AHEAD):
                send_b(0, t).start()
    for h in range(2):
        own_a(h).start()

    @pl.loop(0, AHEAD)
    def _(t):
        pass_on(t)

    start_load_first(0)
    for h in range(2):
        own_a(h).wait()
    for copy in load_b(0, 0):
        copy.wait()

    @pl.loop(0, n_blocks + SLOTS)
    def _(s):
        @pl.when(s < n_blocks)
        def _():
            @pl.when(s > 0)
            def _():
                for copy in load_b(s, 0):
                    copy.wait()

            @pl.loop(0, TILES)
            def _(m):
                @pl.when(s == 0)
                def _():
                    for h in range(2):
                        send_a(m, h).wait_recv()

                @pl.when(s >= SLOTS)
                def _():
                    send_p(s - SLOTS, m).wait_send()

                p_buf[lax.rem(s, SLOTS), rows_of(m), :] = product(1, m, 0)
                send_p(s, m).start()

            @pl.when(s + AHEAD < n_blocks)
            def _():
                pass_on(s + AHEAD)

            @pl.when(s + 1 < n_blocks)
            def _():
                start_load_first(s + 1)

        @pl.when(s >= SLOTS)
        def _():
            q = s - SLOTS
            for copy in load_b(q, 1):
                copy.wait()

            @pl.loop(0, TILES)
            def _(m):
                q_buf[m] = product(0, m, 1)

            @pl.when(q + 1 < n_blocks)
            def _():
                for copy in load_b(q + 1, 1):
                    copy.start()

            @pl.loop(0, TILES)
            def _(m):
                send_p(q, m).wait_recv()
                load_r(q, m).start()
                load_r(q, m).wait()

                @pl.when(q > 0)
                def _():
                    store_c(q - 1, m).wait()

                c_buf[m] = (q_buf[m] + r_buf[m]).astype(c_buf.dtype)
                store_c(q, m).start()

        @pl.when(s == SLOTS - 1)
        def _():
            for copy in load_b(0, 1):
                copy.start()

    for m in range(TILES):
        store_c(n_blocks - 1, m).wait()
        for h in range(2):
            send_a(m, h).wait_send()

    @pl.loop(n_blocks - SLOTS, n_blocks)
    def _(s):
        for m in range(TILES):
            send_p(s, m).wait_send()

    @pl.loop(0, n_blocks)
    def _(t):
        for way in range(3):
            send_b(way, t).wait_send()


def device_product(block, a_rows, b_rows):
    rows, _ = a_rows.shape
    depth, n_cols = b_rows.shape
    n_blocks, tile = n_cols // block, rows // TILES
    anywhere = pl.BlockSpec(memory_space=pl.ANY)
    dma = pltpu.SemaphoreType.DMA
    c_rows, _, _ = pl.pallas_call(
        functools.partial(kernel, n_blocks, tile),
        out_shape=(
            jax.ShapeDtypeStruct((rows, n_cols), jnp.bfloat16),
            jax.ShapeDtypeStruct((3, n_blocks, depth, block), jnp.bfloat16),
            jax.ShapeDtypeStruct((n_blocks, rows, block), jnp.float32),
        ),
        in_specs=[anywhere] * 2,
        out_specs=(anywhere,) * 3,
        scratch_shapes=[
            pltpu.VMEM((2, rows, 4 * depth), jnp.bfloat16),
            pltpu.VMEM((2, 4 * depth, block), jnp.bfloat16),
            pltpu.VMEM((SLOTS, rows, block), jnp.float32),
            pltpu.VMEM((TILES, tile, block), jnp.float32),
            pltpu.VMEM((TILES, tile, block), jnp.float32),
            pltpu.VMEM((TILES, tile, block), jnp.bfloat16),
            dma((2,)),
            dma((TILES, 2)),
            dma((TILES, 2)),
            dma((3, n_blocks)),
            dma((3, n_blocks)),
            dma((2, 4)),
            dma((n_blocks, TILES)),
            dma((n_blocks, TILES)),
            dma((TILES,)),
            dma((TILES,)),
        ],
        compiler_params=pltpu.CompilerParams(
            collective_id=0, has_side_effects=True, vmem_limit_bytes=66_000_000
        ),
        name="split_sum_product",
    )(a_rows, b_rows)
    return c_rows


def solution(mesh, block=BLOCK):
    all_axes = ("depth", "row", "col")
    return jax.shard_map(
        functools.partial(device_product, block),
        mesh=mesh,
        in_specs=(P(all_axes, None), P(all_axes, None)),
        out_specs=P(all_axes, None),
        check_vma=False,
    )
```

```python
import functools

import jax
import jax.numpy as jnp
from jax import lax
from jax.experimental import pallas as pl
from jax.experimental.pallas import tpu as pltpu
from jax.sharding import PartitionSpec as P


MESH = pl.DeviceIdType.MESH
BLOCK = 512
TILES = 4
AHEAD = 4
SLOTS = 3
LATE = 128


def kernel(
    n_blocks, tile, a_ref, b_ref, c_ref, r_got, p_early, p_late, q_last, b_got,
    a_buf, b_buf, p_buf, q_buf, r_buf, c_buf,
    a_own_sem, a_send, a_recv, b_send, b_recv, b_load_sem, p_send, r_recv, r_load_sem, c_sem, q_sem, last_sem,
):
    last = n_blocks - 1
    col, row, core = lax.axis_index("col"), lax.axis_index("row"), lax.axis_index("depth")
    neighbour, partner, sibling = {"col": 1 - col}, {"row": 1 - row}, {"depth": 1 - core}
    depth, block = b_ref.shape[0], b_buf.shape[2]

    def rows_of(m):
        return pl.ds(pl.multiple_of(m * tile, tile), tile)

    def cols_of(t):
        return pl.ds(pl.multiple_of(t * block, block), block)

    def a_cols(h, r):
        return pl.ds(pl.multiple_of((h * 4 + r * 2) * depth, depth), 2 * depth)

    def a_half(h):
        return pl.ds(h * 2 * depth, 2 * depth)

    def own_a(h):
        return pltpu.make_async_copy(a_ref.at[:, a_cols(h, row)], a_buf.at[0, :, a_half(h)], a_own_sem.at[h])

    def send_a(m, h):
        return pltpu.make_async_remote_copy(
            src_ref=a_ref.at[rows_of(m), a_cols(h, 1 - row)], dst_ref=a_buf.at[1, rows_of(m), a_half(h)],
            send_sem=a_send.at[m, h], recv_sem=a_recv.at[m, h], device_id=partner, device_id_type=MESH)

    def send_b(way, t):
        return pltpu.make_async_remote_copy(
            src_ref=b_got.at[0, t] if way == 2 else b_ref.at[:, cols_of(t)], dst_ref=b_got.at[way, t],
            send_sem=b_send.at[way, t], recv_sem=b_recv.at[way, t],
            device_id=neighbour if way == 0 else sibling, device_id_type=MESH)

    def load_b(t, slot):
        places = (core * 2 + col, core * 2 + 1 - col, (1 - core) * 2 + col, (1 - core) * 2 + 1 - col)
        return [
            pltpu.make_async_copy(
                b_ref.at[:, cols_of(t)] if i == 0 else b_got.at[i - 1, t],
                b_buf.at[slot, pl.ds(pl.multiple_of(place * depth, depth), depth), :], b_load_sem.at[slot, i])
            for i, place in enumerate(places)
        ]

    def send_p(s, m):
        return pltpu.make_async_remote_copy(
            src_ref=p_buf.at[lax.rem(s, SLOTS), rows_of(m)], dst_ref=r_got.at[s, rows_of(m)],
            send_sem=p_send.at[s, m], recv_sem=r_recv.at[s, m], device_id=partner, device_id_type=MESH)

    def load_r(q, m):
        return pltpu.make_async_copy(r_got.at[q, rows_of(m)], r_buf.at[m], r_load_sem.at[m])

    def store_c(q, m):
        return pltpu.make_async_copy(c_buf.at[m], c_ref.at[rows_of(m), cols_of(q)], c_sem.at[m])

    def store_q(q, m):
        return pltpu.make_async_copy(q_buf.at[m], q_last.at[q - last + 1, rows_of(m)], q_sem.at[m])

    def store_p(m):
        early = p_early.shape[1]
        return [
            pltpu.make_async_copy(
                p_buf.at[last % SLOTS, rows_of(m), pl.ds(start, out.shape[1])], out.at[rows_of(m)], last_sem.at[i, m])
            for i, (start, out) in enumerate(((0, p_early), (early, p_late)))
        ]

    def product(whose, m, slot):
        return jnp.dot(a_buf[whose, rows_of(m), :], b_buf[slot], preferred_element_type=jnp.float32)

    def pass_on(t):
        send_b(0, t).wait_recv()
        send_b(2, t).start()
        send_b(1, t).start()

        @pl.when(t + AHEAD < n_blocks)
        def _():
            send_b(0, t + AHEAD).start()

    def start_load_first(t):
        send_b(1, t).wait_recv()
        send_b(2, t).wait_recv()
        for copy in load_b(t, 0):
            copy.start()

    barrier = pltpu.get_barrier_semaphore()
    for other in (neighbour, partner, sibling):
        pl.semaphore_signal(barrier, inc=1, device_id=other, device_id_type=MESH)
    pl.semaphore_wait(barrier, 3)

    for m in range(TILES):
        for h in range(2):
            send_a(m, h).start()
        if m == 0:
            for t in range(AHEAD):
                send_b(0, t).start()
    for h in range(2):
        own_a(h).start()

    @pl.loop(0, AHEAD)
    def _(t):
        pass_on(t)

    start_load_first(0)
    for h in range(2):
        own_a(h).wait()
    for copy in load_b(0, 0):
        copy.wait()

    @pl.loop(0, n_blocks + SLOTS)
    def _(s):
        @pl.when(s < n_blocks)
        def _():
            @pl.when(s > 0)
            def _():
                for copy in load_b(s, 0):
                    copy.wait()

            @pl.loop(0, TILES)
            def _(m):
                @pl.when(s == 0)
                def _():
                    for h in range(2):
                        send_a(m, h).wait_recv()

                @pl.when(s >= SLOTS)
                def _():
                    send_p(s - SLOTS, m).wait_send()

                p_buf[lax.rem(s, SLOTS), rows_of(m), :] = product(1, m, 0)

                @pl.when(s < last)
                def _():
                    send_p(s, m).start()

                @pl.when(s == last)
                def _():
                    for copy in store_p(m):
                        copy.start()

            @pl.when(s + AHEAD < n_blocks)
            def _():
                pass_on(s + AHEAD)

            @pl.when(s + 1 < n_blocks)
            def _():
                start_load_first(s + 1)

        @pl.when(s >= SLOTS)
        def _():
            q = s - SLOTS
            for copy in load_b(q, 1):
                copy.wait()

            @pl.loop(0, TILES)
            def _(m):
                @pl.when(q == last)
                def _():
                    store_q(q - 1, m).wait()

                q_buf[m] = product(0, m, 1)

                @pl.when(q >= last - 1)
                def _():
                    store_q(q, m).start()

            @pl.when(q + 1 < n_blocks)
            def _():
                for copy in load_b(q + 1, 1):
                    copy.start()

            @pl.when(q < last - 1)
            def _():
                @pl.loop(0, TILES)
                def _(m):
                    send_p(q, m).wait_recv()
                    load_r(q, m).start()
                    load_r(q, m).wait()

                    @pl.when(q > 0)
                    def _():
                        store_c(q - 1, m).wait()

                    c_buf[m] = (q_buf[m] + r_buf[m]).astype(c_buf.dtype)
                    store_c(q, m).start()

        @pl.when(s == SLOTS - 1)
        def _():
            for copy in load_b(0, 1):
                copy.start()

    @pl.loop(0, n_blocks)
    def _(t):
        for way in range(3):
            send_b(way, t).wait_send()

    for m in range(TILES):
        store_c(last - 2, m).wait()
        store_q(last, m).wait()
        for copy in store_p(m):
            copy.wait()
        for h in range(2):
            send_a(m, h).wait_send()

    @pl.loop(n_blocks - SLOTS, last)
    def _(s):
        for m in range(TILES):
            send_p(s, m).wait_send()

    for m in range(TILES):
        send_p(last - 1, m).wait_recv()


def write_out(n_done, c_ref, q_ref, r_ref, out_ref):
    @pl.when(pl.program_id(0) < n_done)
    def _():
        out_ref[...] = c_ref[...]

    @pl.when(pl.program_id(0) == n_done)
    def _():
        out_ref[...] = (q_ref[0] + r_ref[0]).astype(out_ref.dtype)


def device_product(block, a_rows, b_rows):
    rows, _ = a_rows.shape
    depth, n_cols = b_rows.shape
    n_blocks, tile, early = n_cols // block, rows // TILES, block - LATE
    last = n_blocks - 1
    anywhere = pl.BlockSpec(memory_space=pl.ANY)
    dma = pltpu.SemaphoreType.DMA
    c_main, r_got, p_early, p_late, q_last, _ = pl.pallas_call(
        functools.partial(kernel, n_blocks, tile),
        out_shape=(
            jax.ShapeDtypeStruct((rows, n_cols), jnp.bfloat16),
            jax.ShapeDtypeStruct((last, rows, block), jnp.float32),
            jax.ShapeDtypeStruct((rows, early), jnp.float32),
            jax.ShapeDtypeStruct((rows, LATE), jnp.float32),
            jax.ShapeDtypeStruct((2, rows, block), jnp.float32),
            jax.ShapeDtypeStruct((3, n_blocks, depth, block), jnp.bfloat16),
        ),
        in_specs=[anywhere] * 2,
        out_specs=(anywhere,) * 6,
        scratch_shapes=[
            pltpu.VMEM((2, rows, 4 * depth), jnp.bfloat16),
            pltpu.VMEM((2, 4 * depth, block), jnp.bfloat16),
            pltpu.VMEM((SLOTS, rows, block), jnp.float32),
            pltpu.VMEM((TILES, tile, block), jnp.float32),
            pltpu.VMEM((TILES, tile, block), jnp.float32),
            pltpu.VMEM((TILES, tile, block), jnp.bfloat16),
            dma((2,)),
            dma((TILES, 2)),
            dma((TILES, 2)),
            dma((3, n_blocks)),
            dma((3, n_blocks)),
            dma((2, 4)),
            dma((last, TILES)),
            dma((last, TILES)),
            dma((TILES,)),
            dma((TILES,)),
            dma((TILES,)),
            dma((2, TILES)),
        ],
        compiler_params=pltpu.CompilerParams(
            collective_id=0, has_side_effects=True, vmem_limit_bytes=66_000_000
        ),
        name="split_sum_product",
    )(a_rows, b_rows)

    swap = [(0, 1), (1, 0)]
    got_early = lax.ppermute(p_early, "row", swap)
    got_late = lax.ppermute(p_late, "row", swap)
    out = pl.pallas_call(
        functools.partial(write_out, last - 1),
        grid=(last,),
        out_shape=jax.ShapeDtypeStruct((rows, n_cols), jnp.bfloat16),
        in_specs=[
            pl.BlockSpec((rows, block), lambda i: (0, jnp.minimum(i, last - 2))),
            pl.BlockSpec((1, rows, block), lambda i: (0, 0, 0)),
            pl.BlockSpec((1, rows, block), lambda i: (last - 1, 0, 0)),
        ],
        out_specs=pl.BlockSpec((rows, block), lambda i: (0, i)),
        cost_estimate=pl.CostEstimate(flops=20_000_000_000, bytes_accessed=4 * rows * n_cols, transcendentals=0),
        name="write_out",
    )(c_main, q_last, r_got)
    for start, part in ((0, got_early), (early, got_late)):
        own = lax.slice(q_last, (1, 0, start), (2, rows, start + part.shape[1]))[0]
        out = lax.dynamic_update_slice(out, (own + part).astype(out.dtype), (0, last * block + start))
    return out


def solution(mesh, block=BLOCK):
    all_axes = ("depth", "row", "col")
    return jax.shard_map(
        functools.partial(device_product, block),
        mesh=mesh,
        in_specs=(P(all_axes, None), P(all_axes, None)),
        out_specs=P(all_axes, None),
        check_vma=False,
    )
```

```python
import functools

import jax
import jax.numpy as jnp
from jax import lax
from jax.experimental import pallas as pl
from jax.experimental.pallas import tpu as pltpu
from jax.sharding import PartitionSpec as P


MESH = pl.DeviceIdType.MESH
BLOCK = 512
TILES = 4
AHEAD = 4
SLOTS = 3
LATE = 128
RING = 2 * (SLOTS + 1)


def kernel(
    n_blocks, tile, a_ref, b_ref, c_ref, r_got, p_early, p_late, q_last, b_got,
    a_buf, b_buf, p_buf, q_buf, r_buf, c_buf,
    a_own_sem, a_send, a_recv, b_send, b_recv, b_load_sem, first_send, first_recv, p_send, r_recv, r_load_sem, c_sem, q_sem, last_sem,
):
    last = n_blocks - 1
    col, row, core = lax.axis_index("col"), lax.axis_index("row"), lax.axis_index("depth")
    neighbour, partner, sibling = {"col": 1 - col}, {"row": 1 - row}, {"depth": 1 - core}
    depth, block = b_ref.shape[0], b_buf.shape[2]

    def rows_of(m):
        return pl.ds(pl.multiple_of(m * tile, tile), tile)

    def cols_of(t):
        return pl.ds(pl.multiple_of(t * block, block), block)

    def a_cols(h, r):
        return pl.ds(pl.multiple_of((h * 4 + r * 2) * depth, depth), 2 * depth)

    def a_half(h):
        return pl.ds(h * 2 * depth, 2 * depth)

    def own_a(h):
        return pltpu.make_async_copy(a_ref.at[:, a_cols(h, row)], a_buf.at[0, :, a_half(h)], a_own_sem.at[h])

    def send_a(m, h):
        return pltpu.make_async_remote_copy(
            src_ref=a_ref.at[rows_of(m), a_cols(h, 1 - row)], dst_ref=a_buf.at[1, rows_of(m), a_half(h)],
            send_sem=a_send.at[m, h], recv_sem=a_recv.at[m, h], device_id=partner, device_id_type=MESH)

    def send_b(way, t):
        return pltpu.make_async_remote_copy(
            src_ref=b_got.at[0, t] if way == 2 else b_ref.at[:, cols_of(t)], dst_ref=b_got.at[way, t],
            send_sem=b_send.at[way, lax.rem(t, RING)], recv_sem=b_recv.at[way, lax.rem(t, RING)],
            device_id=neighbour if way == 0 else sibling, device_id_type=MESH)

    def load_b(t, slot):
        places = (core * 2 + col, core * 2 + 1 - col, (1 - core) * 2 + col, (1 - core) * 2 + 1 - col)
        return [
            pltpu.make_async_copy(
                b_ref.at[:, cols_of(t)] if i == 0 else b_got.at[i - 1, t],
                b_buf.at[slot, pl.ds(pl.multiple_of(place * depth, depth), depth), :], b_load_sem.at[slot, i])
            for i, place in enumerate(places)
        ]

    def send_first(m):
        return pltpu.make_async_remote_copy(
            src_ref=p_buf.at[0, rows_of(m)], dst_ref=r_got.at[0, rows_of(m)],
            send_sem=first_send.at[m], recv_sem=first_recv.at[m], device_id=partner, device_id_type=MESH)

    def send_block(s):
        return pltpu.make_async_remote_copy(
            src_ref=p_buf.at[lax.rem(s, SLOTS)], dst_ref=r_got.at[s],
            send_sem=p_send.at[lax.rem(s, SLOTS)], recv_sem=r_recv.at[lax.rem(s, RING)], device_id=partner, device_id_type=MESH)

    def load_r(q, m):
        return pltpu.make_async_copy(r_got.at[q, rows_of(m)], r_buf.at[m], r_load_sem.at[m])

    def store_c(q, m):
        return pltpu.make_async_copy(c_buf.at[m], c_ref.at[rows_of(m), cols_of(q)], c_sem.at[m])

    def store_q(q, m):
        return pltpu.make_async_copy(q_buf.at[m], q_last.at[q - last + 1, rows_of(m)], q_sem.at[m])

    def store_p(m):
        early = p_early.shape[1]
        return [
            pltpu.make_async_copy(
                p_buf.at[last % SLOTS, rows_of(m), pl.ds(start, out.shape[1])], out.at[rows_of(m)], last_sem.at[i, m])
            for i, (start, out) in enumerate(((0, p_early), (early, p_late)))
        ]

    def product(whose, m, slot):
        return jnp.dot(a_buf[whose, rows_of(m), :], b_buf[slot], preferred_element_type=jnp.float32)

    def pass_on(t):
        @pl.when(t >= RING - AHEAD)
        def _():
            send_b(0, t + AHEAD - RING).wait_send()

        @pl.when(t >= RING)
        def _():
            send_b(1, t - RING).wait_send()
            send_b(2, t - RING).wait_send()

        send_b(0, t).wait_recv()
        send_b(2, t).start()
        send_b(1, t).start()

        @pl.when(t + AHEAD < n_blocks)
        def _():
            send_b(0, t + AHEAD).start()

    def start_load_first(t):
        send_b(1, t).wait_recv()
        send_b(2, t).wait_recv()
        for copy in load_b(t, 0):
            copy.start()

    barrier = pltpu.get_barrier_semaphore()
    for other in (neighbour, partner, sibling):
        pl.semaphore_signal(barrier, inc=1, device_id=other, device_id_type=MESH)
    pl.semaphore_wait(barrier, 3)

    for m in range(TILES):
        for h in range(2):
            send_a(m, h).start()
        if m == 0:
            for t in range(AHEAD):
                send_b(0, t).start()
    for h in range(2):
        own_a(h).start()

    @pl.loop(0, AHEAD)
    def _(t):
        pass_on(t)

    start_load_first(0)
    for h in range(2):
        own_a(h).wait()
    for copy in load_b(0, 0):
        copy.wait()

    @pl.loop(0, n_blocks + SLOTS)
    def _(s):
        @pl.when(s < n_blocks)
        def _():
            @pl.when(s > 0)
            def _():
                for copy in load_b(s, 0):
                    copy.wait()

            @pl.when(s == SLOTS)
            def _():
                for m in range(TILES):
                    send_first(m).wait_send()

            @pl.when(s > SLOTS)
            def _():
                send_block(s - SLOTS).wait_send()

            @pl.loop(0, TILES)
            def _(m):
                @pl.when(s == 0)
                def _():
                    for h in range(2):
                        send_a(m, h).wait_recv()

                p_buf[lax.rem(s, SLOTS), rows_of(m), :] = product(1, m, 0)

                @pl.when(s == 0)
                def _():
                    send_first(m).start()

                @pl.when(s == last)
                def _():
                    for copy in store_p(m):
                        copy.start()

            @pl.when(jnp.logical_and(s > 0, s < last))
            def _():
                send_block(s).start()

            @pl.when(s + AHEAD < n_blocks)
            def _():
                pass_on(s + AHEAD)

            @pl.when(s + 1 < n_blocks)
            def _():
                start_load_first(s + 1)

        @pl.when(s >= SLOTS)
        def _():
            q = s - SLOTS

            @pl.when(q == 0)
            def _():
                for m in range(TILES):
                    send_first(m).wait_recv()

            @pl.when(jnp.logical_and(q > 0, q < last - 1))
            def _():
                send_block(q).wait_recv()

            @pl.when(q < last - 1)
            def _():
                for m in range(TILES):
                    load_r(q, m).start()

            for copy in load_b(q, 1):
                copy.wait()

            @pl.loop(0, TILES)
            def _(m):
                @pl.when(q == last)
                def _():
                    store_q(q - 1, m).wait()

                q_buf[m] = product(0, m, 1)

                @pl.when(q >= last - 1)
                def _():
                    store_q(q, m).start()

            @pl.when(q + 1 < n_blocks)
            def _():
                for copy in load_b(q + 1, 1):
                    copy.start()

            @pl.when(q < last - 1)
            def _():
                @pl.loop(0, TILES)
                def _(m):
                    load_r(q, m).wait()

                    @pl.when(q > 0)
                    def _():
                        store_c(q - 1, m).wait()

                    c_buf[m] = (q_buf[m] + r_buf[m]).astype(c_buf.dtype)
                    store_c(q, m).start()

        @pl.when(s == SLOTS - 1)
        def _():
            for copy in load_b(0, 1):
                copy.start()

    @pl.loop(n_blocks - RING, n_blocks)
    def _(t):
        send_b(1, t).wait_send()
        send_b(2, t).wait_send()

        @pl.when(t >= n_blocks - RING + AHEAD)
        def _():
            send_b(0, t).wait_send()

    for m in range(TILES):
        store_c(last - 2, m).wait()
        store_q(last, m).wait()
        for copy in store_p(m):
            copy.wait()
        for h in range(2):
            send_a(m, h).wait_send()

    @pl.loop(n_blocks - SLOTS, last)
    def _(s):
        send_block(s).wait_send()

    send_block(last - 1).wait_recv()


def write_out(n_done, c_ref, q_ref, r_ref, out_ref):
    @pl.when(pl.program_id(0) < n_done)
    def _():
        out_ref[...] = c_ref[...]

    @pl.when(pl.program_id(0) == n_done)
    def _():
        out_ref[...] = (q_ref[0] + r_ref[0]).astype(out_ref.dtype)


def device_product(block, a_rows, b_rows):
    rows, _ = a_rows.shape
    depth, n_cols = b_rows.shape
    n_blocks, tile, early = n_cols // block, rows // TILES, block - LATE
    last = n_blocks - 1
    anywhere = pl.BlockSpec(memory_space=pl.ANY)
    dma = pltpu.SemaphoreType.DMA
    c_main, r_got, p_early, p_late, q_last, _ = pl.pallas_call(
        functools.partial(kernel, n_blocks, tile),
        out_shape=(
            jax.ShapeDtypeStruct((rows, n_cols), jnp.bfloat16),
            jax.ShapeDtypeStruct((last, rows, block), jnp.float32),
            jax.ShapeDtypeStruct((rows, early), jnp.float32),
            jax.ShapeDtypeStruct((rows, LATE), jnp.float32),
            jax.ShapeDtypeStruct((2, rows, block), jnp.float32),
            jax.ShapeDtypeStruct((3, n_blocks, depth, block), jnp.bfloat16),
        ),
        in_specs=[anywhere] * 2,
        out_specs=(anywhere,) * 6,
        scratch_shapes=[
            pltpu.VMEM((2, rows, 4 * depth), jnp.bfloat16),
            pltpu.VMEM((2, 4 * depth, block), jnp.bfloat16),
            pltpu.VMEM((SLOTS, rows, block), jnp.float32),
            pltpu.VMEM((TILES, tile, block), jnp.float32),
            pltpu.VMEM((TILES, tile, block), jnp.float32),
            pltpu.VMEM((TILES, tile, block), jnp.bfloat16),
            dma((2,)),
            dma((TILES, 2)),
            dma((TILES, 2)),
            dma((3, RING)),
            dma((3, RING)),
            dma((2, 4)),
            dma((TILES,)),
            dma((TILES,)),
            dma((SLOTS,)),
            dma((RING,)),
            dma((TILES,)),
            dma((TILES,)),
            dma((TILES,)),
            dma((2, TILES)),
        ],
        compiler_params=pltpu.CompilerParams(
            collective_id=0, has_side_effects=True, vmem_limit_bytes=66_000_000
        ),
        name="split_sum_product",
    )(a_rows, b_rows)

    swap = [(0, 1), (1, 0)]
    got_early = lax.ppermute(p_early, "row", swap)
    got_late = lax.ppermute(p_late, "row", swap)
    out = pl.pallas_call(
        functools.partial(write_out, last - 1),
        grid=(last,),
        out_shape=jax.ShapeDtypeStruct((rows, n_cols), jnp.bfloat16),
        in_specs=[
            pl.BlockSpec((rows, block), lambda i: (0, jnp.minimum(i, last - 2))),
            pl.BlockSpec((1, rows, block), lambda i: (0, 0, 0)),
            pl.BlockSpec((1, rows, block), lambda i: (last - 1, 0, 0)),
        ],
        out_specs=pl.BlockSpec((rows, block), lambda i: (0, i)),
        cost_estimate=pl.CostEstimate(flops=20_000_000_000, bytes_accessed=4 * rows * n_cols, transcendentals=0),
        name="write_out",
    )(c_main, q_last, r_got)
    for start, part in ((0, got_early), (early, got_late)):
        own = lax.slice(q_last, (1, 0, start), (2, rows, start + part.shape[1]))[0]
        out = lax.dynamic_update_slice(out, (own + part).astype(out.dtype), (0, last * block + start))
    return out


def solution(mesh, block=BLOCK):
    all_axes = ("depth", "row", "col")
    return jax.shard_map(
        functools.partial(device_product, block),
        mesh=mesh,
        in_specs=(P(all_axes, None), P(all_axes, None)),
        out_specs=P(all_axes, None),
        check_vma=False,
    )
```

```python
import functools

import jax
import jax.numpy as jnp
from jax import lax
from jax.experimental import pallas as pl
from jax.experimental.pallas import tpu as pltpu
from jax.sharding import PartitionSpec as P


MESH = pl.DeviceIdType.MESH
BLOCK = 512
TILES = 4
AHEAD = 4
SLOTS = 3
LATE = 256
RING = 2 * (SLOTS + 1)


def kernel(
    n_blocks, tile, a_ref, b_ref, c_ref, r_got, p_early, p_late, q_early, q_late, q_done, b_got,
    a_buf, b_buf, p_buf, q_buf, r_buf, c_buf,
    a_own_sem, a_send, a_recv, b_send, b_recv, b_load_sem, first_send, first_recv, p_send, r_recv, r_load_sem, c_sem, q_sem, last_sem,
):
    last = n_blocks - 1
    col, row, core = lax.axis_index("col"), lax.axis_index("row"), lax.axis_index("depth")
    neighbour, partner, sibling = {"col": 1 - col}, {"row": 1 - row}, {"depth": 1 - core}
    depth, block = b_ref.shape[0], b_buf.shape[2]

    def rows_of(m):
        return pl.ds(pl.multiple_of(m * tile, tile), tile)

    def cols_of(t):
        return pl.ds(pl.multiple_of(t * block, block), block)

    def a_cols(h, r):
        return pl.ds(pl.multiple_of((h * 4 + r * 2) * depth, depth), 2 * depth)

    def a_half(h):
        return pl.ds(h * 2 * depth, 2 * depth)

    def own_a(h):
        return pltpu.make_async_copy(a_ref.at[:, a_cols(h, row)], a_buf.at[0, :, a_half(h)], a_own_sem.at[h])

    def send_a(m, h):
        return pltpu.make_async_remote_copy(
            src_ref=a_ref.at[rows_of(m), a_cols(h, 1 - row)], dst_ref=a_buf.at[1, rows_of(m), a_half(h)],
            send_sem=a_send.at[m, h], recv_sem=a_recv.at[m, h], device_id=partner, device_id_type=MESH)

    def send_b(way, t):
        return pltpu.make_async_remote_copy(
            src_ref=b_got.at[0, t] if way == 2 else b_ref.at[:, cols_of(t)], dst_ref=b_got.at[way, t],
            send_sem=b_send.at[way, lax.rem(t, RING)], recv_sem=b_recv.at[way, lax.rem(t, RING)],
            device_id=neighbour if way == 0 else sibling, device_id_type=MESH)

    def load_b(t, slot):
        places = (core * 2 + col, core * 2 + 1 - col, (1 - core) * 2 + col, (1 - core) * 2 + 1 - col)
        return [
            pltpu.make_async_copy(
                b_ref.at[:, cols_of(t)] if i == 0 else b_got.at[i - 1, t],
                b_buf.at[slot, pl.ds(pl.multiple_of(place * depth, depth), depth), :], b_load_sem.at[slot, i])
            for i, place in enumerate(places)
        ]

    def send_first(m):
        return pltpu.make_async_remote_copy(
            src_ref=p_buf.at[0, rows_of(m)], dst_ref=r_got.at[0, rows_of(m)],
            send_sem=first_send.at[m], recv_sem=first_recv.at[m], device_id=partner, device_id_type=MESH)

    def send_block(s):
        return pltpu.make_async_remote_copy(
            src_ref=p_buf.at[lax.rem(s, SLOTS)], dst_ref=r_got.at[s],
            send_sem=p_send.at[lax.rem(s, SLOTS)], recv_sem=r_recv.at[lax.rem(s, RING)], device_id=partner, device_id_type=MESH)

    def load_r(q):
        return pltpu.make_async_copy(r_got.at[q], r_buf, r_load_sem)

    def store_c(q):
        return pltpu.make_async_copy(c_buf, c_ref.at[:, cols_of(q)], c_sem)

    parts = (pl.ds(0, p_early.shape[1]), pl.ds(p_early.shape[1], p_late.shape[1]))

    def store_q_done():
        return pltpu.make_async_copy(q_buf, q_done, q_sem.at[0])

    def store_q():
        return [
            pltpu.make_async_copy(q_buf.at[:, part], out, q_sem.at[i])
            for i, (part, out) in enumerate(zip(parts, (q_early, q_late)))
        ]

    def store_p():
        return [
            pltpu.make_async_copy(p_buf.at[last % SLOTS, :, part], out, last_sem.at[i])
            for i, (part, out) in enumerate(zip(parts, (p_early, p_late)))
        ]

    def product(whose, m, slot):
        return jnp.dot(a_buf[whose, rows_of(m), :], b_buf[slot], preferred_element_type=jnp.float32)

    def pass_on(t):
        @pl.when(t >= RING - AHEAD)
        def _():
            send_b(0, t + AHEAD - RING).wait_send()

        @pl.when(t >= RING)
        def _():
            send_b(1, t - RING).wait_send()
            send_b(2, t - RING).wait_send()

        send_b(0, t).wait_recv()
        send_b(2, t).start()
        send_b(1, t).start()

        @pl.when(t + AHEAD < n_blocks)
        def _():
            send_b(0, t + AHEAD).start()

    def start_load_first(t):
        send_b(1, t).wait_recv()
        send_b(2, t).wait_recv()
        for copy in load_b(t, 0):
            copy.start()

    barrier = pltpu.get_barrier_semaphore()
    for other in (neighbour, partner, sibling):
        pl.semaphore_signal(barrier, inc=1, device_id=other, device_id_type=MESH)
    pl.semaphore_wait(barrier, 3)

    for m in range(TILES):
        for h in range(2):
            send_a(m, h).start()
        if m == 0:
            for t in range(AHEAD):
                send_b(0, t).start()
    for h in range(2):
        own_a(h).start()

    @pl.loop(0, AHEAD)
    def _(t):
        pass_on(t)

    start_load_first(0)
    for h in range(2):
        own_a(h).wait()
    for copy in load_b(0, 0):
        copy.wait()

    @pl.loop(0, n_blocks + SLOTS)
    def _(s):
        @pl.when(s < n_blocks)
        def _():
            @pl.when(s > 0)
            def _():
                for copy in load_b(s, 0):
                    copy.wait()

            @pl.when(s == SLOTS)
            def _():
                for m in range(TILES):
                    send_first(m).wait_send()

            @pl.when(s > SLOTS)
            def _():
                send_block(s - SLOTS).wait_send()

            @pl.loop(0, TILES)
            def _(m):
                @pl.when(s == 0)
                def _():
                    for h in range(2):
                        send_a(m, h).wait_recv()

                p_buf[lax.rem(s, SLOTS), rows_of(m), :] = product(1, m, 0)

                @pl.when(s == 0)
                def _():
                    send_first(m).start()

            @pl.when(s == last)
            def _():
                for copy in store_p():
                    copy.start()

            @pl.when(jnp.logical_and(s > 0, s < last))
            def _():
                send_block(s).start()

            @pl.when(s + AHEAD < n_blocks)
            def _():
                pass_on(s + AHEAD)

            @pl.when(s + 1 < n_blocks)
            def _():
                start_load_first(s + 1)

        @pl.when(s >= SLOTS)
        def _():
            q = s - SLOTS

            @pl.when(q == 0)
            def _():
                for m in range(TILES):
                    send_first(m).wait_recv()

            @pl.when(jnp.logical_and(q > 0, q < last - 1))
            def _():
                send_block(q).wait_recv()

            @pl.when(q < last - 1)
            def _():
                load_r(q).start()

            for copy in load_b(q, 1):
                copy.wait()

            @pl.when(q == last)
            def _():
                store_q_done().wait()

            @pl.loop(0, TILES)
            def _(m):
                q_buf[rows_of(m), :] = product(0, m, 1)

            @pl.when(q == last - 1)
            def _():
                store_q_done().start()

            @pl.when(q == last)
            def _():
                for copy in store_q():
                    copy.start()

            @pl.when(q + 1 < n_blocks)
            def _():
                for copy in load_b(q + 1, 1):
                    copy.start()

            @pl.when(q < last - 1)
            def _():
                load_r(q).wait()

                @pl.when(q > 0)
                def _():
                    store_c(q - 1).wait()

                @pl.loop(0, TILES)
                def _(m):
                    rows = rows_of(m)
                    c_buf[rows, :] = (q_buf[rows, :] + r_buf[rows, :]).astype(c_buf.dtype)

                store_c(q).start()

        @pl.when(s == SLOTS - 1)
        def _():
            for copy in load_b(0, 1):
                copy.start()

    @pl.loop(n_blocks - RING, n_blocks)
    def _(t):
        send_b(1, t).wait_send()
        send_b(2, t).wait_send()

        @pl.when(t >= n_blocks - RING + AHEAD)
        def _():
            send_b(0, t).wait_send()

    store_c(last - 2).wait()
    for copy in store_q() + store_p():
        copy.wait()
    for m in range(TILES):
        for h in range(2):
            send_a(m, h).wait_send()

    @pl.loop(n_blocks - SLOTS, last)
    def _(s):
        send_block(s).wait_send()

    send_block(last - 1).wait_recv()


def write_out(n_done, c_ref, q_ref, r_ref, out_ref):
    @pl.when(pl.program_id(0) < n_done)
    def _():
        out_ref[...] = c_ref[...]

    @pl.when(pl.program_id(0) == n_done)
    def _():
        out_ref[...] = (q_ref[...] + r_ref[0]).astype(out_ref.dtype)


def device_product(block, a_rows, b_rows):
    rows, _ = a_rows.shape
    depth, n_cols = b_rows.shape
    n_blocks, tile, early = n_cols // block, rows // TILES, block - LATE
    last = n_blocks - 1
    anywhere = pl.BlockSpec(memory_space=pl.ANY)
    dma = pltpu.SemaphoreType.DMA
    c_main, r_got, p_early, p_late, q_early, q_late, q_done, _ = pl.pallas_call(
        functools.partial(kernel, n_blocks, tile),
        out_shape=(
            jax.ShapeDtypeStruct((rows, n_cols), jnp.bfloat16),
            jax.ShapeDtypeStruct((last, rows, block), jnp.float32),
            jax.ShapeDtypeStruct((rows, early), jnp.float32),
            jax.ShapeDtypeStruct((rows, LATE), jnp.float32),
            jax.ShapeDtypeStruct((rows, early), jnp.float32),
            jax.ShapeDtypeStruct((rows, LATE), jnp.float32),
            jax.ShapeDtypeStruct((rows, block), jnp.float32),
            jax.ShapeDtypeStruct((3, n_blocks, depth, block), jnp.bfloat16),
        ),
        in_specs=[anywhere] * 2,
        out_specs=(anywhere,) * 8,
        scratch_shapes=[
            pltpu.VMEM((2, rows, 4 * depth), jnp.bfloat16),
            pltpu.VMEM((2, 4 * depth, block), jnp.bfloat16),
            pltpu.VMEM((SLOTS, rows, block), jnp.float32),
            pltpu.VMEM((rows, block), jnp.float32),
            pltpu.VMEM((rows, block), jnp.float32),
            pltpu.VMEM((rows, block), jnp.bfloat16),
            dma((2,)),
            dma((TILES, 2)),
            dma((TILES, 2)),
            dma((3, RING)),
            dma((3, RING)),
            dma((2, 4)),
            dma((TILES,)),
            dma((TILES,)),
            dma((SLOTS,)),
            dma((RING,)),
            dma,
            dma,
            dma((2,)),
            dma((2,)),
        ],
        compiler_params=pltpu.CompilerParams(
            collective_id=0, has_side_effects=True, vmem_limit_bytes=66_000_000
        ),
        name="split_sum_product",
    )(a_rows, b_rows)

    swap = [(0, 1), (1, 0)]
    got_early = lax.ppermute(p_early, "row", swap)
    got_late = lax.ppermute(p_late, "row", swap)
    out = pl.pallas_call(
        functools.partial(write_out, last - 1),
        grid=(last,),
        out_shape=jax.ShapeDtypeStruct((rows, n_cols), jnp.bfloat16),
        in_specs=[
            pl.BlockSpec((rows, block), lambda i: (0, jnp.minimum(i, last - 2))),
            pl.BlockSpec((rows, block), lambda i: (0, 0)),
            pl.BlockSpec((1, rows, block), lambda i: (last - 1, 0, 0)),
        ],
        out_specs=pl.BlockSpec((rows, block), lambda i: (0, i)),
        cost_estimate=pl.CostEstimate(flops=20_000_000_000, bytes_accessed=4 * rows * n_cols, transcendentals=0),
        name="write_out",
    )(c_main, q_done, r_got)
    for start, own, part in ((0, q_early, got_early), (early, q_late, got_late)):
        out = lax.dynamic_update_slice(out, (own + part).astype(out.dtype), (0, last * block + start))
    return out


def solution(mesh, block=BLOCK):
    all_axes = ("depth", "row", "col")
    return jax.shard_map(
        functools.partial(device_product, block),
        mesh=mesh,
        in_specs=(P(all_axes, None), P(all_axes, None)),
        out_specs=P(all_axes, None),
        check_vma=False,
    )
```

```python
import functools

import jax
import jax.numpy as jnp
from jax import lax
from jax.experimental import pallas as pl
from jax.experimental.pallas import tpu as pltpu
from jax.sharding import PartitionSpec as P


MESH = pl.DeviceIdType.MESH
BLOCK = 512
TILES = 4
AHEAD = 4
SLOTS = 3
LATE = 256
RING = 2 * (SLOTS + 1)


def kernel(
    n_blocks, tile, a_ref, b_ref, c_ref, r_got, p_early, p_late, q_early, q_late, q_done, b_got,
    a_buf, b_buf, p_buf, q_buf, r_buf, c_buf,
    a_own_sem, a_send, a_recv, b_send, b_recv, b_load_sem, first_send, first_recv, p_send, r_recv, r_load_sem, c_sem, q_sem, last_sem,
):
    last = n_blocks - 1
    col, row, core = lax.axis_index("col"), lax.axis_index("row"), lax.axis_index("depth")
    neighbour, partner, sibling = {"col": 1 - col}, {"row": 1 - row}, {"depth": 1 - core}
    depth, block = b_ref.shape[0], b_buf.shape[2]

    def rows_of(m):
        return pl.ds(pl.multiple_of(m * tile, tile), tile)

    def cols_of(t):
        return pl.ds(pl.multiple_of(t * block, block), block)

    def a_cols(h, r):
        return pl.ds(pl.multiple_of((h * 4 + r * 2) * depth, depth), 2 * depth)

    def a_half(h):
        return pl.ds(h * 2 * depth, 2 * depth)

    def own_a(h):
        return pltpu.make_async_copy(a_ref.at[:, a_cols(h, row)], a_buf.at[0, :, a_half(h)], a_own_sem.at[h])

    def send_a(m, h):
        return pltpu.make_async_remote_copy(
            src_ref=a_ref.at[rows_of(m), a_cols(h, 1 - row)], dst_ref=a_buf.at[1, rows_of(m), a_half(h)],
            send_sem=a_send.at[m, h], recv_sem=a_recv.at[m, h], device_id=partner, device_id_type=MESH)

    def send_b(way, t):
        return pltpu.make_async_remote_copy(
            src_ref=b_got.at[0, t] if way == 2 else b_ref.at[:, cols_of(t)], dst_ref=b_got.at[way, t],
            send_sem=b_send.at[way, lax.rem(t, RING)], recv_sem=b_recv.at[way, lax.rem(t, RING)],
            device_id=neighbour if way == 0 else sibling, device_id_type=MESH)

    def load_b(t, slot):
        places = (core * 2 + col, core * 2 + 1 - col, (1 - core) * 2 + col, (1 - core) * 2 + 1 - col)
        return [
            pltpu.make_async_copy(
                b_ref.at[:, cols_of(t)] if i == 0 else b_got.at[i - 1, t],
                b_buf.at[slot, pl.ds(pl.multiple_of(place * depth, depth), depth), :], b_load_sem.at[slot, i])
            for i, place in enumerate(places)
        ]

    def send_first(m):
        return pltpu.make_async_remote_copy(
            src_ref=p_buf.at[0, rows_of(m)], dst_ref=r_got.at[0, rows_of(m)],
            send_sem=first_send.at[m], recv_sem=first_recv.at[m], device_id=partner, device_id_type=MESH)

    def send_block(s):
        return pltpu.make_async_remote_copy(
            src_ref=p_buf.at[lax.rem(s, SLOTS)], dst_ref=r_got.at[s],
            send_sem=p_send.at[lax.rem(s, SLOTS)], recv_sem=r_recv.at[lax.rem(s, RING)], device_id=partner, device_id_type=MESH)

    def load_r(q):
        return pltpu.make_async_copy(r_got.at[q], r_buf, r_load_sem)

    def store_c(q):
        return pltpu.make_async_copy(c_buf, c_ref.at[:, cols_of(q)], c_sem)

    parts = (pl.ds(0, p_early.shape[1]), pl.ds(p_early.shape[1], p_late.shape[1]))

    def store_q_done():
        return pltpu.make_async_copy(q_buf, q_done, q_sem.at[0])

    def store_q():
        return [
            pltpu.make_async_copy(q_buf.at[:, part], out, q_sem.at[i])
            for i, (part, out) in enumerate(zip(parts, (q_early, q_late)))
        ]

    def store_p():
        return [
            pltpu.make_async_copy(p_buf.at[last % SLOTS, :, part], out, last_sem.at[i])
            for i, (part, out) in enumerate(zip(parts, (p_early, p_late)))
        ]

    def product(whose, m, slot):
        return jnp.dot(a_buf[whose, rows_of(m), :], b_buf[slot], preferred_element_type=jnp.float32)

    def pass_on(t):
        @pl.when(t >= RING - AHEAD)
        def _():
            send_b(0, t + AHEAD - RING).wait_send()

        @pl.when(t >= RING)
        def _():
            send_b(1, t - RING).wait_send()
            send_b(2, t - RING).wait_send()

        send_b(0, t).wait_recv()
        send_b(2, t).start()
        send_b(1, t).start()

        @pl.when(t + AHEAD < n_blocks)
        def _():
            send_b(0, t + AHEAD).start()

    def start_load_first(t):
        send_b(1, t).wait_recv()
        send_b(2, t).wait_recv()
        for copy in load_b(t, 0):
            copy.start()

    barrier = pltpu.get_barrier_semaphore()
    for other in (neighbour, partner, sibling):
        pl.semaphore_signal(barrier, inc=1, device_id=other, device_id_type=MESH)
    pl.semaphore_wait(barrier, 3)

    def start_a(tiles):
        for m in tiles:
            for h in range(2):
                send_a(m, h).start()

    early, late = range(2), range(2, TILES)
    start_a(early)
    for t in range(AHEAD):
        send_b(0, t).start()

    @pl.when(core == 0)
    def _():
        start_a(late)

    @pl.loop(0, AHEAD)
    def _(t):
        pass_on(t)

    @pl.when(core == 1)
    def _():
        for m in early:
            for h in range(2):
                send_a(m, h).wait_send()

    for h in range(2):
        own_a(h).start()
    for h in range(2):
        own_a(h).wait()

    @pl.when(core == 1)
    def _():
        start_a(late)

    start_load_first(0)
    for copy in load_b(0, 0):
        copy.wait()

    @pl.loop(0, n_blocks + SLOTS)
    def _(s):
        @pl.when(s < n_blocks)
        def _():
            @pl.when(s > 0)
            def _():
                for copy in load_b(s, 0):
                    copy.wait()

            @pl.when(s == SLOTS)
            def _():
                for m in range(TILES):
                    send_first(m).wait_send()

            @pl.when(s > SLOTS)
            def _():
                send_block(s - SLOTS).wait_send()

            @pl.loop(0, TILES)
            def _(m):
                @pl.when(s == 0)
                def _():
                    for h in range(2):
                        send_a(m, h).wait_recv()

                p_buf[lax.rem(s, SLOTS), rows_of(m), :] = product(1, m, 0)

                @pl.when(s == 0)
                def _():
                    send_first(m).start()

            @pl.when(s == last)
            def _():
                for copy in store_p():
                    copy.start()

            @pl.when(jnp.logical_and(s > 0, s < last))
            def _():
                send_block(s).start()

            @pl.when(s + AHEAD < n_blocks)
            def _():
                pass_on(s + AHEAD)

            @pl.when(s + 1 < n_blocks)
            def _():
                start_load_first(s + 1)

        @pl.when(s >= SLOTS)
        def _():
            q = s - SLOTS

            @pl.when(q == 0)
            def _():
                for m in range(TILES):
                    send_first(m).wait_recv()

            @pl.when(jnp.logical_and(q > 0, q < last - 1))
            def _():
                send_block(q).wait_recv()

            @pl.when(q < last - 1)
            def _():
                load_r(q).start()

            for copy in load_b(q, 1):
                copy.wait()

            @pl.when(q == last)
            def _():
                store_q_done().wait()

            @pl.loop(0, TILES)
            def _(m):
                q_buf[rows_of(m), :] = product(0, m, 1)

            @pl.when(q == last - 1)
            def _():
                store_q_done().start()

            @pl.when(q == last)
            def _():
                for copy in store_q():
                    copy.start()

            @pl.when(q + 1 < n_blocks)
            def _():
                for copy in load_b(q + 1, 1):
                    copy.start()

            @pl.when(q < last - 1)
            def _():
                load_r(q).wait()

                @pl.when(q > 0)
                def _():
                    store_c(q - 1).wait()

                @pl.loop(0, TILES)
                def _(m):
                    rows = rows_of(m)
                    c_buf[rows, :] = (q_buf[rows, :] + r_buf[rows, :]).astype(c_buf.dtype)

                store_c(q).start()

        @pl.when(s == SLOTS - 1)
        def _():
            for copy in load_b(0, 1):
                copy.start()

    @pl.loop(n_blocks - RING, n_blocks)
    def _(t):
        send_b(1, t).wait_send()
        send_b(2, t).wait_send()

        @pl.when(t >= n_blocks - RING + AHEAD)
        def _():
            send_b(0, t).wait_send()

    store_c(last - 2).wait()
    for copy in store_q() + store_p():
        copy.wait()
    for h in range(2):
        @pl.when(core == 0)
        def _():
            for m in early:
                send_a(m, h).wait_send()

        for m in late:
            send_a(m, h).wait_send()

    @pl.loop(n_blocks - SLOTS, last)
    def _(s):
        send_block(s).wait_send()

    send_block(last - 1).wait_recv()


def write_out(n_done, c_ref, q_ref, r_ref, out_ref):
    @pl.when(pl.program_id(0) < n_done)
    def _():
        out_ref[...] = c_ref[...]

    @pl.when(pl.program_id(0) == n_done)
    def _():
        out_ref[...] = (q_ref[...] + r_ref[0]).astype(out_ref.dtype)


def device_product(block, a_rows, b_rows):
    rows, _ = a_rows.shape
    depth, n_cols = b_rows.shape
    n_blocks, tile, early = n_cols // block, rows // TILES, block - LATE
    last = n_blocks - 1
    anywhere = pl.BlockSpec(memory_space=pl.ANY)
    dma = pltpu.SemaphoreType.DMA
    c_main, r_got, p_early, p_late, q_early, q_late, q_done, _ = pl.pallas_call(
        functools.partial(kernel, n_blocks, tile),
        out_shape=(
            jax.ShapeDtypeStruct((rows, n_cols), jnp.bfloat16),
            jax.ShapeDtypeStruct((last, rows, block), jnp.float32),
            jax.ShapeDtypeStruct((rows, early), jnp.float32),
            jax.ShapeDtypeStruct((rows, LATE), jnp.float32),
            jax.ShapeDtypeStruct((rows, early), jnp.float32),
            jax.ShapeDtypeStruct((rows, LATE), jnp.float32),
            jax.ShapeDtypeStruct((rows, block), jnp.float32),
            jax.ShapeDtypeStruct((3, n_blocks, depth, block), jnp.bfloat16),
        ),
        in_specs=[anywhere] * 2,
        out_specs=(anywhere,) * 8,
        scratch_shapes=[
            pltpu.VMEM((2, rows, 4 * depth), jnp.bfloat16),
            pltpu.VMEM((2, 4 * depth, block), jnp.bfloat16),
            pltpu.VMEM((SLOTS, rows, block), jnp.float32),
            pltpu.VMEM((rows, block), jnp.float32),
            pltpu.VMEM((rows, block), jnp.float32),
            pltpu.VMEM((rows, block), jnp.bfloat16),
            dma((2,)),
            dma((TILES, 2)),
            dma((TILES, 2)),
            dma((3, RING)),
            dma((3, RING)),
            dma((2, 4)),
            dma((TILES,)),
            dma((TILES,)),
            dma((SLOTS,)),
            dma((RING,)),
            dma,
            dma,
            dma((2,)),
            dma((2,)),
        ],
        compiler_params=pltpu.CompilerParams(
            collective_id=0, has_side_effects=True, vmem_limit_bytes=66_000_000
        ),
        name="split_sum_product",
    )(a_rows, b_rows)

    swap = [(0, 1), (1, 0)]
    got_early = lax.ppermute(p_early, "row", swap)
    got_late = lax.ppermute(p_late, "row", swap)
    out = pl.pallas_call(
        functools.partial(write_out, last - 1),
        grid=(last,),
        out_shape=jax.ShapeDtypeStruct((rows, n_cols), jnp.bfloat16),
        in_specs=[
            pl.BlockSpec((rows, block), lambda i: (0, jnp.minimum(i, last - 2))),
            pl.BlockSpec((rows, block), lambda i: (0, 0)),
            pl.BlockSpec((1, rows, block), lambda i: (last - 1, 0, 0)),
        ],
        out_specs=pl.BlockSpec((rows, block), lambda i: (0, i)),
        cost_estimate=pl.CostEstimate(flops=20_000_000_000, bytes_accessed=4 * rows * n_cols, transcendentals=0),
        name="write_out",
    )(c_main, q_done, r_got)
    for start, own, part in ((0, q_early, got_early), (early, q_late, got_late)):
        out = lax.dynamic_update_slice(out, (own + part).astype(out.dtype), (0, last * block + start))
    return out


def solution(mesh, block=BLOCK):
    all_axes = ("depth", "row", "col")
    return jax.shard_map(
        functools.partial(device_product, block),
        mesh=mesh,
        in_specs=(P(all_axes, None), P(all_axes, None)),
        out_specs=P(all_axes, None),
        check_vma=False,
    )
```

```python
import functools

import jax
import jax.numpy as jnp
from jax import lax
from jax.experimental import pallas as pl
from jax.experimental.pallas import tpu as pltpu
from jax.sharding import PartitionSpec as P


MESH = pl.DeviceIdType.MESH
BLOCK = 512
TILES = 4
AHEAD = 4
SLOTS = 3
LATE = 128
PIECES = 2
RING = 2 * (SLOTS + 1)


def kernel(
    n_blocks, tile, a_ref, b_ref, c_ref, r_got, p_early, p_late, q_early, q_late, q_done, b_got,
    a_buf, b_buf, p_buf, q_buf, r_buf, c_buf,
    a_own_sem, a_send, a_recv, b_send, b_recv, b_load_sem, first_send, first_recv, p_send, r_recv, r_load_sem, c_sem, q_sem, last_sem, here_sem,
):
    last = n_blocks - 1
    col, row, core = lax.axis_index("col"), lax.axis_index("row"), lax.axis_index("depth")
    neighbour, partner, sibling = {"col": 1 - col}, {"row": 1 - row}, {"depth": 1 - core}
    depth, block = b_ref.shape[0], b_buf.shape[2]

    def rows_of(m):
        return pl.ds(pl.multiple_of(m * tile, tile), tile)

    def cols_of(t):
        return pl.ds(pl.multiple_of(t * block, block), block)

    def a_cols(h, r):
        return pl.ds(pl.multiple_of((h * 4 + r * 2) * depth, depth), 2 * depth)

    def a_half(h):
        return pl.ds(h * 2 * depth, 2 * depth)

    def own_a(h):
        return pltpu.make_async_copy(a_ref.at[:, a_cols(h, row)], a_buf.at[0, :, a_half(h)], a_own_sem.at[h])

    def send_a(m, h):
        return pltpu.make_async_remote_copy(
            src_ref=a_ref.at[rows_of(m), a_cols(h, 1 - row)], dst_ref=a_buf.at[1, rows_of(m), a_half(h)],
            send_sem=a_send.at[m, h], recv_sem=a_recv.at[m, h], device_id=partner, device_id_type=MESH)

    def send_b(way, t):
        return pltpu.make_async_remote_copy(
            src_ref=b_got.at[0, t] if way == 2 else b_ref.at[:, cols_of(t)], dst_ref=b_got.at[way, t],
            send_sem=b_send.at[way, lax.rem(t, RING)], recv_sem=b_recv.at[way, lax.rem(t, RING)],
            device_id=neighbour if way == 0 else sibling, device_id_type=MESH)

    def load_b(t, slot):
        places = (core * 2 + col, core * 2 + 1 - col, (1 - core) * 2 + col, (1 - core) * 2 + 1 - col)
        return [
            pltpu.make_async_copy(
                b_ref.at[:, cols_of(t)] if i == 0 else b_got.at[i - 1, t],
                b_buf.at[slot, pl.ds(pl.multiple_of(place * depth, depth), depth), :], b_load_sem.at[slot, i])
            for i, place in enumerate(places)
        ]

    def send_first(m):
        return pltpu.make_async_remote_copy(
            src_ref=p_buf.at[0, rows_of(m)], dst_ref=r_got.at[0, rows_of(m)],
            send_sem=first_send.at[m], recv_sem=first_recv.at[m], device_id=partner, device_id_type=MESH)

    def send_block(s):
        return pltpu.make_async_remote_copy(
            src_ref=p_buf.at[lax.rem(s, SLOTS)], dst_ref=r_got.at[s],
            send_sem=p_send.at[lax.rem(s, SLOTS)], recv_sem=r_recv.at[lax.rem(s, RING)], device_id=partner, device_id_type=MESH)

    def load_r(q):
        return pltpu.make_async_copy(r_got.at[q], r_buf, r_load_sem)

    def store_c(q):
        return pltpu.make_async_copy(c_buf, c_ref.at[:, cols_of(q)], c_sem)

    parts = (pl.ds(0, p_early.shape[0]), pl.ds(p_early.shape[0], p_late.shape[0]))

    def store_q_done():
        return pltpu.make_async_copy(q_buf, q_done, q_sem.at[0])

    def store_q():
        return [
            pltpu.make_async_copy(q_buf.at[part], out, q_sem.at[i])
            for i, (part, out) in enumerate(zip(parts, (q_early, q_late)))
        ]

    def store_p():
        return [
            pltpu.make_async_copy(p_buf.at[last % SLOTS, part], out, last_sem.at[i])
            for i, (part, out) in enumerate(zip(parts, (p_early, p_late)))
        ]

    def product(whose, m, slot):
        return jnp.dot(a_buf[whose, rows_of(m), :], b_buf[slot], preferred_element_type=jnp.float32)

    def pass_on(t):
        @pl.when(t >= RING - AHEAD)
        def _():
            send_b(0, t + AHEAD - RING).wait_send()

        @pl.when(t >= RING)
        def _():
            send_b(1, t - RING).wait_send()
            send_b(2, t - RING).wait_send()

        send_b(0, t).wait_recv()
        send_b(2, t).start()
        send_b(1, t).start()

        @pl.when(t + AHEAD < n_blocks)
        def _():
            send_b(0, t + AHEAD).start()

    def start_load_first(t):
        send_b(1, t).wait_recv()
        send_b(2, t).wait_recv()
        for copy in load_b(t, 0):
            copy.start()

    barrier = pltpu.get_barrier_semaphore()
    root = jnp.logical_and(col == 0, core == 0)
    pl.semaphore_signal(barrier, inc=1, device_id=partner, device_id_type=MESH)

    @pl.when(jnp.logical_or(root, col == 1))
    def _():
        pl.semaphore_signal(barrier, inc=1, device_id=sibling, device_id_type=MESH)

    @pl.when(jnp.logical_or(root, core == 1))
    def _():
        pl.semaphore_signal(barrier, inc=1, device_id=neighbour, device_id_type=MESH)

    @pl.when(root)
    def _():
        pl.semaphore_wait(barrier, 1)

    @pl.when(jnp.logical_not(root))
    def _():
        pl.semaphore_wait(barrier, 3)

    @pl.when(jnp.logical_and(col == 0, core == 1))
    def _():
        pl.semaphore_signal(here_sem, inc=1, device_id=sibling, device_id_type=MESH)

    @pl.when(jnp.logical_and(col == 1, core == 0))
    def _():
        pl.semaphore_signal(here_sem, inc=1, device_id=neighbour, device_id_type=MESH)

    def start_a(tiles):
        for m in tiles:
            for h in range(2):
                send_a(m, h).start()

    early, late = range(2), range(2, TILES)
    start_a(early)

    @pl.when(root)
    def _():
        pl.semaphore_wait(here_sem, 2)

    for t in range(AHEAD):
        send_b(0, t).start()

    @pl.when(core == 0)
    def _():
        start_a(late)

    @pl.when(core == 0)
    def _():
        for h in range(2):
            own_a(h).start()

    pass_on(0)
    pass_on(1)
    start_load_first(0)

    @pl.loop(2, AHEAD)
    def _(t):
        pass_on(t)

    @pl.when(core == 1)
    def _():
        for m in early:
            for h in range(2):
                send_a(m, h).wait_send()
        for h in range(2):
            own_a(h).start()

    for h in range(2):
        own_a(h).wait()

    @pl.when(core == 1)
    def _():
        start_a(late)

    for copy in load_b(0, 0):
        copy.wait()

    @pl.loop(0, n_blocks + SLOTS)
    def _(s):
        @pl.when(s < n_blocks)
        def _():
            @pl.when(s > 0)
            def _():
                for copy in load_b(s, 0):
                    copy.wait()

            @pl.when(s == SLOTS)
            def _():
                for m in range(TILES):
                    send_first(m).wait_send()

            @pl.when(s > SLOTS)
            def _():
                send_block(s - SLOTS).wait_send()

            @pl.loop(0, TILES)
            def _(m):
                @pl.when(s == 0)
                def _():
                    for h in range(2):
                        send_a(m, h).wait_recv()

                p_buf[lax.rem(s, SLOTS), rows_of(m), :] = product(1, m, 0)

                @pl.when(s == 0)
                def _():
                    send_first(m).start()

            @pl.when(s == last)
            def _():
                for copy in store_p():
                    copy.start()

            @pl.when(jnp.logical_and(s > 0, s < last))
            def _():
                send_block(s).start()

            @pl.when(s + AHEAD < n_blocks)
            def _():
                pass_on(s + AHEAD)

            @pl.when(s + 1 < n_blocks)
            def _():
                start_load_first(s + 1)

        @pl.when(s >= SLOTS)
        def _():
            q = s - SLOTS

            @pl.when(q == 0)
            def _():
                for m in range(TILES):
                    send_first(m).wait_recv()

            @pl.when(jnp.logical_and(q > 0, q < last - 1))
            def _():
                send_block(q).wait_recv()

            @pl.when(q < last - 1)
            def _():
                load_r(q).start()

            for copy in load_b(q, 1):
                copy.wait()

            @pl.when(q == last)
            def _():
                store_q_done().wait()

            @pl.loop(0, TILES)
            def _(m):
                q_buf[rows_of(m), :] = product(0, m, 1)

            @pl.when(q == last - 1)
            def _():
                store_q_done().start()

            @pl.when(q == last)
            def _():
                for copy in store_q():
                    copy.start()

            @pl.when(q + 1 < n_blocks)
            def _():
                for copy in load_b(q + 1, 1):
                    copy.start()

            @pl.when(q < last - 1)
            def _():
                load_r(q).wait()

                @pl.when(q > 0)
                def _():
                    store_c(q - 1).wait()

                @pl.loop(0, TILES)
                def _(m):
                    rows = rows_of(m)
                    c_buf[rows, :] = (q_buf[rows, :] + r_buf[rows, :]).astype(c_buf.dtype)

                store_c(q).start()

        @pl.when(s == SLOTS - 1)
        def _():
            for copy in load_b(0, 1):
                copy.start()

    @pl.loop(n_blocks - RING, n_blocks)
    def _(t):
        send_b(1, t).wait_send()
        send_b(2, t).wait_send()

        @pl.when(t >= n_blocks - RING + AHEAD)
        def _():
            send_b(0, t).wait_send()

    store_c(last - 2).wait()
    for copy in store_q() + store_p():
        copy.wait()
    for h in range(2):
        @pl.when(core == 0)
        def _():
            for m in early:
                send_a(m, h).wait_send()

        for m in late:
            send_a(m, h).wait_send()

    @pl.loop(n_blocks - SLOTS, last)
    def _(s):
        send_block(s).wait_send()

    send_block(last - 1).wait_recv()


def write_out(c_ref, q_ref, r_ref, out_ref, c_buf, q_buf, r_buf, o_buf, load_sem, store_sem):
    rows, done = c_buf.shape
    step = rows // PIECES

    def load(i):
        some = pl.ds(i * step, step)
        return pltpu.make_async_copy(c_ref.at[some, pl.ds(0, done)], c_buf.at[some], load_sem.at[i])

    def store(i):
        some = pl.ds(i * step, step)
        return pltpu.make_async_copy(c_buf.at[some], out_ref.at[some, pl.ds(0, done)], store_sem.at[i])

    load_q = pltpu.make_async_copy(q_ref, q_buf, load_sem.at[PIECES])
    load_r = pltpu.make_async_copy(r_ref.at[r_ref.shape[0] - 1], r_buf, load_sem.at[PIECES + 1])
    store_sum = pltpu.make_async_copy(o_buf, out_ref.at[:, pl.ds(done, o_buf.shape[1])], store_sem.at[PIECES])
    for i in range(PIECES):
        load(i).start()
    load_q.start()
    load_r.start()
    for i in range(PIECES):
        load(i).wait()
        store(i).start()
    load_q.wait()
    load_r.wait()
    o_buf[...] = (q_buf[...] + r_buf[...]).astype(o_buf.dtype)
    store_sum.start()
    for i in range(PIECES):
        store(i).wait()
    store_sum.wait()


def device_product(block, a_rows, b_rows):
    rows, _ = a_rows.shape
    depth, n_cols = b_rows.shape
    n_blocks, tile, early = n_cols // block, rows // TILES, rows - LATE
    last = n_blocks - 1
    anywhere = pl.BlockSpec(memory_space=pl.ANY)
    dma = pltpu.SemaphoreType.DMA
    c_main, r_got, p_early, p_late, q_early, q_late, q_done, _ = pl.pallas_call(
        functools.partial(kernel, n_blocks, tile),
        out_shape=(
            jax.ShapeDtypeStruct((rows, n_cols), jnp.bfloat16),
            jax.ShapeDtypeStruct((last, rows, block), jnp.float32),
            jax.ShapeDtypeStruct((early, block), jnp.float32),
            jax.ShapeDtypeStruct((LATE, block), jnp.float32),
            jax.ShapeDtypeStruct((early, block), jnp.float32),
            jax.ShapeDtypeStruct((LATE, block), jnp.float32),
            jax.ShapeDtypeStruct((rows, block), jnp.float32),
            jax.ShapeDtypeStruct((3, n_blocks, depth, block), jnp.bfloat16),
        ),
        in_specs=[anywhere] * 2,
        out_specs=(anywhere,) * 8,
        scratch_shapes=[
            pltpu.VMEM((2, rows, 4 * depth), jnp.bfloat16),
            pltpu.VMEM((2, 4 * depth, block), jnp.bfloat16),
            pltpu.VMEM((SLOTS, rows, block), jnp.float32),
            pltpu.VMEM((rows, block), jnp.float32),
            pltpu.VMEM((rows, block), jnp.float32),
            pltpu.VMEM((rows, block), jnp.bfloat16),
            dma((2,)),
            dma((TILES, 2)),
            dma((TILES, 2)),
            dma((3, RING)),
            dma((3, RING)),
            dma((2, 4)),
            dma((TILES,)),
            dma((TILES,)),
            dma((SLOTS,)),
            dma((RING,)),
            dma,
            dma,
            dma((2,)),
            dma((2,)),
            pltpu.SemaphoreType.REGULAR,
        ],
        compiler_params=pltpu.CompilerParams(
            collective_id=0, has_side_effects=True, vmem_limit_bytes=66_000_000
        ),
        name="split_sum_product",
    )(a_rows, b_rows)

    swap = [(0, 1), (1, 0)]
    got_early = lax.ppermute(p_early, "row", swap)
    got_late = lax.ppermute(p_late, "row", swap)
    out = pl.pallas_call(
        write_out,
        out_shape=jax.ShapeDtypeStruct((rows, n_cols), jnp.bfloat16),
        in_specs=[anywhere] * 3,
        out_specs=anywhere,
        scratch_shapes=[
            pltpu.VMEM((rows, (last - 1) * block), jnp.bfloat16),
            pltpu.VMEM((rows, block), jnp.float32),
            pltpu.VMEM((rows, block), jnp.float32),
            pltpu.VMEM((rows, block), jnp.bfloat16),
            dma((PIECES + 2,)),
            dma((PIECES + 1,)),
        ],
        cost_estimate=pl.CostEstimate(flops=20_000_000_000, bytes_accessed=4 * rows * n_cols, transcendentals=0),
        name="write_out",
    )(c_main, q_done, r_got)
    for start, own, part in ((0, q_early, got_early), (early, q_late, got_late)):
        out = lax.dynamic_update_slice(out, (own + part).astype(out.dtype), (start, last * block))
    return out


def solution(mesh, block=BLOCK):
    all_axes = ("depth", "row", "col")
    return jax.shard_map(
        functools.partial(device_product, block),
        mesh=mesh,
        in_specs=(P(all_axes, None), P(all_axes, None)),
        out_specs=P(all_axes, None),
        check_vma=False,
    )
```

```python
import functools

import jax
import jax.numpy as jnp
from jax import lax
from jax.experimental import pallas as pl
from jax.experimental.pallas import tpu as pltpu
from jax.sharding import PartitionSpec as P


MESH = pl.DeviceIdType.MESH
BLOCK = 512
TILES = 4
AHEAD = 4
SLOTS = 3
LATE = 128
HUB = (1, 0)
PIECES = 2
RING = 2 * (SLOTS + 1)


def kernel(
    n_blocks, tile, a_ref, b_ref, c_ref, r_got, p_early, p_late, q_early, q_late, q_done, b_got,
    a_buf, b_buf, p_buf, q_buf, r_buf, c_buf,
    a_own_sem, a_send, a_recv, b_send, b_recv, b_load_sem, first_send, first_recv, p_send, r_recv, r_load_sem, c_sem, q_sem, last_sem, here_sem,
):
    last = n_blocks - 1
    col, row, core = lax.axis_index("col"), lax.axis_index("row"), lax.axis_index("depth")
    neighbour, partner, sibling = {"col": 1 - col}, {"row": 1 - row}, {"depth": 1 - core}
    depth, block = b_ref.shape[0], b_buf.shape[2]

    def rows_of(m):
        return pl.ds(pl.multiple_of(m * tile, tile), tile)

    def cols_of(t):
        return pl.ds(pl.multiple_of(t * block, block), block)

    def a_cols(h, r):
        return pl.ds(pl.multiple_of((h * 4 + r * 2) * depth, depth), 2 * depth)

    def a_half(h):
        return pl.ds(h * 2 * depth, 2 * depth)

    def own_a(h):
        return pltpu.make_async_copy(a_ref.at[:, a_cols(h, row)], a_buf.at[0, :, a_half(h)], a_own_sem.at[h])

    def send_a(m, h):
        return pltpu.make_async_remote_copy(
            src_ref=a_ref.at[rows_of(m), a_cols(h, 1 - row)], dst_ref=a_buf.at[1, rows_of(m), a_half(h)],
            send_sem=a_send.at[m, h], recv_sem=a_recv.at[m, h], device_id=partner, device_id_type=MESH)

    def send_b(way, t):
        return pltpu.make_async_remote_copy(
            src_ref=b_got.at[0, t] if way == 2 else b_ref.at[:, cols_of(t)], dst_ref=b_got.at[way, t],
            send_sem=b_send.at[way, lax.rem(t, RING)], recv_sem=b_recv.at[way, lax.rem(t, RING)],
            device_id=neighbour if way == 0 else sibling, device_id_type=MESH)

    def load_b(t, slot):
        places = (core * 2 + col, core * 2 + 1 - col, (1 - core) * 2 + col, (1 - core) * 2 + 1 - col)
        return [
            pltpu.make_async_copy(
                b_ref.at[:, cols_of(t)] if i == 0 else b_got.at[i - 1, t],
                b_buf.at[slot, pl.ds(pl.multiple_of(place * depth, depth), depth), :], b_load_sem.at[slot, i])
            for i, place in enumerate(places)
        ]

    def send_first(m):
        return pltpu.make_async_remote_copy(
            src_ref=p_buf.at[0, rows_of(m)], dst_ref=r_got.at[0, rows_of(m)],
            send_sem=first_send.at[m], recv_sem=first_recv.at[m], device_id=partner, device_id_type=MESH)

    def send_block(s):
        return pltpu.make_async_remote_copy(
            src_ref=p_buf.at[lax.rem(s, SLOTS)], dst_ref=r_got.at[s],
            send_sem=p_send.at[lax.rem(s, SLOTS)], recv_sem=r_recv.at[lax.rem(s, RING)], device_id=partner, device_id_type=MESH)

    def load_r(q):
        return pltpu.make_async_copy(r_got.at[q], r_buf, r_load_sem)

    def store_c(q):
        return pltpu.make_async_copy(c_buf, c_ref.at[:, cols_of(q)], c_sem)

    parts = (pl.ds(0, p_early.shape[0]), pl.ds(p_early.shape[0], p_late.shape[0]))

    def store_q_done():
        return pltpu.make_async_copy(q_buf, q_done, q_sem.at[0])

    def store_q():
        return [
            pltpu.make_async_copy(q_buf.at[part], out, q_sem.at[i])
            for i, (part, out) in enumerate(zip(parts, (q_early, q_late)))
        ]

    def store_p():
        return [
            pltpu.make_async_copy(p_buf.at[last % SLOTS, part], out, last_sem.at[i])
            for i, (part, out) in enumerate(zip(parts, (p_early, p_late)))
        ]

    def product(whose, m, slot):
        return jnp.dot(a_buf[whose, rows_of(m), :], b_buf[slot], preferred_element_type=jnp.float32)

    def pass_on(t):
        @pl.when(t >= RING - AHEAD)
        def _():
            send_b(0, t + AHEAD - RING).wait_send()

        @pl.when(t >= RING)
        def _():
            send_b(1, t - RING).wait_send()
            send_b(2, t - RING).wait_send()

        send_b(0, t).wait_recv()
        send_b(2, t).start()
        send_b(1, t).start()

        @pl.when(t + AHEAD < n_blocks)
        def _():
            send_b(0, t + AHEAD).start()

    def start_load_first(t):
        send_b(1, t).wait_recv()
        send_b(2, t).wait_recv()
        for copy in load_b(t, 0):
            copy.start()

    barrier = pltpu.get_barrier_semaphore()
    is_hub = jnp.logical_and(col == HUB[0], core == HUB[1])
    pl.semaphore_signal(barrier, inc=1, device_id=partner, device_id_type=MESH)

    @pl.when(jnp.logical_not(is_hub))
    def _():
        hub = {"col": HUB[0], "depth": HUB[1]}
        pl.semaphore_signal(barrier, inc=1, device_id=hub, device_id_type=MESH)
        pl.semaphore_wait(barrier, 1)

    @pl.when(is_hub)
    def _():
        pl.semaphore_wait(barrier, 4)
        for other in (neighbour, sibling, {**neighbour, **sibling}):
            pl.semaphore_signal(here_sem, inc=1, device_id=other, device_id_type=MESH)

    def start_a(tiles):
        for m in tiles:
            for h in range(2):
                send_a(m, h).start()

    early, late = range(2), range(2, TILES)
    start_a(early)

    @pl.when(jnp.logical_not(is_hub))
    def _():
        pl.semaphore_wait(here_sem, 1)

    for t in range(AHEAD):
        send_b(0, t).start()

    @pl.when(core == 0)
    def _():
        start_a(late)

    @pl.when(core == 0)
    def _():
        for h in range(2):
            own_a(h).start()

    pass_on(0)
    pass_on(1)
    start_load_first(0)

    @pl.loop(2, AHEAD)
    def _(t):
        pass_on(t)

    @pl.when(core == 1)
    def _():
        for m in early:
            for h in range(2):
                send_a(m, h).wait_send()
        for h in range(2):
            own_a(h).start()

    for h in range(2):
        own_a(h).wait()

    @pl.when(core == 1)
    def _():
        start_a(late)

    for copy in load_b(0, 0):
        copy.wait()

    @pl.loop(0, n_blocks + SLOTS)
    def _(s):
        @pl.when(s < n_blocks)
        def _():
            @pl.when(s > 0)
            def _():
                for copy in load_b(s, 0):
                    copy.wait()

            @pl.when(s == SLOTS)
            def _():
                for m in range(TILES):
                    send_first(m).wait_send()

            @pl.when(s > SLOTS)
            def _():
                send_block(s - SLOTS).wait_send()

            @pl.loop(0, TILES)
            def _(m):
                @pl.when(s == 0)
                def _():
                    for h in range(2):
                        send_a(m, h).wait_recv()

                p_buf[lax.rem(s, SLOTS), rows_of(m), :] = product(1, m, 0)

                @pl.when(s == 0)
                def _():
                    send_first(m).start()

            @pl.when(s == last)
            def _():
                for copy in store_p():
                    copy.start()

            @pl.when(jnp.logical_and(s > 0, s < last))
            def _():
                send_block(s).start()

            @pl.when(s + AHEAD < n_blocks)
            def _():
                pass_on(s + AHEAD)

            @pl.when(s + 1 < n_blocks)
            def _():
                start_load_first(s + 1)

        @pl.when(s >= SLOTS)
        def _():
            q = s - SLOTS

            @pl.when(q == 0)
            def _():
                for m in range(TILES):
                    send_first(m).wait_recv()

            @pl.when(jnp.logical_and(q > 0, q < last - 1))
            def _():
                send_block(q).wait_recv()

            @pl.when(q < last - 1)
            def _():
                load_r(q).start()

            for copy in load_b(q, 1):
                copy.wait()

            @pl.when(q == last)
            def _():
                store_q_done().wait()

            @pl.loop(0, TILES)
            def _(m):
                q_buf[rows_of(m), :] = product(0, m, 1)

            @pl.when(q == last - 1)
            def _():
                store_q_done().start()

            @pl.when(q == last)
            def _():
                for copy in store_q():
                    copy.start()

            @pl.when(q + 1 < n_blocks)
            def _():
                for copy in load_b(q + 1, 1):
                    copy.start()

            @pl.when(q < last - 1)
            def _():
                load_r(q).wait()

                @pl.when(q > 0)
                def _():
                    store_c(q - 1).wait()

                @pl.loop(0, TILES)
                def _(m):
                    rows = rows_of(m)
                    c_buf[rows, :] = (q_buf[rows, :] + r_buf[rows, :]).astype(c_buf.dtype)

                store_c(q).start()

        @pl.when(s == SLOTS - 1)
        def _():
            for copy in load_b(0, 1):
                copy.start()

    @pl.loop(n_blocks - RING, n_blocks)
    def _(t):
        send_b(1, t).wait_send()
        send_b(2, t).wait_send()

        @pl.when(t >= n_blocks - RING + AHEAD)
        def _():
            send_b(0, t).wait_send()

    store_c(last - 2).wait()
    for copy in store_q() + store_p():
        copy.wait()
    for h in range(2):
        @pl.when(core == 0)
        def _():
            for m in early:
                send_a(m, h).wait_send()

        for m in late:
            send_a(m, h).wait_send()

    @pl.loop(n_blocks - SLOTS, last)
    def _(s):
        send_block(s).wait_send()

    send_block(last - 1).wait_recv()


def write_out(c_ref, q_ref, r_ref, out_ref, c_buf, q_buf, r_buf, o_buf, load_sem, store_sem):
    rows, done = c_buf.shape
    step = rows // PIECES

    def load(i):
        some = pl.ds(i * step, step)
        return pltpu.make_async_copy(c_ref.at[some, pl.ds(0, done)], c_buf.at[some], load_sem.at[i])

    def store(i):
        some = pl.ds(i * step, step)
        return pltpu.make_async_copy(c_buf.at[some], out_ref.at[some, pl.ds(0, done)], store_sem.at[i])

    load_q = pltpu.make_async_copy(q_ref, q_buf, load_sem.at[PIECES])
    load_r = pltpu.make_async_copy(r_ref.at[r_ref.shape[0] - 1], r_buf, load_sem.at[PIECES + 1])
    store_sum = pltpu.make_async_copy(o_buf, out_ref.at[:, pl.ds(done, o_buf.shape[1])], store_sem.at[PIECES])
    for i in range(PIECES):
        load(i).start()
    load_q.start()
    load_r.start()
    for i in range(PIECES):
        load(i).wait()
        store(i).start()
    load_q.wait()
    load_r.wait()
    o_buf[...] = (q_buf[...] + r_buf[...]).astype(o_buf.dtype)
    store_sum.start()
    for i in range(PIECES):
        store(i).wait()
    store_sum.wait()


def device_product(block, a_rows, b_rows):
    rows, _ = a_rows.shape
    depth, n_cols = b_rows.shape
    n_blocks, tile, early = n_cols // block, rows // TILES, rows - LATE
    last = n_blocks - 1
    anywhere = pl.BlockSpec(memory_space=pl.ANY)
    dma = pltpu.SemaphoreType.DMA
    c_main, r_got, p_early, p_late, q_early, q_late, q_done, _ = pl.pallas_call(
        functools.partial(kernel, n_blocks, tile),
        out_shape=(
            jax.ShapeDtypeStruct((rows, n_cols), jnp.bfloat16),
            jax.ShapeDtypeStruct((last, rows, block), jnp.float32),
            jax.ShapeDtypeStruct((early, block), jnp.float32),
            jax.ShapeDtypeStruct((LATE, block), jnp.float32),
            jax.ShapeDtypeStruct((early, block), jnp.float32),
            jax.ShapeDtypeStruct((LATE, block), jnp.float32),
            jax.ShapeDtypeStruct((rows, block), jnp.float32),
            jax.ShapeDtypeStruct((3, n_blocks, depth, block), jnp.bfloat16),
        ),
        in_specs=[anywhere] * 2,
        out_specs=(anywhere,) * 8,
        scratch_shapes=[
            pltpu.VMEM((2, rows, 4 * depth), jnp.bfloat16),
            pltpu.VMEM((2, 4 * depth, block), jnp.bfloat16),
            pltpu.VMEM((SLOTS, rows, block), jnp.float32),
            pltpu.VMEM((rows, block), jnp.float32),
            pltpu.VMEM((rows, block), jnp.float32),
            pltpu.VMEM((rows, block), jnp.bfloat16),
            dma((2,)),
            dma((TILES, 2)),
            dma((TILES, 2)),
            dma((3, RING)),
            dma((3, RING)),
            dma((2, 4)),
            dma((TILES,)),
            dma((TILES,)),
            dma((SLOTS,)),
            dma((RING,)),
            dma,
            dma,
            dma((2,)),
            dma((2,)),
            pltpu.SemaphoreType.REGULAR,
        ],
        compiler_params=pltpu.CompilerParams(
            collective_id=0, has_side_effects=True, vmem_limit_bytes=66_000_000
        ),
        name="split_sum_product",
    )(a_rows, b_rows)

    swap = [(0, 1), (1, 0)]
    got_early = lax.ppermute(p_early, "row", swap)
    got_late = lax.ppermute(p_late, "row", swap)
    out = pl.pallas_call(
        write_out,
        out_shape=jax.ShapeDtypeStruct((rows, n_cols), jnp.bfloat16),
        in_specs=[anywhere] * 3,
        out_specs=anywhere,
        scratch_shapes=[
            pltpu.VMEM((rows, (last - 1) * block), jnp.bfloat16),
            pltpu.VMEM((rows, block), jnp.float32),
            pltpu.VMEM((rows, block), jnp.float32),
            pltpu.VMEM((rows, block), jnp.bfloat16),
            dma((PIECES + 2,)),
            dma((PIECES + 1,)),
        ],
        cost_estimate=pl.CostEstimate(flops=20_000_000_000, bytes_accessed=4 * rows * n_cols, transcendentals=0),
        name="write_out",
    )(c_main, q_done, r_got)
    for start, own, part in ((0, q_early, got_early), (early, q_late, got_late)):
        out = lax.dynamic_update_slice(out, (own + part).astype(out.dtype), (start, last * block))
    return out


def solution(mesh, block=BLOCK):
    all_axes = ("depth", "row", "col")
    return jax.shard_map(
        functools.partial(device_product, block),
        mesh=mesh,
        in_specs=(P(all_axes, None), P(all_axes, None)),
        out_specs=P(all_axes, None),
        check_vma=False,
    )
```

```python
import functools

import jax
import jax.numpy as jnp
from jax import lax
from jax.experimental import pallas as pl
from jax.experimental.pallas import tpu as pltpu
from jax.sharding import PartitionSpec as P


MESH = pl.DeviceIdType.MESH
BLOCK = 512
TILES = 4
AHEAD = 4
SLOTS = 3
PARTS = (8, 6, 2)
HUB = (1, 0)
PIECES = 1
RING = 2 * (SLOTS + 1)


def kernel(
    n_blocks, tile, a_ref, b_ref, c_ref, r_got, q_done, b_got, *rest,
):
    p_parts, q_parts, rest = rest[: len(PARTS)], rest[len(PARTS) : 2 * len(PARTS)], rest[2 * len(PARTS) :]
    (a_buf, b_buf, p_buf, q_buf, r_buf, c_buf,
    a_own_sem, a_send, a_recv, b_send, b_recv, b_load_sem, first_send, first_recv, p_send, r_recv, r_load_sem, c_sem, q_sem, last_sem, here_sem) = rest
    last = n_blocks - 1
    col, row, core = lax.axis_index("col"), lax.axis_index("row"), lax.axis_index("depth")
    neighbour, partner, sibling = {"col": 1 - col}, {"row": 1 - row}, {"depth": 1 - core}
    depth, block = b_ref.shape[0], b_buf.shape[2]

    def rows_of(m):
        return pl.ds(pl.multiple_of(m * tile, tile), tile)

    def cols_of(t):
        return pl.ds(pl.multiple_of(t * block, block), block)

    def a_cols(h, r):
        return pl.ds(pl.multiple_of((h * 4 + r * 2) * depth, depth), 2 * depth)

    def a_half(h):
        return pl.ds(h * 2 * depth, 2 * depth)

    def own_a(h):
        return pltpu.make_async_copy(a_ref.at[:, a_cols(h, row)], a_buf.at[0, :, a_half(h)], a_own_sem.at[h])

    def send_a(m, h):
        return pltpu.make_async_remote_copy(
            src_ref=a_ref.at[rows_of(m), a_cols(h, 1 - row)], dst_ref=a_buf.at[1, rows_of(m), a_half(h)],
            send_sem=a_send.at[m, h], recv_sem=a_recv.at[m, h], device_id=partner, device_id_type=MESH)

    def send_b(way, t):
        return pltpu.make_async_remote_copy(
            src_ref=b_got.at[0, t] if way == 2 else b_ref.at[:, cols_of(t)], dst_ref=b_got.at[way, t],
            send_sem=b_send.at[way, lax.rem(t, RING)], recv_sem=b_recv.at[way, lax.rem(t, RING)],
            device_id=neighbour if way == 0 else sibling, device_id_type=MESH)

    def load_b(t, slot):
        places = (core * 2 + col, core * 2 + 1 - col, (1 - core) * 2 + col, (1 - core) * 2 + 1 - col)
        return [
            pltpu.make_async_copy(
                b_ref.at[:, cols_of(t)] if i == 0 else b_got.at[i - 1, t],
                b_buf.at[slot, pl.ds(pl.multiple_of(place * depth, depth), depth), :], b_load_sem.at[slot, i])
            for i, place in enumerate(places)
        ]

    def send_first(m):
        return pltpu.make_async_remote_copy(
            src_ref=p_buf.at[0, rows_of(m)], dst_ref=r_got.at[0, rows_of(m)],
            send_sem=first_send.at[m], recv_sem=first_recv.at[m], device_id=partner, device_id_type=MESH)

    def send_block(s):
        return pltpu.make_async_remote_copy(
            src_ref=p_buf.at[lax.rem(s, SLOTS)], dst_ref=r_got.at[s],
            send_sem=p_send.at[lax.rem(s, SLOTS)], recv_sem=r_recv.at[lax.rem(s, RING)], device_id=partner, device_id_type=MESH)

    def load_r(q):
        return pltpu.make_async_copy(r_got.at[q], r_buf, r_load_sem)

    def store_c(q):
        return pltpu.make_async_copy(c_buf, c_ref.at[:, cols_of(q)], c_sem)

    sixteenth = p_buf.shape[1] // sum(PARTS)
    parts = [pl.ds(sum(PARTS[:i]) * sixteenth, n * sixteenth) for i, n in enumerate(PARTS)]

    def store_q_done():
        return pltpu.make_async_copy(q_buf, q_done, q_sem.at[0])

    def store_q():
        return [
            pltpu.make_async_copy(q_buf.at[part], out, q_sem.at[i])
            for i, (part, out) in enumerate(zip(parts, q_parts))
        ]

    def store_p():
        return [
            pltpu.make_async_copy(p_buf.at[last % SLOTS, part], out, last_sem.at[i])
            for i, (part, out) in enumerate(zip(parts, p_parts))
        ]

    def product(whose, m, slot):
        return jnp.dot(a_buf[whose, rows_of(m), :], b_buf[slot], preferred_element_type=jnp.float32)

    def pass_on(t):
        @pl.when(t >= RING - AHEAD)
        def _():
            send_b(0, t + AHEAD - RING).wait_send()

        @pl.when(t >= RING)
        def _():
            send_b(1, t - RING).wait_send()
            send_b(2, t - RING).wait_send()

        send_b(0, t).wait_recv()
        send_b(2, t).start()
        send_b(1, t).start()

        @pl.when(t + AHEAD < n_blocks)
        def _():
            send_b(0, t + AHEAD).start()

    def start_load_first(t):
        send_b(1, t).wait_recv()
        send_b(2, t).wait_recv()
        for copy in load_b(t, 0):
            copy.start()

    barrier = pltpu.get_barrier_semaphore()
    is_hub = jnp.logical_and(col == HUB[0], core == HUB[1])
    pl.semaphore_signal(barrier, inc=1, device_id=partner, device_id_type=MESH)

    @pl.when(jnp.logical_not(is_hub))
    def _():
        hub = {"col": HUB[0], "depth": HUB[1]}
        pl.semaphore_signal(barrier, inc=1, device_id=hub, device_id_type=MESH)
        pl.semaphore_wait(barrier, 1)

    @pl.when(is_hub)
    def _():
        pl.semaphore_wait(barrier, 4)
        for other in (neighbour, sibling, {**neighbour, **sibling}):
            pl.semaphore_signal(here_sem, inc=1, device_id=other, device_id_type=MESH)

    def start_a(tiles):
        for m in tiles:
            for h in range(2):
                send_a(m, h).start()

    early, late = range(2), range(2, TILES)
    start_a(early)

    @pl.when(jnp.logical_not(is_hub))
    def _():
        pl.semaphore_wait(here_sem, 1)

    for t in range(AHEAD):
        send_b(0, t).start()

    @pl.when(core == 0)
    def _():
        start_a(late)

    @pl.when(core == 0)
    def _():
        for h in range(2):
            own_a(h).start()

    pass_on(0)
    pass_on(1)
    start_load_first(0)

    @pl.loop(2, AHEAD)
    def _(t):
        pass_on(t)

    @pl.when(core == 1)
    def _():
        for m in early:
            for h in range(2):
                send_a(m, h).wait_send()
        for h in range(2):
            own_a(h).start()

    for h in range(2):
        own_a(h).wait()

    @pl.when(core == 1)
    def _():
        start_a(late)

    for copy in load_b(0, 0):
        copy.wait()

    @pl.loop(0, n_blocks + SLOTS)
    def _(s):
        @pl.when(s < n_blocks)
        def _():
            @pl.when(s > 0)
            def _():
                for copy in load_b(s, 0):
                    copy.wait()

            @pl.when(s == SLOTS)
            def _():
                for m in range(TILES):
                    send_first(m).wait_send()

            @pl.when(s > SLOTS)
            def _():
                send_block(s - SLOTS).wait_send()

            @pl.loop(0, TILES)
            def _(m):
                @pl.when(s == 0)
                def _():
                    for h in range(2):
                        send_a(m, h).wait_recv()

                p_buf[lax.rem(s, SLOTS), rows_of(m), :] = product(1, m, 0)

                @pl.when(s == 0)
                def _():
                    send_first(m).start()

            @pl.when(s == last)
            def _():
                for copy in store_p():
                    copy.start()

            @pl.when(jnp.logical_and(s > 0, s < last))
            def _():
                send_block(s).start()

            @pl.when(s + AHEAD < n_blocks)
            def _():
                pass_on(s + AHEAD)

            @pl.when(s + 1 < n_blocks)
            def _():
                start_load_first(s + 1)

        @pl.when(s >= SLOTS)
        def _():
            q = s - SLOTS

            @pl.when(q == 0)
            def _():
                for m in range(TILES):
                    send_first(m).wait_recv()

            @pl.when(jnp.logical_and(q > 0, q < last - 1))
            def _():
                send_block(q).wait_recv()

            @pl.when(q < last - 1)
            def _():
                load_r(q).start()

            for copy in load_b(q, 1):
                copy.wait()

            @pl.when(q == last)
            def _():
                store_q_done().wait()

            @pl.loop(0, TILES)
            def _(m):
                q_buf[rows_of(m), :] = product(0, m, 1)

            @pl.when(q == last - 1)
            def _():
                store_q_done().start()

            @pl.when(q == last)
            def _():
                for copy in store_q():
                    copy.start()

            @pl.when(q + 1 < n_blocks)
            def _():
                for copy in load_b(q + 1, 1):
                    copy.start()

            @pl.when(q < last - 1)
            def _():
                load_r(q).wait()

                @pl.when(q > 0)
                def _():
                    store_c(q - 1).wait()

                @pl.loop(0, TILES)
                def _(m):
                    rows = rows_of(m)
                    c_buf[rows, :] = (q_buf[rows, :] + r_buf[rows, :]).astype(c_buf.dtype)

                store_c(q).start()

        @pl.when(s == SLOTS - 1)
        def _():
            for copy in load_b(0, 1):
                copy.start()

    @pl.loop(n_blocks - RING, n_blocks)
    def _(t):
        send_b(1, t).wait_send()
        send_b(2, t).wait_send()

        @pl.when(t >= n_blocks - RING + AHEAD)
        def _():
            send_b(0, t).wait_send()

    store_c(last - 2).wait()
    for copy in store_q() + store_p():
        copy.wait()
    for h in range(2):
        @pl.when(core == 0)
        def _():
            for m in early:
                send_a(m, h).wait_send()

        for m in late:
            send_a(m, h).wait_send()

    @pl.loop(n_blocks - SLOTS, last)
    def _(s):
        send_block(s).wait_send()

    send_block(last - 1).wait_recv()


def write_out(c_ref, q_ref, r_ref, out_ref, c_buf, q_buf, r_buf, o_buf, load_sem, store_sem):
    rows, done = c_buf.shape
    step = rows // PIECES

    def load(i):
        some = pl.ds(i * step, step)
        return pltpu.make_async_copy(c_ref.at[some, pl.ds(0, done)], c_buf.at[some], load_sem.at[i])

    def store(i):
        some = pl.ds(i * step, step)
        return pltpu.make_async_copy(c_buf.at[some], out_ref.at[some, pl.ds(0, done)], store_sem.at[i])

    load_q = pltpu.make_async_copy(q_ref, q_buf, load_sem.at[PIECES])
    load_r = pltpu.make_async_copy(r_ref.at[r_ref.shape[0] - 1], r_buf, load_sem.at[PIECES + 1])
    store_sum = pltpu.make_async_copy(o_buf, out_ref.at[:, pl.ds(done, o_buf.shape[1])], store_sem.at[PIECES])
    load_q.start()
    load_r.start()
    for i in range(PIECES):
        load(i).start()
    for i in range(PIECES):
        load(i).wait()
        store(i).start()
    load_q.wait()
    load_r.wait()
    o_buf[...] = (q_buf[...] + r_buf[...]).astype(o_buf.dtype)
    store_sum.start()
    for i in range(PIECES):
        store(i).wait()
    store_sum.wait()


def device_product(block, a_rows, b_rows):
    rows, _ = a_rows.shape
    depth, n_cols = b_rows.shape
    n_blocks, tile, sixteenth = n_cols // block, rows // TILES, rows // sum(PARTS)
    last = n_blocks - 1
    anywhere = pl.BlockSpec(memory_space=pl.ANY)
    dma = pltpu.SemaphoreType.DMA
    parts = [jax.ShapeDtypeStruct((n * sixteenth, block), jnp.float32) for n in PARTS]
    c_main, r_got, q_done, _, *rest = pl.pallas_call(
        functools.partial(kernel, n_blocks, tile),
        out_shape=(
            jax.ShapeDtypeStruct((rows, n_cols), jnp.bfloat16),
            jax.ShapeDtypeStruct((last, rows, block), jnp.float32),
            jax.ShapeDtypeStruct((rows, block), jnp.float32),
            jax.ShapeDtypeStruct((3, n_blocks, depth, block), jnp.bfloat16),
            *parts,
            *parts,
        ),
        in_specs=[anywhere] * 2,
        out_specs=(anywhere,) * (4 + 2 * len(PARTS)),
        scratch_shapes=[
            pltpu.VMEM((2, rows, 4 * depth), jnp.bfloat16),
            pltpu.VMEM((2, 4 * depth, block), jnp.bfloat16),
            pltpu.VMEM((SLOTS, rows, block), jnp.float32),
            pltpu.VMEM((rows, block), jnp.float32),
            pltpu.VMEM((rows, block), jnp.float32),
            pltpu.VMEM((rows, block), jnp.bfloat16),
            dma((2,)),
            dma((TILES, 2)),
            dma((TILES, 2)),
            dma((3, RING)),
            dma((3, RING)),
            dma((2, 4)),
            dma((TILES,)),
            dma((TILES,)),
            dma((SLOTS,)),
            dma((RING,)),
            dma,
            dma,
            dma((len(PARTS),)),
            dma((len(PARTS),)),
            pltpu.SemaphoreType.REGULAR,
        ],
        compiler_params=pltpu.CompilerParams(
            collective_id=0, has_side_effects=True, vmem_limit_bytes=66_000_000
        ),
        name="split_sum_product",
    )(a_rows, b_rows)

    p_parts, q_parts = rest[: len(PARTS)], rest[len(PARTS) :]
    got = []
    for part in p_parts:
        got.append(lax.ppermute(part, "row", [(0, 1), (1, 0)]))
    out = pl.pallas_call(
        write_out,
        out_shape=jax.ShapeDtypeStruct((rows, n_cols), jnp.bfloat16),
        in_specs=[anywhere] * 3,
        out_specs=anywhere,
        scratch_shapes=[
            pltpu.VMEM((rows, (last - 1) * block), jnp.bfloat16),
            pltpu.VMEM((rows, block), jnp.float32),
            pltpu.VMEM((rows, block), jnp.float32),
            pltpu.VMEM((rows, block), jnp.bfloat16),
            dma((PIECES + 2,)),
            dma((PIECES + 1,)),
        ],
        cost_estimate=pl.CostEstimate(flops=20_000_000_000, bytes_accessed=4 * rows * n_cols, transcendentals=0),
        name="write_out",
    )(c_main, q_done, r_got)
    for i, (own, part) in enumerate(zip(q_parts, got)):
        start = sum(PARTS[:i]) * sixteenth
        out = lax.dynamic_update_slice(out, (own + part).astype(out.dtype), (start, last * block))
    return out


def solution(mesh, block=BLOCK):
    all_axes = ("depth", "row", "col")
    return jax.shard_map(
        functools.partial(device_product, block),
        mesh=mesh,
        in_specs=(P(all_axes, None), P(all_axes, None)),
        out_specs=P(all_axes, None),
        check_vma=False,
    )
```

```python
import functools

import jax
import jax.numpy as jnp
from jax import lax
from jax.experimental import pallas as pl
from jax.experimental.pallas import tpu as pltpu
from jax.sharding import PartitionSpec as P


MESH = pl.DeviceIdType.MESH
BLOCK = 512
TILES = 4
AHEAD = 4
SLOTS = 3
LATE = 128
HUB = (1, 0)
SLAB = 16
ROUND = 8
PIECES = 2
RING = 2 * (SLOTS + 1)


def kernel(
    n_blocks, tile, a_ref, b_ref, c_ref, r_got, p_early, p_late, q_early, q_late, q_done, b_got, relay,
    a_buf, b_buf, p_buf, q_buf, r_buf, c_buf,
    a_own_sem, a_send, a_recv, b_send, b_recv, b_load_sem, first_send, first_recv, p_send, r_recv, r_load_sem, c_sem, q_sem, last_sem, here_sem, hop_send, hop_recv,
):
    last = n_blocks - 1
    col, row, core = lax.axis_index("col"), lax.axis_index("row"), lax.axis_index("depth")
    neighbour, partner, sibling = {"col": 1 - col}, {"row": 1 - row}, {"depth": 1 - core}
    depth, block = b_ref.shape[0], b_buf.shape[2]

    def rows_of(m):
        return pl.ds(pl.multiple_of(m * tile, tile), tile)

    def cols_of(t):
        return pl.ds(pl.multiple_of(t * block, block), block)

    def a_cols(h, r):
        return pl.ds(pl.multiple_of((h * 4 + r * 2) * depth, depth), 2 * depth)

    def a_half(h):
        return pl.ds(h * 2 * depth, 2 * depth)

    def own_a(h):
        return pltpu.make_async_copy(a_ref.at[:, a_cols(h, row)], a_buf.at[0, :, a_half(h)], a_own_sem.at[h])

    def send_a(m, h):
        return pltpu.make_async_remote_copy(
            src_ref=a_ref.at[rows_of(m), a_cols(h, 1 - row)], dst_ref=a_buf.at[1, rows_of(m), a_half(h)],
            send_sem=a_send.at[m, h], recv_sem=a_recv.at[m, h], device_id=partner, device_id_type=MESH)

    def send_b(way, t):
        return pltpu.make_async_remote_copy(
            src_ref=b_got.at[0, t] if way == 2 else b_ref.at[:, cols_of(t)], dst_ref=b_got.at[way, t],
            send_sem=b_send.at[way, lax.rem(t, RING)], recv_sem=b_recv.at[way, lax.rem(t, RING)],
            device_id=neighbour if way == 0 else sibling, device_id_type=MESH)

    def load_b(t, slot):
        places = (core * 2 + col, core * 2 + 1 - col, (1 - core) * 2 + col, (1 - core) * 2 + 1 - col)
        return [
            pltpu.make_async_copy(
                b_ref.at[:, cols_of(t)] if i == 0 else b_got.at[i - 1, t],
                b_buf.at[slot, pl.ds(pl.multiple_of(place * depth, depth), depth), :], b_load_sem.at[slot, i])
            for i, place in enumerate(places)
        ]

    def send_first(m):
        return pltpu.make_async_remote_copy(
            src_ref=p_buf.at[0, rows_of(m)], dst_ref=r_got.at[0, rows_of(m)],
            send_sem=first_send.at[m], recv_sem=first_recv.at[m], device_id=partner, device_id_type=MESH)

    def send_block(s):
        return pltpu.make_async_remote_copy(
            src_ref=p_buf.at[lax.rem(s, SLOTS)], dst_ref=r_got.at[s],
            send_sem=p_send.at[lax.rem(s, SLOTS)], recv_sem=r_recv.at[lax.rem(s, RING)], device_id=partner, device_id_type=MESH)

    slab, rest = pl.ds(0, SLAB), pl.ds(SLAB, p_buf.shape[1] - SLAB)

    def at(c, r):
        return jnp.logical_and(core == 1, jnp.logical_and(col == c, row == r))

    def send_rest():
        return pltpu.make_async_remote_copy(
            src_ref=p_buf.at[ROUND % SLOTS, rest], dst_ref=r_got.at[ROUND, rest],
            send_sem=p_send.at[ROUND % SLOTS], recv_sem=r_recv.at[ROUND % RING], device_id=partner, device_id_type=MESH)

    def hop(i):
        sources = (p_buf.at[ROUND % SLOTS, slab], relay.at[0], relay.at[1])
        targets = (relay.at[0], relay.at[1], r_got.at[ROUND, slab])
        return pltpu.make_async_remote_copy(
            src_ref=sources[i], dst_ref=targets[i], send_sem=hop_send.at[i], recv_sem=hop_recv.at[i],
            device_id=partner if i == 1 else neighbour, device_id_type=MESH)

    def load_r(q):
        return pltpu.make_async_copy(r_got.at[q], r_buf, r_load_sem)

    def store_c(q):
        return pltpu.make_async_copy(c_buf, c_ref.at[:, cols_of(q)], c_sem)

    parts = (pl.ds(0, p_early.shape[0]), pl.ds(p_early.shape[0], p_late.shape[0]))

    def store_q_done():
        return pltpu.make_async_copy(q_buf, q_done, q_sem.at[0])

    def store_q():
        return [
            pltpu.make_async_copy(q_buf.at[part], out, q_sem.at[i])
            for i, (part, out) in enumerate(zip(parts, (q_early, q_late)))
        ]

    def store_p():
        return [
            pltpu.make_async_copy(p_buf.at[last % SLOTS, part], out, last_sem.at[i])
            for i, (part, out) in enumerate(zip(parts, (p_early, p_late)))
        ]

    def product(whose, m, slot):
        return jnp.dot(a_buf[whose, rows_of(m), :], b_buf[slot], preferred_element_type=jnp.float32)

    def pass_on(t):
        @pl.when(t >= RING - AHEAD)
        def _():
            send_b(0, t + AHEAD - RING).wait_send()

        @pl.when(t >= RING)
        def _():
            send_b(1, t - RING).wait_send()
            send_b(2, t - RING).wait_send()

        send_b(0, t).wait_recv()
        send_b(2, t).start()
        send_b(1, t).start()

        @pl.when(t + AHEAD < n_blocks)
        def _():
            send_b(0, t + AHEAD).start()

    def start_load_first(t):
        send_b(1, t).wait_recv()
        send_b(2, t).wait_recv()
        for copy in load_b(t, 0):
            copy.start()

    barrier = pltpu.get_barrier_semaphore()
    is_hub = jnp.logical_and(col == HUB[0], core == HUB[1])
    pl.semaphore_signal(barrier, inc=1, device_id=partner, device_id_type=MESH)

    @pl.when(jnp.logical_not(is_hub))
    def _():
        hub = {"col": HUB[0], "depth": HUB[1]}
        pl.semaphore_signal(barrier, inc=1, device_id=hub, device_id_type=MESH)
        pl.semaphore_wait(barrier, 1)

    @pl.when(is_hub)
    def _():
        pl.semaphore_wait(barrier, 4)
        for other in (neighbour, sibling, {**neighbour, **sibling}):
            pl.semaphore_signal(here_sem, inc=1, device_id=other, device_id_type=MESH)

    def start_a(tiles):
        for m in tiles:
            for h in range(2):
                send_a(m, h).start()

    early, late = range(2), range(2, TILES)
    start_a(early)

    @pl.when(jnp.logical_not(is_hub))
    def _():
        pl.semaphore_wait(here_sem, 1)

    for t in range(AHEAD):
        send_b(0, t).start()

    @pl.when(core == 0)
    def _():
        start_a(late)

    @pl.when(core == 0)
    def _():
        for h in range(2):
            own_a(h).start()

    pass_on(0)
    pass_on(1)
    start_load_first(0)

    @pl.loop(2, AHEAD)
    def _(t):
        pass_on(t)

    @pl.when(core == 1)
    def _():
        for m in early:
            for h in range(2):
                send_a(m, h).wait_send()
        for h in range(2):
            own_a(h).start()

    for h in range(2):
        own_a(h).wait()

    @pl.when(core == 1)
    def _():
        start_a(late)

    for copy in load_b(0, 0):
        copy.wait()

    @pl.loop(0, n_blocks + SLOTS)
    def _(s):
        @pl.when(s < n_blocks)
        def _():
            @pl.when(s > 0)
            def _():
                for copy in load_b(s, 0):
                    copy.wait()

            @pl.when(s == SLOTS)
            def _():
                for m in range(TILES):
                    send_first(m).wait_send()

            slab_sent = jnp.logical_and(s == ROUND + SLOTS, at(0, 1))

            @pl.when(jnp.logical_and(s > SLOTS, jnp.logical_not(slab_sent)))
            def _():
                send_block(s - SLOTS).wait_send()

            @pl.when(slab_sent)
            def _():
                send_rest().wait_send()
                hop(0).wait_send()

            @pl.loop(0, TILES)
            def _(m):
                @pl.when(s == 0)
                def _():
                    for h in range(2):
                        send_a(m, h).wait_recv()

                p_buf[lax.rem(s, SLOTS), rows_of(m), :] = product(1, m, 0)

                @pl.when(s == 0)
                def _():
                    send_first(m).start()

            @pl.when(s == last)
            def _():
                for copy in store_p():
                    copy.start()

            slab_goes = jnp.logical_and(s == ROUND, at(0, 1))

            @pl.when(jnp.logical_and(jnp.logical_and(s > 0, s < last), jnp.logical_not(slab_goes)))
            def _():
                send_block(s).start()

            @pl.when(slab_goes)
            def _():
                send_rest().start()
                hop(0).start()

            for i, place in ((1, (1, 1)), (2, (1, 0))):
                @pl.when(jnp.logical_and(s == ROUND + i, at(*place)))
                def _():
                    hop(i - 1).wait_recv()
                    hop(i).start()

            @pl.when(s + AHEAD < n_blocks)
            def _():
                pass_on(s + AHEAD)

            @pl.when(s + 1 < n_blocks)
            def _():
                start_load_first(s + 1)

        @pl.when(s >= SLOTS)
        def _():
            q = s - SLOTS

            @pl.when(q == 0)
            def _():
                for m in range(TILES):
                    send_first(m).wait_recv()

            slab_comes = jnp.logical_and(q == ROUND, at(0, 0))

            @pl.when(jnp.logical_and(jnp.logical_and(q > 0, q < last - 1), jnp.logical_not(slab_comes)))
            def _():
                send_block(q).wait_recv()

            @pl.when(slab_comes)
            def _():
                send_rest().wait_recv()
                hop(2).wait_recv()

            @pl.when(q < last - 1)
            def _():
                load_r(q).start()

            for copy in load_b(q, 1):
                copy.wait()

            @pl.when(q == last)
            def _():
                store_q_done().wait()

            @pl.loop(0, TILES)
            def _(m):
                q_buf[rows_of(m), :] = product(0, m, 1)

            @pl.when(q == last - 1)
            def _():
                store_q_done().start()

            @pl.when(q == last)
            def _():
                for copy in store_q():
                    copy.start()

            @pl.when(q + 1 < n_blocks)
            def _():
                for copy in load_b(q + 1, 1):
                    copy.start()

            @pl.when(q < last - 1)
            def _():
                load_r(q).wait()

                @pl.when(q > 0)
                def _():
                    store_c(q - 1).wait()

                @pl.loop(0, TILES)
                def _(m):
                    rows = rows_of(m)
                    c_buf[rows, :] = (q_buf[rows, :] + r_buf[rows, :]).astype(c_buf.dtype)

                store_c(q).start()

        @pl.when(s == SLOTS - 1)
        def _():
            for copy in load_b(0, 1):
                copy.start()

    @pl.loop(n_blocks - RING, n_blocks)
    def _(t):
        send_b(1, t).wait_send()
        send_b(2, t).wait_send()

        @pl.when(t >= n_blocks - RING + AHEAD)
        def _():
            send_b(0, t).wait_send()

    for i, place in ((1, (1, 1)), (2, (1, 0))):
        @pl.when(at(*place))
        def _():
            hop(i).wait_send()

    store_c(last - 2).wait()
    for copy in store_q() + store_p():
        copy.wait()
    for h in range(2):
        @pl.when(core == 0)
        def _():
            for m in early:
                send_a(m, h).wait_send()

        for m in late:
            send_a(m, h).wait_send()

    @pl.loop(n_blocks - SLOTS, last)
    def _(s):
        send_block(s).wait_send()

    send_block(last - 1).wait_recv()


def write_out(c_ref, q_ref, r_ref, out_ref, c_buf, q_buf, r_buf, o_buf, load_sem, store_sem):
    rows, done = c_buf.shape
    step = rows // PIECES

    def load(i):
        some = pl.ds(i * step, step)
        return pltpu.make_async_copy(c_ref.at[some, pl.ds(0, done)], c_buf.at[some], load_sem.at[i])

    def store(i):
        some = pl.ds(i * step, step)
        return pltpu.make_async_copy(c_buf.at[some], out_ref.at[some, pl.ds(0, done)], store_sem.at[i])

    load_q = pltpu.make_async_copy(q_ref, q_buf, load_sem.at[PIECES])
    load_r = pltpu.make_async_copy(r_ref.at[r_ref.shape[0] - 1], r_buf, load_sem.at[PIECES + 1])
    store_sum = pltpu.make_async_copy(o_buf, out_ref.at[:, pl.ds(done, o_buf.shape[1])], store_sem.at[PIECES])
    for i in range(PIECES):
        load(i).start()
    load_q.start()
    load_r.start()
    for i in range(PIECES):
        load(i).wait()
        store(i).start()
    load_q.wait()
    load_r.wait()
    o_buf[...] = (q_buf[...] + r_buf[...]).astype(o_buf.dtype)
    store_sum.start()
    for i in range(PIECES):
        store(i).wait()
    store_sum.wait()


def device_product(block, a_rows, b_rows):
    rows, _ = a_rows.shape
    depth, n_cols = b_rows.shape
    n_blocks, tile, early = n_cols // block, rows // TILES, rows - LATE
    last = n_blocks - 1
    anywhere = pl.BlockSpec(memory_space=pl.ANY)
    dma = pltpu.SemaphoreType.DMA
    c_main, r_got, p_early, p_late, q_early, q_late, q_done, _, _ = pl.pallas_call(
        functools.partial(kernel, n_blocks, tile),
        out_shape=(
            jax.ShapeDtypeStruct((rows, n_cols), jnp.bfloat16),
            jax.ShapeDtypeStruct((last, rows, block), jnp.float32),
            jax.ShapeDtypeStruct((early, block), jnp.float32),
            jax.ShapeDtypeStruct((LATE, block), jnp.float32),
            jax.ShapeDtypeStruct((early, block), jnp.float32),
            jax.ShapeDtypeStruct((LATE, block), jnp.float32),
            jax.ShapeDtypeStruct((rows, block), jnp.float32),
            jax.ShapeDtypeStruct((3, n_blocks, depth, block), jnp.bfloat16),
            jax.ShapeDtypeStruct((2, SLAB, block), jnp.float32),
        ),
        in_specs=[anywhere] * 2,
        out_specs=(anywhere,) * 9,
        scratch_shapes=[
            pltpu.VMEM((2, rows, 4 * depth), jnp.bfloat16),
            pltpu.VMEM((2, 4 * depth, block), jnp.bfloat16),
            pltpu.VMEM((SLOTS, rows, block), jnp.float32),
            pltpu.VMEM((rows, block), jnp.float32),
            pltpu.VMEM((rows, block), jnp.float32),
            pltpu.VMEM((rows, block), jnp.bfloat16),
            dma((2,)),
            dma((TILES, 2)),
            dma((TILES, 2)),
            dma((3, RING)),
            dma((3, RING)),
            dma((2, 4)),
            dma((TILES,)),
            dma((TILES,)),
            dma((SLOTS,)),
            dma((RING,)),
            dma,
            dma,
            dma((2,)),
            dma((2,)),
            pltpu.SemaphoreType.REGULAR,
            dma((3,)),
            dma((3,)),
        ],
        compiler_params=pltpu.CompilerParams(
            collective_id=0, has_side_effects=True, vmem_limit_bytes=66_000_000
        ),
        name="split_sum_product",
    )(a_rows, b_rows)

    swap = [(0, 1), (1, 0)]
    got_early = lax.ppermute(p_early, "row", swap)
    got_late = lax.ppermute(p_late, "row", swap)
    out = pl.pallas_call(
        write_out,
        out_shape=jax.ShapeDtypeStruct((rows, n_cols), jnp.bfloat16),
        in_specs=[anywhere] * 3,
        out_specs=anywhere,
        scratch_shapes=[
            pltpu.VMEM((rows, (last - 1) * block), jnp.bfloat16),
            pltpu.VMEM((rows, block), jnp.float32),
            pltpu.VMEM((rows, block), jnp.float32),
            pltpu.VMEM((rows, block), jnp.bfloat16),
            dma((PIECES + 2,)),
            dma((PIECES + 1,)),
        ],
        cost_estimate=pl.CostEstimate(flops=20_000_000_000, bytes_accessed=4 * rows * n_cols, transcendentals=0),
        name="write_out",
    )(c_main, q_done, r_got)
    for start, own, part in ((0, q_early, got_early), (early, q_late, got_late)):
        out = lax.dynamic_update_slice(out, (own + part).astype(out.dtype), (start, last * block))
    return out


def solution(mesh, block=BLOCK):
    all_axes = ("depth", "row", "col")
    return jax.shard_map(
        functools.partial(device_product, block),
        mesh=mesh,
        in_specs=(P(all_axes, None), P(all_axes, None)),
        out_specs=P(all_axes, None),
        check_vma=False,
    )
```

```python
import functools

import jax
import jax.numpy as jnp
from jax import lax
from jax.experimental import pallas as pl
from jax.experimental.pallas import tpu as pltpu
from jax.sharding import PartitionSpec as P


MESH = pl.DeviceIdType.MESH
BLOCK = 512
TILES = 4
AHEAD = 4
SLOTS = 3
PARTS = (16, 12, 3, 1)
HUB = (1, 0)
SLAB = 16
ROUND = 8
PIECES = 1
RING = 2 * (SLOTS + 1)


def kernel(
    n_blocks, tile, a_ref, b_ref, c_ref, r_got, q_done, b_got, relay, *others,
):
    p_parts, q_parts, scratch = others[: len(PARTS)], others[len(PARTS) : 2 * len(PARTS)], others[2 * len(PARTS) :]
    (
        a_buf, b_buf, p_buf, q_buf, r_buf, c_buf,
        a_own_sem, a_send, a_recv, b_send, b_recv, b_load_sem, first_send, first_recv, p_send, r_recv,
        r_load_sem, c_sem, q_sem, last_sem, here_sem, hop_send, hop_recv,
    ) = scratch
    last = n_blocks - 1
    col, row, core = lax.axis_index("col"), lax.axis_index("row"), lax.axis_index("depth")
    neighbour, partner, sibling = {"col": 1 - col}, {"row": 1 - row}, {"depth": 1 - core}
    depth, block = b_ref.shape[0], b_buf.shape[2]

    def rows_of(m):
        return pl.ds(pl.multiple_of(m * tile, tile), tile)

    def cols_of(t):
        return pl.ds(pl.multiple_of(t * block, block), block)

    def a_cols(h, r):
        return pl.ds(pl.multiple_of((h * 4 + r * 2) * depth, depth), 2 * depth)

    def a_half(h):
        return pl.ds(h * 2 * depth, 2 * depth)

    def own_a(h):
        return pltpu.make_async_copy(a_ref.at[:, a_cols(h, row)], a_buf.at[0, :, a_half(h)], a_own_sem.at[h])

    def send_a(m, h):
        return pltpu.make_async_remote_copy(
            src_ref=a_ref.at[rows_of(m), a_cols(h, 1 - row)], dst_ref=a_buf.at[1, rows_of(m), a_half(h)],
            send_sem=a_send.at[m, h], recv_sem=a_recv.at[m, h], device_id=partner, device_id_type=MESH)

    def send_b(way, t):
        return pltpu.make_async_remote_copy(
            src_ref=b_got.at[0, t] if way == 2 else b_ref.at[:, cols_of(t)], dst_ref=b_got.at[way, t],
            send_sem=b_send.at[way, lax.rem(t, RING)], recv_sem=b_recv.at[way, lax.rem(t, RING)],
            device_id=neighbour if way == 0 else sibling, device_id_type=MESH)

    def load_b(t, slot):
        places = (core * 2 + col, core * 2 + 1 - col, (1 - core) * 2 + col, (1 - core) * 2 + 1 - col)
        return [
            pltpu.make_async_copy(
                b_ref.at[:, cols_of(t)] if i == 0 else b_got.at[i - 1, t],
                b_buf.at[slot, pl.ds(pl.multiple_of(place * depth, depth), depth), :], b_load_sem.at[slot, i])
            for i, place in enumerate(places)
        ]

    def send_first(m):
        return pltpu.make_async_remote_copy(
            src_ref=p_buf.at[0, rows_of(m)], dst_ref=r_got.at[0, rows_of(m)],
            send_sem=first_send.at[m], recv_sem=first_recv.at[m], device_id=partner, device_id_type=MESH)

    def send_block(s):
        return pltpu.make_async_remote_copy(
            src_ref=p_buf.at[lax.rem(s, SLOTS)], dst_ref=r_got.at[s],
            send_sem=p_send.at[lax.rem(s, SLOTS)], recv_sem=r_recv.at[lax.rem(s, RING)], device_id=partner, device_id_type=MESH)

    slab, rest = pl.ds(0, SLAB), pl.ds(SLAB, p_buf.shape[1] - SLAB)

    def at(c, r):
        return jnp.logical_and(core == 1, jnp.logical_and(col == c, row == r))

    def send_rest():
        return pltpu.make_async_remote_copy(
            src_ref=p_buf.at[ROUND % SLOTS, rest], dst_ref=r_got.at[ROUND, rest],
            send_sem=p_send.at[ROUND % SLOTS], recv_sem=r_recv.at[ROUND % RING], device_id=partner, device_id_type=MESH)

    def hop(i):
        sources = (p_buf.at[ROUND % SLOTS, slab], relay.at[0], relay.at[1])
        targets = (relay.at[0], relay.at[1], r_got.at[ROUND, slab])
        return pltpu.make_async_remote_copy(
            src_ref=sources[i], dst_ref=targets[i], send_sem=hop_send.at[i], recv_sem=hop_recv.at[i],
            device_id=partner if i == 1 else neighbour, device_id_type=MESH)

    def load_r(q):
        return pltpu.make_async_copy(r_got.at[q], r_buf, r_load_sem)

    def store_c(q):
        return pltpu.make_async_copy(c_buf, c_ref.at[:, cols_of(q)], c_sem)

    unit = p_buf.shape[1] // sum(PARTS)
    parts = [pl.ds(sum(PARTS[:i]) * unit, n * unit) for i, n in enumerate(PARTS)]

    def store_q_done():
        return pltpu.make_async_copy(q_buf, q_done, q_sem.at[0])

    def store_q():
        return [
            pltpu.make_async_copy(q_buf.at[part], out, q_sem.at[i])
            for i, (part, out) in enumerate(zip(parts, q_parts))
        ]

    def store_p():
        return [
            pltpu.make_async_copy(p_buf.at[last % SLOTS, part], out, last_sem.at[i])
            for i, (part, out) in enumerate(zip(parts, p_parts))
        ]

    def product(whose, m, slot):
        return jnp.dot(a_buf[whose, rows_of(m), :], b_buf[slot], preferred_element_type=jnp.float32)

    def pass_on(t):
        @pl.when(t >= RING - AHEAD)
        def _():
            send_b(0, t + AHEAD - RING).wait_send()

        @pl.when(t >= RING)
        def _():
            send_b(1, t - RING).wait_send()
            send_b(2, t - RING).wait_send()

        send_b(0, t).wait_recv()
        send_b(2, t).start()
        send_b(1, t).start()

        @pl.when(t + AHEAD < n_blocks)
        def _():
            send_b(0, t + AHEAD).start()

    def start_load_first(t):
        send_b(1, t).wait_recv()
        send_b(2, t).wait_recv()
        for copy in load_b(t, 0):
            copy.start()

    barrier = pltpu.get_barrier_semaphore()
    is_hub = jnp.logical_and(col == HUB[0], core == HUB[1])
    pl.semaphore_signal(barrier, inc=1, device_id=partner, device_id_type=MESH)

    @pl.when(jnp.logical_not(is_hub))
    def _():
        hub = {"col": HUB[0], "depth": HUB[1]}
        pl.semaphore_signal(barrier, inc=1, device_id=hub, device_id_type=MESH)
        pl.semaphore_wait(barrier, 1)

    @pl.when(is_hub)
    def _():
        pl.semaphore_wait(barrier, 4)
        for other in (neighbour, sibling, {**neighbour, **sibling}):
            pl.semaphore_signal(here_sem, inc=1, device_id=other, device_id_type=MESH)

    def start_a(tiles):
        for m in tiles:
            for h in range(2):
                send_a(m, h).start()

    early, late = range(2), range(2, TILES)
    start_a(early)

    @pl.when(jnp.logical_not(is_hub))
    def _():
        pl.semaphore_wait(here_sem, 1)

    for t in range(AHEAD):
        send_b(0, t).start()

    @pl.when(core == 0)
    def _():
        start_a(late)

    @pl.when(core == 0)
    def _():
        for h in range(2):
            own_a(h).start()

    pass_on(0)
    pass_on(1)
    start_load_first(0)

    @pl.loop(2, AHEAD)
    def _(t):
        pass_on(t)

    @pl.when(core == 1)
    def _():
        for m in early:
            for h in range(2):
                send_a(m, h).wait_send()
        for h in range(2):
            own_a(h).start()

    for h in range(2):
        own_a(h).wait()

    @pl.when(core == 1)
    def _():
        start_a(late)

    for copy in load_b(0, 0):
        copy.wait()

    @pl.loop(0, n_blocks + SLOTS)
    def _(s):
        @pl.when(s < n_blocks)
        def _():
            @pl.when(s > 0)
            def _():
                for copy in load_b(s, 0):
                    copy.wait()

            @pl.when(s == SLOTS)
            def _():
                for m in range(TILES):
                    send_first(m).wait_send()

            slab_sent = jnp.logical_and(s == ROUND + SLOTS, at(0, 1))

            @pl.when(jnp.logical_and(s > SLOTS, jnp.logical_not(slab_sent)))
            def _():
                send_block(s - SLOTS).wait_send()

            @pl.when(slab_sent)
            def _():
                send_rest().wait_send()
                hop(0).wait_send()

            @pl.loop(0, TILES)
            def _(m):
                @pl.when(s == 0)
                def _():
                    for h in range(2):
                        send_a(m, h).wait_recv()

                p_buf[lax.rem(s, SLOTS), rows_of(m), :] = product(1, m, 0)

                @pl.when(s == 0)
                def _():
                    send_first(m).start()

            @pl.when(s == last)
            def _():
                for copy in store_p():
                    copy.start()

            slab_goes = jnp.logical_and(s == ROUND, at(0, 1))

            @pl.when(jnp.logical_and(jnp.logical_and(s > 0, s < last), jnp.logical_not(slab_goes)))
            def _():
                send_block(s).start()

            @pl.when(slab_goes)
            def _():
                send_rest().start()
                hop(0).start()

            for i, place in ((1, (1, 1)), (2, (1, 0))):
                @pl.when(jnp.logical_and(s == ROUND + i, at(*place)))
                def _():
                    hop(i - 1).wait_recv()
                    hop(i).start()

            @pl.when(s + AHEAD < n_blocks)
            def _():
                pass_on(s + AHEAD)

            @pl.when(s + 1 < n_blocks)
            def _():
                start_load_first(s + 1)

        @pl.when(s >= SLOTS)
        def _():
            q = s - SLOTS

            @pl.when(q == 0)
            def _():
                for m in range(TILES):
                    send_first(m).wait_recv()

            slab_comes = jnp.logical_and(q == ROUND, at(0, 0))

            @pl.when(jnp.logical_and(jnp.logical_and(q > 0, q < last - 1), jnp.logical_not(slab_comes)))
            def _():
                send_block(q).wait_recv()

            @pl.when(slab_comes)
            def _():
                send_rest().wait_recv()
                hop(2).wait_recv()

            @pl.when(q < last - 1)
            def _():
                load_r(q).start()

            for copy in load_b(q, 1):
                copy.wait()

            @pl.when(q == last)
            def _():
                store_q_done().wait()

            @pl.loop(0, TILES)
            def _(m):
                q_buf[rows_of(m), :] = product(0, m, 1)

            @pl.when(q == last - 1)
            def _():
                store_q_done().start()

            @pl.when(q == last)
            def _():
                for copy in store_q():
                    copy.start()

            @pl.when(q + 1 < n_blocks)
            def _():
                for copy in load_b(q + 1, 1):
                    copy.start()

            @pl.when(q < last - 1)
            def _():
                load_r(q).wait()

                @pl.when(q > 0)
                def _():
                    store_c(q - 1).wait()

                @pl.loop(0, TILES)
                def _(m):
                    rows = rows_of(m)
                    c_buf[rows, :] = (q_buf[rows, :] + r_buf[rows, :]).astype(c_buf.dtype)

                store_c(q).start()

        @pl.when(s == SLOTS - 1)
        def _():
            for copy in load_b(0, 1):
                copy.start()

    @pl.loop(n_blocks - RING, n_blocks)
    def _(t):
        send_b(1, t).wait_send()
        send_b(2, t).wait_send()

        @pl.when(t >= n_blocks - RING + AHEAD)
        def _():
            send_b(0, t).wait_send()

    for i, place in ((1, (1, 1)), (2, (1, 0))):
        @pl.when(at(*place))
        def _():
            hop(i).wait_send()

    store_c(last - 2).wait()
    for copy in store_q() + store_p():
        copy.wait()
    for h in range(2):
        @pl.when(core == 0)
        def _():
            for m in early:
                send_a(m, h).wait_send()

        for m in late:
            send_a(m, h).wait_send()

    @pl.loop(n_blocks - SLOTS, last)
    def _(s):
        send_block(s).wait_send()

    send_block(last - 1).wait_recv()


def write_out(c_ref, q_ref, r_ref, out_ref, c_buf, q_buf, r_buf, o_buf, load_sem, store_sem):
    rows, done = c_buf.shape
    step = rows // PIECES

    def load(i):
        some = pl.ds(i * step, step)
        return pltpu.make_async_copy(c_ref.at[some, pl.ds(0, done)], c_buf.at[some], load_sem.at[i])

    def store(i):
        some = pl.ds(i * step, step)
        return pltpu.make_async_copy(c_buf.at[some], out_ref.at[some, pl.ds(0, done)], store_sem.at[i])

    load_q = pltpu.make_async_copy(q_ref, q_buf, load_sem.at[PIECES])
    load_r = pltpu.make_async_copy(r_ref.at[r_ref.shape[0] - 1], r_buf, load_sem.at[PIECES + 1])
    store_sum = pltpu.make_async_copy(o_buf, out_ref.at[:, pl.ds(done, o_buf.shape[1])], store_sem.at[PIECES])
    load_q.start()
    load_r.start()
    for i in range(PIECES):
        load(i).start()
    for i in range(PIECES):
        load(i).wait()
        store(i).start()
    load_q.wait()
    load_r.wait()
    o_buf[...] = (q_buf[...] + r_buf[...]).astype(o_buf.dtype)
    store_sum.start()
    for i in range(PIECES):
        store(i).wait()
    store_sum.wait()


def device_product(block, a_rows, b_rows):
    rows, _ = a_rows.shape
    depth, n_cols = b_rows.shape
    n_blocks, tile, unit = n_cols // block, rows // TILES, rows // sum(PARTS)
    last = n_blocks - 1
    anywhere = pl.BlockSpec(memory_space=pl.ANY)
    dma = pltpu.SemaphoreType.DMA
    parts = [jax.ShapeDtypeStruct((n * unit, block), jnp.float32) for n in PARTS]
    c_main, r_got, q_done, _, _, *split = pl.pallas_call(
        functools.partial(kernel, n_blocks, tile),
        out_shape=(
            jax.ShapeDtypeStruct((rows, n_cols), jnp.bfloat16),
            jax.ShapeDtypeStruct((last, rows, block), jnp.float32),
            jax.ShapeDtypeStruct((rows, block), jnp.float32),
            jax.ShapeDtypeStruct((3, n_blocks, depth, block), jnp.bfloat16),
            jax.ShapeDtypeStruct((2, SLAB, block), jnp.float32),
            *parts,
            *parts,
        ),
        in_specs=[anywhere] * 2,
        out_specs=(anywhere,) * (5 + 2 * len(PARTS)),
        scratch_shapes=[
            pltpu.VMEM((2, rows, 4 * depth), jnp.bfloat16),
            pltpu.VMEM((2, 4 * depth, block), jnp.bfloat16),
            pltpu.VMEM((SLOTS, rows, block), jnp.float32),
            pltpu.VMEM((rows, block), jnp.float32),
            pltpu.VMEM((rows, block), jnp.float32),
            pltpu.VMEM((rows, block), jnp.bfloat16),
            dma((2,)),
            dma((TILES, 2)),
            dma((TILES, 2)),
            dma((3, RING)),
            dma((3, RING)),
            dma((2, 4)),
            dma((TILES,)),
            dma((TILES,)),
            dma((SLOTS,)),
            dma((RING,)),
            dma,
            dma,
            dma((len(PARTS),)),
            dma((len(PARTS),)),
            pltpu.SemaphoreType.REGULAR,
            dma((3,)),
            dma((3,)),
        ],
        compiler_params=pltpu.CompilerParams(
            collective_id=0, has_side_effects=True, vmem_limit_bytes=66_000_000
        ),
        name="split_sum_product",
    )(a_rows, b_rows)

    p_parts, q_parts = split[: len(PARTS)], split[len(PARTS) :]
    got = []
    for part in p_parts:
        got.append(lax.ppermute(part, "row", [(0, 1), (1, 0)]))
    out = pl.pallas_call(
        write_out,
        out_shape=jax.ShapeDtypeStruct((rows, n_cols), jnp.bfloat16),
        in_specs=[anywhere] * 3,
        out_specs=anywhere,
        scratch_shapes=[
            pltpu.VMEM((rows, (last - 1) * block), jnp.bfloat16),
            pltpu.VMEM((rows, block), jnp.float32),
            pltpu.VMEM((rows, block), jnp.float32),
            pltpu.VMEM((rows, block), jnp.bfloat16),
            dma((PIECES + 2,)),
            dma((PIECES + 1,)),
        ],
        cost_estimate=pl.CostEstimate(flops=20_000_000_000, bytes_accessed=4 * rows * n_cols, transcendentals=0),
        name="write_out",
    )(c_main, q_done, r_got)
    for i, (own, part) in enumerate(zip(q_parts, got)):
        start = sum(PARTS[:i]) * unit
        out = lax.dynamic_update_slice(out, (own + part).astype(out.dtype), (start, last * block))
    return out


def solution(mesh, block=BLOCK):
    all_axes = ("depth", "row", "col")
    return jax.shard_map(
        functools.partial(device_product, block),
        mesh=mesh,
        in_specs=(P(all_axes, None), P(all_axes, None)),
        out_specs=P(all_axes, None),
        check_vma=False,
    )
```

```python
import functools

import jax
import jax.numpy as jnp
from jax import lax
from jax.experimental import pallas as pl
from jax.experimental.pallas import tpu as pltpu
from jax.sharding import PartitionSpec as P


MESH = pl.DeviceIdType.MESH
BLOCK = 512
TILES = 4
AHEAD = 4
SLOTS = 3
PARTS = (28, 3, 1)
HUB = (1, 0)
SLAB = (16, 3)
ROUND = 8
PIECES = 1
RING = 2 * (SLOTS + 1)


def kernel(
    n_blocks, tile, a_ref, b_ref, c_ref, r_got, q_done, b_got, relay, *others,
):
    p_parts, q_parts, scratch = others[: len(PARTS)], others[len(PARTS) : 2 * len(PARTS)], others[2 * len(PARTS) :]
    (
        a_buf, b_buf, p_buf, q_buf, r_buf, c_buf,
        a_own_sem, a_send, a_recv, b_send, b_recv, b_load_sem, first_send, first_recv, p_send, r_recv,
        r_load_sem, c_sem, q_sem, last_sem, here_sem, hop_send, hop_recv,
    ) = scratch
    last = n_blocks - 1
    col, row, core = lax.axis_index("col"), lax.axis_index("row"), lax.axis_index("depth")
    neighbour, partner, sibling = {"col": 1 - col}, {"row": 1 - row}, {"depth": 1 - core}
    depth, block = b_ref.shape[0], b_buf.shape[2]

    def rows_of(m):
        return pl.ds(pl.multiple_of(m * tile, tile), tile)

    def cols_of(t):
        return pl.ds(pl.multiple_of(t * block, block), block)

    def a_cols(h, r):
        return pl.ds(pl.multiple_of((h * 4 + r * 2) * depth, depth), 2 * depth)

    def a_half(h):
        return pl.ds(h * 2 * depth, 2 * depth)

    def own_a(h):
        return pltpu.make_async_copy(a_ref.at[:, a_cols(h, row)], a_buf.at[0, :, a_half(h)], a_own_sem.at[h])

    def send_a(m, h):
        return pltpu.make_async_remote_copy(
            src_ref=a_ref.at[rows_of(m), a_cols(h, 1 - row)], dst_ref=a_buf.at[1, rows_of(m), a_half(h)],
            send_sem=a_send.at[m, h], recv_sem=a_recv.at[m, h], device_id=partner, device_id_type=MESH)

    def send_b(way, t):
        return pltpu.make_async_remote_copy(
            src_ref=b_got.at[0, t] if way == 2 else b_ref.at[:, cols_of(t)], dst_ref=b_got.at[way, t],
            send_sem=b_send.at[way, lax.rem(t, RING)], recv_sem=b_recv.at[way, lax.rem(t, RING)],
            device_id=neighbour if way == 0 else sibling, device_id_type=MESH)

    def load_b(t, slot):
        places = (core * 2 + col, core * 2 + 1 - col, (1 - core) * 2 + col, (1 - core) * 2 + 1 - col)
        return [
            pltpu.make_async_copy(
                b_ref.at[:, cols_of(t)] if i == 0 else b_got.at[i - 1, t],
                b_buf.at[slot, pl.ds(pl.multiple_of(place * depth, depth), depth), :], b_load_sem.at[slot, i])
            for i, place in enumerate(places)
        ]

    def send_first(m):
        return pltpu.make_async_remote_copy(
            src_ref=p_buf.at[0, rows_of(m)], dst_ref=r_got.at[0, rows_of(m)],
            send_sem=first_send.at[m], recv_sem=first_recv.at[m], device_id=partner, device_id_type=MESH)

    def send_block(s):
        return pltpu.make_async_remote_copy(
            src_ref=p_buf.at[lax.rem(s, SLOTS)], dst_ref=r_got.at[s],
            send_sem=p_send.at[lax.rem(s, SLOTS)], recv_sem=r_recv.at[lax.rem(s, RING)], device_id=partner, device_id_type=MESH)

    slab, rest = pl.ds(0, SLAB[0]), pl.ds(SLAB[0], p_buf.shape[1] - SLAB[0])
    wide = SLAB[1] * block // 4
    side, corner = pl.ds(0, wide), pl.ds(wide, block - wide)

    def at(c, r):
        return jnp.logical_and(core == 1, jnp.logical_and(col == c, row == r))

    def send_rest():
        return [
            pltpu.make_async_remote_copy(
                src_ref=p_buf.at[ROUND % SLOTS, *part], dst_ref=r_got.at[ROUND, *part],
                send_sem=send, recv_sem=recv, device_id=partner, device_id_type=MESH)
            for part, send, recv in (
                ((rest, slice(None)), p_send.at[ROUND % SLOTS], r_recv.at[ROUND % RING]),
                ((slab, corner), hop_send.at[3], hop_recv.at[3]),
            )
        ]

    def hop(i):
        sources = (p_buf.at[ROUND % SLOTS, slab, side], relay.at[0], relay.at[1])
        targets = (relay.at[0], relay.at[1], r_got.at[ROUND, slab, side])
        return pltpu.make_async_remote_copy(
            src_ref=sources[i], dst_ref=targets[i], send_sem=hop_send.at[i], recv_sem=hop_recv.at[i],
            device_id=partner if i == 1 else neighbour, device_id_type=MESH)

    def load_r(q):
        return pltpu.make_async_copy(r_got.at[q], r_buf, r_load_sem)

    def store_c(q):
        return pltpu.make_async_copy(c_buf, c_ref.at[:, cols_of(q)], c_sem)

    unit = p_buf.shape[1] // sum(PARTS)
    parts = [pl.ds(sum(PARTS[:i]) * unit, n * unit) for i, n in enumerate(PARTS)]

    def store_q_done():
        return pltpu.make_async_copy(q_buf, q_done, q_sem.at[0])

    def store_q():
        return [
            pltpu.make_async_copy(q_buf.at[part], out, q_sem.at[i])
            for i, (part, out) in enumerate(zip(parts, q_parts))
        ]

    def store_p():
        return [
            pltpu.make_async_copy(p_buf.at[last % SLOTS, part], out, last_sem.at[i])
            for i, (part, out) in enumerate(zip(parts, p_parts))
        ]

    def product(whose, m, slot):
        return jnp.dot(a_buf[whose, rows_of(m), :], b_buf[slot], preferred_element_type=jnp.float32)

    def pass_on(t):
        @pl.when(t >= RING - AHEAD)
        def _():
            send_b(0, t + AHEAD - RING).wait_send()

        @pl.when(t >= RING)
        def _():
            send_b(1, t - RING).wait_send()
            send_b(2, t - RING).wait_send()

        send_b(0, t).wait_recv()
        send_b(2, t).start()
        send_b(1, t).start()

        @pl.when(t + AHEAD < n_blocks)
        def _():
            send_b(0, t + AHEAD).start()

    def start_load_first(t):
        send_b(1, t).wait_recv()
        send_b(2, t).wait_recv()
        for copy in load_b(t, 0):
            copy.start()

    barrier = pltpu.get_barrier_semaphore()
    is_hub = jnp.logical_and(col == HUB[0], core == HUB[1])
    pl.semaphore_signal(barrier, inc=1, device_id=partner, device_id_type=MESH)

    @pl.when(jnp.logical_not(is_hub))
    def _():
        hub = {"col": HUB[0], "depth": HUB[1]}
        pl.semaphore_signal(barrier, inc=1, device_id=hub, device_id_type=MESH)
        pl.semaphore_wait(barrier, 1)

    @pl.when(is_hub)
    def _():
        pl.semaphore_wait(barrier, 4)
        for other in (neighbour, sibling, {**neighbour, **sibling}):
            pl.semaphore_signal(here_sem, inc=1, device_id=other, device_id_type=MESH)

    def start_a(tiles):
        for m in tiles:
            for h in range(2):
                send_a(m, h).start()

    early, late = range(2), range(2, TILES)
    start_a(early)

    @pl.when(jnp.logical_not(is_hub))
    def _():
        pl.semaphore_wait(here_sem, 1)

    for t in range(AHEAD):
        send_b(0, t).start()

    @pl.when(core == 0)
    def _():
        start_a(late)

    for h in range(2):
        own_a(h).start()
    pass_on(0)
    pass_on(1)
    start_load_first(0)

    @pl.loop(2, AHEAD)
    def _(t):
        pass_on(t)

    for h in range(2):
        own_a(h).wait()
    for copy in load_b(0, 0):
        copy.wait()

    @pl.loop(0, n_blocks + SLOTS)
    def _(s):
        @pl.when(s < n_blocks)
        def _():
            @pl.when(s > 0)
            def _():
                for copy in load_b(s, 0):
                    copy.wait()

            @pl.when(s == SLOTS)
            def _():
                for m in range(TILES):
                    send_first(m).wait_send()

            slab_sent = jnp.logical_and(s == ROUND + SLOTS, at(0, 1))

            @pl.when(jnp.logical_and(s > SLOTS, jnp.logical_not(slab_sent)))
            def _():
                send_block(s - SLOTS).wait_send()

            @pl.when(slab_sent)
            def _():
                for copy in (*send_rest(), hop(0)):
                    copy.wait_send()

            @pl.loop(0, TILES)
            def _(m):
                @pl.when(s == 0)
                def _():
                    for h in range(2):
                        send_a(m, h).wait_recv()

                p_buf[lax.rem(s, SLOTS), rows_of(m), :] = product(1, m, 0)

                held = jnp.logical_and(core == 1, m < len(early))

                @pl.when(jnp.logical_and(s == 0, jnp.logical_not(held)))
                def _():
                    send_first(m).start()

                @pl.when(jnp.logical_and(jnp.logical_and(s == 0, core == 1), m == len(early) - 1))
                def _():
                    start_a(late)
                    for first in early:
                        send_first(first).start()

            @pl.when(s == last)
            def _():
                for copy in store_p():
                    copy.start()

            slab_goes = jnp.logical_and(s == ROUND, at(0, 1))

            @pl.when(jnp.logical_and(jnp.logical_and(s > 0, s < last), jnp.logical_not(slab_goes)))
            def _():
                send_block(s).start()

            @pl.when(slab_goes)
            def _():
                for copy in (*send_rest(), hop(0)):
                    copy.start()

            for i, place in ((1, (1, 1)), (2, (1, 0))):
                @pl.when(jnp.logical_and(s == ROUND + i, at(*place)))
                def _():
                    hop(i - 1).wait_recv()
                    hop(i).start()

            @pl.when(s + AHEAD < n_blocks)
            def _():
                pass_on(s + AHEAD)

            @pl.when(s + 1 < n_blocks)
            def _():
                start_load_first(s + 1)

        @pl.when(s >= SLOTS)
        def _():
            q = s - SLOTS

            @pl.when(q == 0)
            def _():
                for m in range(TILES):
                    send_first(m).wait_recv()

            slab_comes = jnp.logical_and(q == ROUND, at(0, 0))

            @pl.when(jnp.logical_and(jnp.logical_and(q > 0, q < last - 1), jnp.logical_not(slab_comes)))
            def _():
                send_block(q).wait_recv()

            @pl.when(slab_comes)
            def _():
                for copy in (*send_rest(), hop(2)):
                    copy.wait_recv()

            @pl.when(q < last - 1)
            def _():
                load_r(q).start()

            for copy in load_b(q, 1):
                copy.wait()

            @pl.when(q == last)
            def _():
                store_q_done().wait()

            @pl.loop(0, TILES)
            def _(m):
                q_buf[rows_of(m), :] = product(0, m, 1)

            @pl.when(q == last - 1)
            def _():
                store_q_done().start()

            @pl.when(q == last)
            def _():
                for copy in store_q():
                    copy.start()

            @pl.when(q + 1 < n_blocks)
            def _():
                for copy in load_b(q + 1, 1):
                    copy.start()

            @pl.when(q < last - 1)
            def _():
                load_r(q).wait()

                @pl.when(q > 0)
                def _():
                    store_c(q - 1).wait()

                @pl.loop(0, TILES)
                def _(m):
                    rows = rows_of(m)
                    c_buf[rows, :] = (q_buf[rows, :] + r_buf[rows, :]).astype(c_buf.dtype)

                store_c(q).start()

        @pl.when(s == SLOTS - 1)
        def _():
            for copy in load_b(0, 1):
                copy.start()

    @pl.loop(n_blocks - RING, n_blocks)
    def _(t):
        send_b(1, t).wait_send()
        send_b(2, t).wait_send()

        @pl.when(t >= n_blocks - RING + AHEAD)
        def _():
            send_b(0, t).wait_send()

    for i, place in ((1, (1, 1)), (2, (1, 0))):
        @pl.when(at(*place))
        def _():
            hop(i).wait_send()

    store_c(last - 2).wait()
    for copy in store_q() + store_p():
        copy.wait()
    for m in range(TILES):
        for h in range(2):
            send_a(m, h).wait_send()

    @pl.loop(n_blocks - SLOTS, last)
    def _(s):
        send_block(s).wait_send()

    send_block(last - 1).wait_recv()


def write_out(c_ref, q_ref, r_ref, out_ref, c_buf, q_buf, r_buf, o_buf, load_sem, store_sem):
    rows, done = c_buf.shape
    step = rows // PIECES

    def load(i):
        some = pl.ds(i * step, step)
        return pltpu.make_async_copy(c_ref.at[some, pl.ds(0, done)], c_buf.at[some], load_sem.at[i])

    def store(i):
        some = pl.ds(i * step, step)
        return pltpu.make_async_copy(c_buf.at[some], out_ref.at[some, pl.ds(0, done)], store_sem.at[i])

    load_q = pltpu.make_async_copy(q_ref, q_buf, load_sem.at[PIECES])
    load_r = pltpu.make_async_copy(r_ref.at[r_ref.shape[0] - 1], r_buf, load_sem.at[PIECES + 1])
    store_sum = pltpu.make_async_copy(o_buf, out_ref.at[:, pl.ds(done, o_buf.shape[1])], store_sem.at[PIECES])
    load_q.start()
    load_r.start()
    for i in range(PIECES):
        load(i).start()
    for i in range(PIECES):
        load(i).wait()
        store(i).start()
    load_q.wait()
    load_r.wait()
    o_buf[...] = (q_buf[...] + r_buf[...]).astype(o_buf.dtype)
    store_sum.start()
    for i in range(PIECES):
        store(i).wait()
    store_sum.wait()


def device_product(block, a_rows, b_rows):
    rows, _ = a_rows.shape
    depth, n_cols = b_rows.shape
    n_blocks, tile, unit = n_cols // block, rows // TILES, rows // sum(PARTS)
    last = n_blocks - 1
    anywhere = pl.BlockSpec(memory_space=pl.ANY)
    dma = pltpu.SemaphoreType.DMA
    parts = [jax.ShapeDtypeStruct((n * unit, block), jnp.float32) for n in PARTS]
    c_main, r_got, q_done, _, _, *split = pl.pallas_call(
        functools.partial(kernel, n_blocks, tile),
        out_shape=(
            jax.ShapeDtypeStruct((rows, n_cols), jnp.bfloat16),
            jax.ShapeDtypeStruct((last, rows, block), jnp.float32),
            jax.ShapeDtypeStruct((rows, block), jnp.float32),
            jax.ShapeDtypeStruct((3, n_blocks, depth, block), jnp.bfloat16),
            jax.ShapeDtypeStruct((2, SLAB[0], SLAB[1] * block // 4), jnp.float32),
            *parts,
            *parts,
        ),
        in_specs=[anywhere] * 2,
        out_specs=(anywhere,) * (5 + 2 * len(PARTS)),
        scratch_shapes=[
            pltpu.VMEM((2, rows, 4 * depth), jnp.bfloat16),
            pltpu.VMEM((2, 4 * depth, block), jnp.bfloat16),
            pltpu.VMEM((SLOTS, rows, block), jnp.float32),
            pltpu.VMEM((rows, block), jnp.float32),
            pltpu.VMEM((rows, block), jnp.float32),
            pltpu.VMEM((rows, block), jnp.bfloat16),
            dma((2,)),
            dma((TILES, 2)),
            dma((TILES, 2)),
            dma((3, RING)),
            dma((3, RING)),
            dma((2, 4)),
            dma((TILES,)),
            dma((TILES,)),
            dma((SLOTS,)),
            dma((RING,)),
            dma,
            dma,
            dma((len(PARTS),)),
            dma((len(PARTS),)),
            pltpu.SemaphoreType.REGULAR,
            dma((4,)),
            dma((4,)),
        ],
        compiler_params=pltpu.CompilerParams(
            collective_id=0, has_side_effects=True, vmem_limit_bytes=66_000_000
        ),
        name="split_sum_product",
    )(a_rows, b_rows)

    p_parts, q_parts = split[: len(PARTS)], split[len(PARTS) :]
    got = []
    for part in p_parts:
        got.append(lax.ppermute(part, "row", [(0, 1), (1, 0)]))
    out = pl.pallas_call(
        write_out,
        out_shape=jax.ShapeDtypeStruct((rows, n_cols), jnp.bfloat16),
        in_specs=[anywhere] * 3,
        out_specs=anywhere,
        scratch_shapes=[
            pltpu.VMEM((rows, (last - 1) * block), jnp.bfloat16),
            pltpu.VMEM((rows, block), jnp.float32),
            pltpu.VMEM((rows, block), jnp.float32),
            pltpu.VMEM((rows, block), jnp.bfloat16),
            dma((PIECES + 2,)),
            dma((PIECES + 1,)),
        ],
        compiler_params=pltpu.CompilerParams(vmem_limit_bytes=50_000_000),
        cost_estimate=pl.CostEstimate(flops=20_000_000_000, bytes_accessed=4 * rows * n_cols, transcendentals=0),
        name="write_out",
    )(c_main, q_done, r_got)
    for i, (own, part) in enumerate(zip(q_parts, got)):
        start = sum(PARTS[:i]) * unit
        out = lax.dynamic_update_slice(out, (own + part).astype(out.dtype), (start, last * block))
    return out


def solution(mesh, block=BLOCK):
    all_axes = ("depth", "row", "col")
    return jax.shard_map(
        functools.partial(device_product, block),
        mesh=mesh,
        in_specs=(P(all_axes, None), P(all_axes, None)),
        out_specs=P(all_axes, None),
        check_vma=False,
    )
```

```python
import functools

import jax
import jax.numpy as jnp
from jax import lax
from jax.experimental import pallas as pl
from jax.experimental.pallas import tpu as pltpu
from jax.sharding import PartitionSpec as P


MESH = pl.DeviceIdType.MESH
BLOCK = 512
TILES = 4
AHEAD = 4
SLOTS = 3
PARTS = (28, 3, 1)
HUB = (1, 0)
SLAB = (16, 3)
ROUND = 8
PIECES = 1
RING = 2 * (SLOTS + 1)


def kernel(
    n_blocks, tile, a_ref, b_ref, c_ref, r_got, q_done, b_got, relay, *others,
):
    p_parts, q_parts, scratch = others[: len(PARTS)], others[len(PARTS) : 2 * len(PARTS)], others[2 * len(PARTS) :]
    (
        a_buf, b_buf, p_buf, q_buf, r_buf, c_buf,
        a_own_sem, a_send, a_recv, b_send, b_recv, b_load_sem, first_send, first_recv, p_send, r_recv,
        r_load_sem, c_sem, q_sem, last_sem, here_sem, hop_send, hop_recv,
    ) = scratch
    last = n_blocks - 1
    col, row, core = lax.axis_index("col"), lax.axis_index("row"), lax.axis_index("depth")
    neighbour, partner, sibling = {"col": 1 - col}, {"row": 1 - row}, {"depth": 1 - core}
    depth, block = b_ref.shape[0], b_buf.shape[2]

    def rows_of(m):
        return pl.ds(pl.multiple_of(m * tile, tile), tile)

    def cols_of(t):
        return pl.ds(pl.multiple_of(t * block, block), block)

    def a_cols(h, r):
        return pl.ds(pl.multiple_of((h * 4 + r * 2) * depth, depth), 2 * depth)

    def a_half(h):
        return pl.ds(h * 2 * depth, 2 * depth)

    def own_a(h):
        return pltpu.make_async_copy(a_ref.at[:, a_cols(h, row)], a_buf.at[0, :, a_half(h)], a_own_sem.at[h])

    def send_a(m, h):
        return pltpu.make_async_remote_copy(
            src_ref=a_ref.at[rows_of(m), a_cols(h, 1 - row)], dst_ref=a_buf.at[1, rows_of(m), a_half(h)],
            send_sem=a_send.at[m, h], recv_sem=a_recv.at[m, h], device_id=partner, device_id_type=MESH)

    def send_b(way, t):
        return pltpu.make_async_remote_copy(
            src_ref=b_got.at[0, t] if way == 2 else b_ref.at[:, cols_of(t)], dst_ref=b_got.at[way, t],
            send_sem=b_send.at[way, lax.rem(t, RING)], recv_sem=b_recv.at[way, lax.rem(t, RING)],
            device_id=neighbour if way == 0 else sibling, device_id_type=MESH)

    def load_b(t, slot):
        places = (core * 2 + col, core * 2 + 1 - col, (1 - core) * 2 + col, (1 - core) * 2 + 1 - col)
        return [
            pltpu.make_async_copy(
                b_ref.at[:, cols_of(t)] if i == 0 else b_got.at[i - 1, t],
                b_buf.at[slot, pl.ds(pl.multiple_of(place * depth, depth), depth), :], b_load_sem.at[slot, i])
            for i, place in enumerate(places)
        ]

    def send_first(m):
        return pltpu.make_async_remote_copy(
            src_ref=p_buf.at[0, rows_of(m)], dst_ref=r_got.at[0, rows_of(m)],
            send_sem=first_send.at[m], recv_sem=first_recv.at[m], device_id=partner, device_id_type=MESH)

    def send_block(s):
        return pltpu.make_async_remote_copy(
            src_ref=p_buf.at[lax.rem(s, SLOTS)], dst_ref=r_got.at[s],
            send_sem=p_send.at[lax.rem(s, SLOTS)], recv_sem=r_recv.at[lax.rem(s, RING)], device_id=partner, device_id_type=MESH)

    slab, rest = pl.ds(0, SLAB[0]), pl.ds(SLAB[0], p_buf.shape[1] - SLAB[0])
    wide = SLAB[1] * block // 4
    side, corner = pl.ds(0, wide), pl.ds(wide, block - wide)

    def at(c, r):
        return jnp.logical_and(core == 1, jnp.logical_and(col == c, row == r))

    def send_rest():
        return [
            pltpu.make_async_remote_copy(
                src_ref=p_buf.at[ROUND % SLOTS, *part], dst_ref=r_got.at[ROUND, *part],
                send_sem=send, recv_sem=recv, device_id=partner, device_id_type=MESH)
            for part, send, recv in (
                ((rest, slice(None)), p_send.at[ROUND % SLOTS], r_recv.at[ROUND % RING]),
                ((slab, corner), hop_send.at[3], hop_recv.at[3]),
            )
        ]

    def hop(i):
        sources = (p_buf.at[ROUND % SLOTS, slab, side], relay.at[0], relay.at[1])
        targets = (relay.at[0], relay.at[1], r_got.at[ROUND, slab, side])
        return pltpu.make_async_remote_copy(
            src_ref=sources[i], dst_ref=targets[i], send_sem=hop_send.at[i], recv_sem=hop_recv.at[i],
            device_id=partner if i == 1 else neighbour, device_id_type=MESH)

    def load_r(q):
        return pltpu.make_async_copy(r_got.at[q], r_buf, r_load_sem)

    def store_c(q):
        return pltpu.make_async_copy(c_buf, c_ref.at[:, cols_of(q)], c_sem)

    unit = p_buf.shape[1] // sum(PARTS)
    parts = [pl.ds(sum(PARTS[:i]) * unit, n * unit) for i, n in enumerate(PARTS)]

    def store_q_done():
        return pltpu.make_async_copy(q_buf, q_done, q_sem.at[0])

    def store_q():
        return [
            pltpu.make_async_copy(q_buf.at[part], out, q_sem.at[i])
            for i, (part, out) in enumerate(zip(parts, q_parts))
        ]

    def store_p():
        return [
            pltpu.make_async_copy(p_buf.at[last % SLOTS, part], out, last_sem.at[i])
            for i, (part, out) in enumerate(zip(parts, p_parts))
        ]

    def product(whose, m, slot):
        return jnp.dot(a_buf[whose, rows_of(m), :], b_buf[slot], preferred_element_type=jnp.float32)

    def pass_on(t):
        @pl.when(t >= RING - AHEAD)
        def _():
            send_b(0, t + AHEAD - RING).wait_send()

        @pl.when(t >= RING)
        def _():
            send_b(1, t - RING).wait_send()
            send_b(2, t - RING).wait_send()

        send_b(0, t).wait_recv()
        send_b(2, t).start()
        send_b(1, t).start()

        @pl.when(t + AHEAD < n_blocks)
        def _():
            send_b(0, t + AHEAD).start()

    def start_load_first(t, slot):
        send_b(1, t).wait_recv()
        send_b(2, t).wait_recv()
        for copy in load_b(t, slot):
            copy.start()

    barrier = pltpu.get_barrier_semaphore()
    is_hub = jnp.logical_and(col == HUB[0], core == HUB[1])
    pl.semaphore_signal(barrier, inc=1, device_id=partner, device_id_type=MESH)

    @pl.when(jnp.logical_not(is_hub))
    def _():
        hub = {"col": HUB[0], "depth": HUB[1]}
        pl.semaphore_signal(barrier, inc=1, device_id=hub, device_id_type=MESH)
        pl.semaphore_wait(barrier, 1)

    @pl.when(is_hub)
    def _():
        pl.semaphore_wait(barrier, 4)
        for other in (neighbour, sibling, {**neighbour, **sibling}):
            pl.semaphore_signal(here_sem, inc=1, device_id=other, device_id_type=MESH)

    def start_a(tiles):
        for m in tiles:
            for h in range(2):
                send_a(m, h).start()

    early, late = range(2), range(2, TILES)
    start_a(early)

    @pl.when(jnp.logical_not(is_hub))
    def _():
        pl.semaphore_wait(here_sem, 1)

    for t in range(AHEAD):
        send_b(0, t).start()

    @pl.when(core == 0)
    def _():
        start_a(late)

    for h in range(2):
        own_a(h).start()
    pass_on(0)
    pass_on(1)
    start_load_first(0, 0)

    @pl.loop(2, AHEAD)
    def _(t):
        pass_on(t)

    for h in range(2):
        own_a(h).wait()
    start_load_first(1, 1)
    for copy in load_b(0, 0):
        copy.wait()

    @pl.loop(0, n_blocks + SLOTS)
    def _(s):
        @pl.when(s < n_blocks)
        def _():
            @pl.when(s == SLOTS)
            def _():
                for m in range(TILES):
                    send_first(m).wait_send()

            slab_sent = jnp.logical_and(s == ROUND + SLOTS, at(0, 1))

            @pl.when(jnp.logical_and(s > SLOTS, jnp.logical_not(slab_sent)))
            def _():
                send_block(s - SLOTS).wait_send()

            @pl.when(slab_sent)
            def _():
                for copy in (*send_rest(), hop(0)):
                    copy.wait_send()

            @pl.when(s == 1)
            def _():
                for copy in load_b(1, 1):
                    copy.wait()

            @pl.when(s > 1)
            def _():
                for copy in load_b(s, 0):
                    copy.wait()

            slot = jnp.where(s == 1, 1, 0)

            @pl.loop(0, TILES)
            def _(m):
                @pl.when(s == 0)
                def _():
                    for h in range(2):
                        send_a(m, h).wait_recv()

                p_buf[lax.rem(s, SLOTS), rows_of(m), :] = product(1, m, slot)

                held = jnp.logical_and(core == 1, m < len(early))

                @pl.when(jnp.logical_and(s == 0, jnp.logical_not(held)))
                def _():
                    send_first(m).start()

                @pl.when(jnp.logical_and(jnp.logical_and(s == 0, core == 1), m == len(early) - 1))
                def _():
                    start_a(late)
                    for first in early:
                        send_first(first).start()

            @pl.when(s == last)
            def _():
                for copy in store_p():
                    copy.start()

            slab_goes = jnp.logical_and(s == ROUND, at(0, 1))

            @pl.when(jnp.logical_and(jnp.logical_and(s > 0, s < last), jnp.logical_not(slab_goes)))
            def _():
                send_block(s).start()

            @pl.when(slab_goes)
            def _():
                for copy in (*send_rest(), hop(0)):
                    copy.start()

            for i, place in ((1, (1, 1)), (2, (1, 0))):
                @pl.when(jnp.logical_and(s == ROUND + i, at(*place)))
                def _():
                    hop(i - 1).wait_recv()
                    hop(i).start()

            @pl.when(s + AHEAD < n_blocks)
            def _():
                pass_on(s + AHEAD)

            @pl.when(s == 0)
            def _():
                start_load_first(2, 0)

            @pl.when(jnp.logical_and(s > 1, s + 1 < n_blocks))
            def _():
                start_load_first(s + 1, 0)

        @pl.when(s >= SLOTS)
        def _():
            q = s - SLOTS

            @pl.when(q == 0)
            def _():
                for m in range(TILES):
                    send_first(m).wait_recv()

            slab_comes = jnp.logical_and(q == ROUND, at(0, 0))

            @pl.when(jnp.logical_and(jnp.logical_and(q > 0, q < last - 1), jnp.logical_not(slab_comes)))
            def _():
                send_block(q).wait_recv()

            @pl.when(slab_comes)
            def _():
                for copy in (*send_rest(), hop(2)):
                    copy.wait_recv()

            @pl.when(q < last - 1)
            def _():
                load_r(q).start()

            for copy in load_b(q, 1):
                copy.wait()

            @pl.when(q == last)
            def _():
                store_q_done().wait()

            @pl.loop(0, TILES)
            def _(m):
                q_buf[rows_of(m), :] = product(0, m, 1)

            @pl.when(q == last - 1)
            def _():
                store_q_done().start()

            @pl.when(q == last)
            def _():
                for copy in store_q():
                    copy.start()

            @pl.when(q + 1 < n_blocks)
            def _():
                for copy in load_b(q + 1, 1):
                    copy.start()

            @pl.when(q < last - 1)
            def _():
                load_r(q).wait()

                @pl.when(q > 0)
                def _():
                    store_c(q - 1).wait()

                @pl.loop(0, TILES)
                def _(m):
                    rows = rows_of(m)
                    c_buf[rows, :] = (q_buf[rows, :] + r_buf[rows, :]).astype(c_buf.dtype)

                store_c(q).start()

        @pl.when(s == SLOTS - 1)
        def _():
            for copy in load_b(0, 1):
                copy.start()

    @pl.loop(n_blocks - RING, n_blocks)
    def _(t):
        send_b(1, t).wait_send()
        send_b(2, t).wait_send()

        @pl.when(t >= n_blocks - RING + AHEAD)
        def _():
            send_b(0, t).wait_send()

    for i, place in ((1, (1, 1)), (2, (1, 0))):
        @pl.when(at(*place))
        def _():
            hop(i).wait_send()

    store_c(last - 2).wait()
    for copy in store_q() + store_p():
        copy.wait()
    for m in range(TILES):
        for h in range(2):
            send_a(m, h).wait_send()

    @pl.loop(n_blocks - SLOTS, last)
    def _(s):
        send_block(s).wait_send()

    send_block(last - 1).wait_recv()


def write_out(c_ref, q_ref, r_ref, out_ref, c_buf, q_buf, r_buf, o_buf, load_sem, store_sem):
    rows, done = c_buf.shape
    step = rows // PIECES

    def load(i):
        some = pl.ds(i * step, step)
        return pltpu.make_async_copy(c_ref.at[some, pl.ds(0, done)], c_buf.at[some], load_sem.at[i])

    def store(i):
        some = pl.ds(i * step, step)
        return pltpu.make_async_copy(c_buf.at[some], out_ref.at[some, pl.ds(0, done)], store_sem.at[i])

    load_q = pltpu.make_async_copy(q_ref, q_buf, load_sem.at[PIECES])
    load_r = pltpu.make_async_copy(r_ref.at[r_ref.shape[0] - 1], r_buf, load_sem.at[PIECES + 1])
    store_sum = pltpu.make_async_copy(o_buf, out_ref.at[:, pl.ds(done, o_buf.shape[1])], store_sem.at[PIECES])
    load_q.start()
    load_r.start()
    for i in range(PIECES):
        load(i).start()
    for i in range(PIECES):
        load(i).wait()
        store(i).start()
    load_q.wait()
    load_r.wait()
    o_buf[...] = (q_buf[...] + r_buf[...]).astype(o_buf.dtype)
    store_sum.start()
    for i in range(PIECES):
        store(i).wait()
    store_sum.wait()


def device_product(block, a_rows, b_rows):
    rows, _ = a_rows.shape
    depth, n_cols = b_rows.shape
    n_blocks, tile, unit = n_cols // block, rows // TILES, rows // sum(PARTS)
    last = n_blocks - 1
    anywhere = pl.BlockSpec(memory_space=pl.ANY)
    dma = pltpu.SemaphoreType.DMA
    parts = [jax.ShapeDtypeStruct((n * unit, block), jnp.float32) for n in PARTS]
    c_main, r_got, q_done, _, _, *split = pl.pallas_call(
        functools.partial(kernel, n_blocks, tile),
        out_shape=(
            jax.ShapeDtypeStruct((rows, n_cols), jnp.bfloat16),
            jax.ShapeDtypeStruct((last, rows, block), jnp.float32),
            jax.ShapeDtypeStruct((rows, block), jnp.float32),
            jax.ShapeDtypeStruct((3, n_blocks, depth, block), jnp.bfloat16),
            jax.ShapeDtypeStruct((2, SLAB[0], SLAB[1] * block // 4), jnp.float32),
            *parts,
            *parts,
        ),
        in_specs=[anywhere] * 2,
        out_specs=(anywhere,) * (5 + 2 * len(PARTS)),
        scratch_shapes=[
            pltpu.VMEM((2, rows, 4 * depth), jnp.bfloat16),
            pltpu.VMEM((2, 4 * depth, block), jnp.bfloat16),
            pltpu.VMEM((SLOTS, rows, block), jnp.float32),
            pltpu.VMEM((rows, block), jnp.float32),
            pltpu.VMEM((rows, block), jnp.float32),
            pltpu.VMEM((rows, block), jnp.bfloat16),
            dma((2,)),
            dma((TILES, 2)),
            dma((TILES, 2)),
            dma((3, RING)),
            dma((3, RING)),
            dma((2, 4)),
            dma((TILES,)),
            dma((TILES,)),
            dma((SLOTS,)),
            dma((RING,)),
            dma,
            dma,
            dma((len(PARTS),)),
            dma((len(PARTS),)),
            pltpu.SemaphoreType.REGULAR,
            dma((4,)),
            dma((4,)),
        ],
        compiler_params=pltpu.CompilerParams(
            collective_id=0, has_side_effects=True, vmem_limit_bytes=66_000_000
        ),
        name="split_sum_product",
    )(a_rows, b_rows)

    p_parts, q_parts = split[: len(PARTS)], split[len(PARTS) :]
    got = []
    for part in p_parts:
        got.append(lax.ppermute(part, "row", [(0, 1), (1, 0)]))
    out = pl.pallas_call(
        write_out,
        out_shape=jax.ShapeDtypeStruct((rows, n_cols), jnp.bfloat16),
        in_specs=[anywhere] * 3,
        out_specs=anywhere,
        scratch_shapes=[
            pltpu.VMEM((rows, (last - 1) * block), jnp.bfloat16),
            pltpu.VMEM((rows, block), jnp.float32),
            pltpu.VMEM((rows, block), jnp.float32),
            pltpu.VMEM((rows, block), jnp.bfloat16),
            dma((PIECES + 2,)),
            dma((PIECES + 1,)),
        ],
        compiler_params=pltpu.CompilerParams(vmem_limit_bytes=50_000_000),
        cost_estimate=pl.CostEstimate(flops=20_000_000_000, bytes_accessed=4 * rows * n_cols, transcendentals=0),
        name="write_out",
    )(c_main, q_done, r_got)
    for i, (own, part) in enumerate(zip(q_parts, got)):
        start = sum(PARTS[:i]) * unit
        out = lax.dynamic_update_slice(out, (own + part).astype(out.dtype), (start, last * block))
    return out


def solution(mesh, block=BLOCK):
    all_axes = ("depth", "row", "col")
    return jax.shard_map(
        functools.partial(device_product, block),
        mesh=mesh,
        in_specs=(P(all_axes, None), P(all_axes, None)),
        out_specs=P(all_axes, None),
        check_vma=False,
    )
```

```python
import functools

import jax
import jax.numpy as jnp
from jax import lax
from jax.experimental import pallas as pl
from jax.experimental.pallas import tpu as pltpu
from jax.sharding import PartitionSpec as P


MESH = pl.DeviceIdType.MESH
BLOCK = 512
TILES = 4
AHEAD = 4
SLOTS = 3
PARTS = (1, 20, 20, 15, 6, 2)
HUB = (1, 0)
SLAB = (16, 3)
ROUND = 8
PIECES = 1
RING = 2 * (SLOTS + 1)


def rectangles(rows, columns):
    unit, half = rows // sum(PARTS), columns // 2
    starts = [sum(PARTS[:i]) * unit for i in range(len(PARTS))]
    whole = [(start, 0, n * unit, columns) for start, n in zip(starts, PARTS)]
    return [(0, 0, PARTS[0] * unit, half), (0, half, PARTS[0] * unit, half), *whole[1:]]


def kernel(
    n_blocks, tile, a_ref, b_ref, c_ref, r_got, q_done, b_got, relay, *others,
):
    n_parts = len(PARTS) + 1
    p_parts, q_parts, scratch = others[:n_parts], others[n_parts : 2 * n_parts], others[2 * n_parts :]
    (
        a_buf, b_buf, p_buf, q_buf, r_buf, c_buf,
        a_own_sem, a_send, a_recv, b_send, b_recv, b_load_sem, first_send, first_recv, p_send, r_recv,
        r_load_sem, c_sem, q_sem, last_sem, here_sem, hop_send, hop_recv,
    ) = scratch
    last = n_blocks - 1
    col, row, core = lax.axis_index("col"), lax.axis_index("row"), lax.axis_index("depth")
    neighbour, partner, sibling = {"col": 1 - col}, {"row": 1 - row}, {"depth": 1 - core}
    depth, block = b_ref.shape[0], b_buf.shape[2]

    def rows_of(m):
        return pl.ds(pl.multiple_of(m * tile, tile), tile)

    def cols_of(t):
        return pl.ds(pl.multiple_of(t * block, block), block)

    def a_cols(h, r):
        return pl.ds(pl.multiple_of((h * 4 + r * 2) * depth, depth), 2 * depth)

    def a_half(h):
        return pl.ds(h * 2 * depth, 2 * depth)

    def own_a(h):
        return pltpu.make_async_copy(a_ref.at[:, a_cols(h, row)], a_buf.at[0, :, a_half(h)], a_own_sem.at[h])

    def send_a(m, h):
        return pltpu.make_async_remote_copy(
            src_ref=a_ref.at[rows_of(m), a_cols(h, 1 - row)], dst_ref=a_buf.at[1, rows_of(m), a_half(h)],
            send_sem=a_send.at[m, h], recv_sem=a_recv.at[m, h], device_id=partner, device_id_type=MESH)

    def send_b(way, t):
        return pltpu.make_async_remote_copy(
            src_ref=b_got.at[0, t] if way == 2 else b_ref.at[:, cols_of(t)], dst_ref=b_got.at[way, t],
            send_sem=b_send.at[way, lax.rem(t, RING)], recv_sem=b_recv.at[way, lax.rem(t, RING)],
            device_id=neighbour if way == 0 else sibling, device_id_type=MESH)

    def load_b(t, slot):
        places = (core * 2 + col, core * 2 + 1 - col, (1 - core) * 2 + col, (1 - core) * 2 + 1 - col)
        return [
            pltpu.make_async_copy(
                b_ref.at[:, cols_of(t)] if i == 0 else b_got.at[i - 1, t],
                b_buf.at[slot, pl.ds(pl.multiple_of(place * depth, depth), depth), :], b_load_sem.at[slot, i])
            for i, place in enumerate(places)
        ]

    def send_first(m):
        return pltpu.make_async_remote_copy(
            src_ref=p_buf.at[0, rows_of(m)], dst_ref=r_got.at[0, rows_of(m)],
            send_sem=first_send.at[m], recv_sem=first_recv.at[m], device_id=partner, device_id_type=MESH)

    def send_block(s):
        return pltpu.make_async_remote_copy(
            src_ref=p_buf.at[lax.rem(s, SLOTS)], dst_ref=r_got.at[s],
            send_sem=p_send.at[lax.rem(s, SLOTS)], recv_sem=r_recv.at[lax.rem(s, RING)], device_id=partner, device_id_type=MESH)

    slab, rest = pl.ds(0, SLAB[0]), pl.ds(SLAB[0], p_buf.shape[1] - SLAB[0])
    wide = SLAB[1] * block // 4
    side, corner = pl.ds(0, wide), pl.ds(wide, block - wide)

    def at(c, r):
        return jnp.logical_and(core == 1, jnp.logical_and(col == c, row == r))

    def send_rest():
        return [
            pltpu.make_async_remote_copy(
                src_ref=p_buf.at[ROUND % SLOTS, *part], dst_ref=r_got.at[ROUND, *part],
                send_sem=send, recv_sem=recv, device_id=partner, device_id_type=MESH)
            for part, send, recv in (
                ((rest, slice(None)), p_send.at[ROUND % SLOTS], r_recv.at[ROUND % RING]),
                ((slab, corner), hop_send.at[3], hop_recv.at[3]),
            )
        ]

    def hop(i):
        sources = (p_buf.at[ROUND % SLOTS, slab, side], relay.at[0], relay.at[1])
        targets = (relay.at[0], relay.at[1], r_got.at[ROUND, slab, side])
        return pltpu.make_async_remote_copy(
            src_ref=sources[i], dst_ref=targets[i], send_sem=hop_send.at[i], recv_sem=hop_recv.at[i],
            device_id=partner if i == 1 else neighbour, device_id_type=MESH)

    def load_r(q):
        return pltpu.make_async_copy(r_got.at[q], r_buf, r_load_sem)

    def store_c(q):
        return pltpu.make_async_copy(c_buf, c_ref.at[:, cols_of(q)], c_sem)

    parts = [
        (pl.ds(row_, rows_), pl.ds(column, columns))
        for row_, column, rows_, columns in rectangles(p_buf.shape[1], block)
    ]

    def store_q_done():
        return pltpu.make_async_copy(q_buf, q_done, q_sem.at[0])

    def store_q():
        return [
            pltpu.make_async_copy(q_buf.at[*part], out, q_sem.at[i])
            for i, (part, out) in enumerate(zip(parts, q_parts))
        ]

    def store_p():
        return [
            pltpu.make_async_copy(p_buf.at[last % SLOTS, *part], out, last_sem.at[i])
            for i, (part, out) in enumerate(zip(parts, p_parts))
        ]

    def product(whose, m, slot):
        return jnp.dot(a_buf[whose, rows_of(m), :], b_buf[slot], preferred_element_type=jnp.float32)

    def pass_on(t):
        @pl.when(t >= RING - AHEAD)
        def _():
            send_b(0, t + AHEAD - RING).wait_send()

        @pl.when(t >= RING)
        def _():
            send_b(1, t - RING).wait_send()
            send_b(2, t - RING).wait_send()

        send_b(0, t).wait_recv()
        send_b(2, t).start()
        send_b(1, t).start()

        @pl.when(t + AHEAD < n_blocks)
        def _():
            send_b(0, t + AHEAD).start()

    def start_load_first(t):
        send_b(1, t).wait_recv()
        send_b(2, t).wait_recv()
        for copy in load_b(t, 0):
            copy.start()

    barrier = pltpu.get_barrier_semaphore()
    is_hub = jnp.logical_and(col == HUB[0], core == HUB[1])
    pl.semaphore_signal(barrier, inc=1, device_id=partner, device_id_type=MESH)

    @pl.when(jnp.logical_not(is_hub))
    def _():
        hub = {"col": HUB[0], "depth": HUB[1]}
        pl.semaphore_signal(barrier, inc=1, device_id=hub, device_id_type=MESH)
        pl.semaphore_wait(barrier, 1)

    @pl.when(is_hub)
    def _():
        pl.semaphore_wait(barrier, 4)
        for other in (neighbour, sibling, {**neighbour, **sibling}):
            pl.semaphore_signal(here_sem, inc=1, device_id=other, device_id_type=MESH)

    def start_a(tiles):
        for m in tiles:
            for h in range(2):
                send_a(m, h).start()

    early, late = range(2), range(2, TILES)
    start_a(early)

    @pl.when(jnp.logical_not(is_hub))
    def _():
        pl.semaphore_wait(here_sem, 1)

    for t in range(AHEAD):
        send_b(0, t).start()

    @pl.when(core == 0)
    def _():
        start_a(late)

    for h in range(2):
        own_a(h).start()
    pass_on(0)
    pass_on(1)
    start_load_first(0)

    @pl.loop(2, AHEAD)
    def _(t):
        pass_on(t)

    for h in range(2):
        own_a(h).wait()
    for copy in load_b(0, 0):
        copy.wait()

    @pl.loop(0, n_blocks + SLOTS)
    def _(s):
        @pl.when(s < n_blocks)
        def _():
            @pl.when(s > 0)
            def _():
                for copy in load_b(s, 0):
                    copy.wait()

            @pl.when(s == SLOTS)
            def _():
                for m in range(TILES):
                    send_first(m).wait_send()

            slab_sent = jnp.logical_and(s == ROUND + SLOTS, at(0, 1))

            @pl.when(jnp.logical_and(s > SLOTS, jnp.logical_not(slab_sent)))
            def _():
                send_block(s - SLOTS).wait_send()

            @pl.when(slab_sent)
            def _():
                for copy in (*send_rest(), hop(0)):
                    copy.wait_send()

            @pl.loop(0, TILES)
            def _(m):
                @pl.when(s == 0)
                def _():
                    for h in range(2):
                        send_a(m, h).wait_recv()

                p_buf[lax.rem(s, SLOTS), rows_of(m), :] = product(1, m, 0)

                held = jnp.logical_and(core == 1, m < len(early))

                @pl.when(jnp.logical_and(s == 0, jnp.logical_not(held)))
                def _():
                    send_first(m).start()

                @pl.when(jnp.logical_and(jnp.logical_and(s == 0, core == 1), m == len(early) - 1))
                def _():
                    start_a(late)
                    for first in early:
                        send_first(first).start()

            @pl.when(s == last)
            def _():
                for copy in store_p():
                    copy.start()

            slab_goes = jnp.logical_and(s == ROUND, at(0, 1))

            @pl.when(jnp.logical_and(jnp.logical_and(s > 0, s < last), jnp.logical_not(slab_goes)))
            def _():
                send_block(s).start()

            @pl.when(slab_goes)
            def _():
                for copy in (*send_rest(), hop(0)):
                    copy.start()

            for i, place in ((1, (1, 1)), (2, (1, 0))):
                @pl.when(jnp.logical_and(s == ROUND + i, at(*place)))
                def _():
                    hop(i - 1).wait_recv()
                    hop(i).start()

            @pl.when(s + AHEAD < n_blocks)
            def _():
                pass_on(s + AHEAD)

            @pl.when(s + 1 < n_blocks)
            def _():
                start_load_first(s + 1)

        @pl.when(s >= SLOTS)
        def _():
            q = s - SLOTS

            @pl.when(q == 0)
            def _():
                for m in range(TILES):
                    send_first(m).wait_recv()

            slab_comes = jnp.logical_and(q == ROUND, at(0, 0))

            @pl.when(jnp.logical_and(jnp.logical_and(q > 0, q < last - 1), jnp.logical_not(slab_comes)))
            def _():
                send_block(q).wait_recv()

            @pl.when(slab_comes)
            def _():
                for copy in (*send_rest(), hop(2)):
                    copy.wait_recv()

            @pl.when(q < last - 1)
            def _():
                load_r(q).start()

            for copy in load_b(q, 1):
                copy.wait()

            @pl.when(q == last)
            def _():
                store_q_done().wait()

            @pl.loop(0, TILES)
            def _(m):
                q_buf[rows_of(m), :] = product(0, m, 1)

            @pl.when(q == last - 1)
            def _():
                store_q_done().start()

            @pl.when(q == last)
            def _():
                for copy in store_q():
                    copy.start()

            @pl.when(q + 1 < n_blocks)
            def _():
                for copy in load_b(q + 1, 1):
                    copy.start()

            @pl.when(q < last - 1)
            def _():
                load_r(q).wait()

                @pl.when(q > 0)
                def _():
                    store_c(q - 1).wait()

                @pl.loop(0, TILES)
                def _(m):
                    rows = rows_of(m)
                    c_buf[rows, :] = (q_buf[rows, :] + r_buf[rows, :]).astype(c_buf.dtype)

                store_c(q).start()

        @pl.when(s == SLOTS - 1)
        def _():
            for copy in load_b(0, 1):
                copy.start()

    @pl.loop(n_blocks - RING, n_blocks)
    def _(t):
        send_b(1, t).wait_send()
        send_b(2, t).wait_send()

        @pl.when(t >= n_blocks - RING + AHEAD)
        def _():
            send_b(0, t).wait_send()

    for i, place in ((1, (1, 1)), (2, (1, 0))):
        @pl.when(at(*place))
        def _():
            hop(i).wait_send()

    store_c(last - 2).wait()
    for copy in store_q() + store_p():
        copy.wait()
    for m in range(TILES):
        for h in range(2):
            send_a(m, h).wait_send()

    @pl.loop(n_blocks - SLOTS, last)
    def _(s):
        send_block(s).wait_send()

    send_block(last - 1).wait_recv()


def write_out(c_ref, q_ref, r_ref, out_ref, c_buf, q_buf, r_buf, o_buf, load_sem, store_sem):
    rows, done = c_buf.shape
    step = rows // PIECES

    def load(i):
        some = pl.ds(i * step, step)
        return pltpu.make_async_copy(c_ref.at[some, pl.ds(0, done)], c_buf.at[some], load_sem.at[i])

    def store(i):
        some = pl.ds(i * step, step)
        return pltpu.make_async_copy(c_buf.at[some], out_ref.at[some, pl.ds(0, done)], store_sem.at[i])

    load_q = pltpu.make_async_copy(q_ref, q_buf, load_sem.at[PIECES])
    load_r = pltpu.make_async_copy(r_ref.at[r_ref.shape[0] - 1], r_buf, load_sem.at[PIECES + 1])
    store_sum = pltpu.make_async_copy(o_buf, out_ref.at[:, pl.ds(done, o_buf.shape[1])], store_sem.at[PIECES])
    load_q.start()
    load_r.start()
    for i in range(PIECES):
        load(i).start()
    for i in range(PIECES):
        load(i).wait()
        store(i).start()
    load_q.wait()
    load_r.wait()
    o_buf[...] = (q_buf[...] + r_buf[...]).astype(o_buf.dtype)
    store_sum.start()
    for i in range(PIECES):
        store(i).wait()
    store_sum.wait()


def device_product(block, a_rows, b_rows):
    rows, _ = a_rows.shape
    depth, n_cols = b_rows.shape
    n_blocks, tile, n_parts = n_cols // block, rows // TILES, len(PARTS) + 1
    last = n_blocks - 1
    anywhere = pl.BlockSpec(memory_space=pl.ANY)
    dma = pltpu.SemaphoreType.DMA
    parts = [jax.ShapeDtypeStruct(place[2:], jnp.float32) for place in rectangles(rows, block)]
    c_main, r_got, q_done, _, _, *split = pl.pallas_call(
        functools.partial(kernel, n_blocks, tile),
        out_shape=(
            jax.ShapeDtypeStruct((rows, n_cols), jnp.bfloat16),
            jax.ShapeDtypeStruct((last, rows, block), jnp.float32),
            jax.ShapeDtypeStruct((rows, block), jnp.float32),
            jax.ShapeDtypeStruct((3, n_blocks, depth, block), jnp.bfloat16),
            jax.ShapeDtypeStruct((2, SLAB[0], SLAB[1] * block // 4), jnp.float32),
            *parts,
            *parts,
        ),
        in_specs=[anywhere] * 2,
        out_specs=(anywhere,) * (5 + 2 * n_parts),
        scratch_shapes=[
            pltpu.VMEM((2, rows, 4 * depth), jnp.bfloat16),
            pltpu.VMEM((2, 4 * depth, block), jnp.bfloat16),
            pltpu.VMEM((SLOTS, rows, block), jnp.float32),
            pltpu.VMEM((rows, block), jnp.float32),
            pltpu.VMEM((rows, block), jnp.float32),
            pltpu.VMEM((rows, block), jnp.bfloat16),
            dma((2,)),
            dma((TILES, 2)),
            dma((TILES, 2)),
            dma((3, RING)),
            dma((3, RING)),
            dma((2, 4)),
            dma((TILES,)),
            dma((TILES,)),
            dma((SLOTS,)),
            dma((RING,)),
            dma,
            dma,
            dma((n_parts,)),
            dma((n_parts,)),
            pltpu.SemaphoreType.REGULAR,
            dma((4,)),
            dma((4,)),
        ],
        compiler_params=pltpu.CompilerParams(
            collective_id=0, has_side_effects=True, vmem_limit_bytes=66_000_000
        ),
        name="split_sum_product",
    )(a_rows, b_rows)

    p_parts, q_parts = split[:n_parts], split[n_parts:]
    pair = ("row", "depth")
    got = []
    lent = lax.ppermute(q_parts[0], pair, [(1, 3)])
    got.append(lax.ppermute(p_parts[0], pair, [(0, 2), (1, 3), (2, 0)]))
    for i, part in enumerate(p_parts[1:], 1):
        got.append(lax.ppermute(part, pair, [(0, 2), (1, 3), (2, 0), (3, 1)]))
    back = lax.ppermute((lent + p_parts[0]).astype(jnp.bfloat16), pair, [(3, 1)])
    out = pl.pallas_call(
        write_out,
        out_shape=jax.ShapeDtypeStruct((rows, n_cols), jnp.bfloat16),
        in_specs=[anywhere] * 3,
        out_specs=anywhere,
        scratch_shapes=[
            pltpu.VMEM((rows, (last - 1) * block), jnp.bfloat16),
            pltpu.VMEM((rows, block), jnp.float32),
            pltpu.VMEM((rows, block), jnp.float32),
            pltpu.VMEM((rows, block), jnp.bfloat16),
            dma((PIECES + 2,)),
            dma((PIECES + 1,)),
        ],
        compiler_params=pltpu.CompilerParams(vmem_limit_bytes=50_000_000),
        cost_estimate=pl.CostEstimate(flops=20_000_000_000, bytes_accessed=4 * rows * n_cols, transcendentals=0),
        name="write_out",
    )(c_main, q_done, r_got)
    finished = [(own + part).astype(out.dtype) for own, part in zip(q_parts, got)]
    lender = jnp.logical_and(lax.axis_index("row") == 0, lax.axis_index("depth") == 1)
    finished[0] = jnp.where(lender, back, finished[0])
    places = rectangles(rows, block)
    for i in (2, 1, 3, 0, *range(4, n_parts)):
        out = lax.dynamic_update_slice(out, finished[i], (places[i][0], last * block + places[i][1]))
    return out


def solution(mesh, block=BLOCK):
    all_axes = ("depth", "row", "col")
    return jax.shard_map(
        functools.partial(device_product, block),
        mesh=mesh,
        in_specs=(P(all_axes, None), P(all_axes, None)),
        out_specs=P(all_axes, None),
        check_vma=False,
    )
```

```python
import functools

import jax
import jax.numpy as jnp
from jax import lax
from jax.experimental import pallas as pl
from jax.experimental.pallas import tpu as pltpu
from jax.sharding import PartitionSpec as P


MESH = pl.DeviceIdType.MESH
BLOCK = 512
TILES = 4
AHEAD = 4
SLOTS = 3
PARTS = (28, 3, 1)
HUB = (1, 0)
SLAB = (16, 3)
ROUND = 8
RING = 2 * (SLOTS + 1)


def kernel(
    n_blocks, tile, a_ref, b_ref, c_ref, r_got, b_got, relay, *others,
):
    p_parts, q_parts, scratch = others[: len(PARTS)], others[len(PARTS) : 2 * len(PARTS)], others[2 * len(PARTS) :]
    (
        a_buf, b_buf, p_buf, q_buf, r_buf, c_buf,
        a_own_sem, a_send, a_recv, b_send, b_recv, b_load_sem, first_send, first_recv, p_send, r_recv,
        r_load_sem, c_sem, q_sem, last_sem, here_sem, hop_send, hop_recv,
    ) = scratch
    last = n_blocks - 1
    col, row, core = lax.axis_index("col"), lax.axis_index("row"), lax.axis_index("depth")
    neighbour, partner, sibling = {"col": 1 - col}, {"row": 1 - row}, {"depth": 1 - core}
    depth, block = b_ref.shape[0], b_buf.shape[2]

    def rows_of(m):
        return pl.ds(pl.multiple_of(m * tile, tile), tile)

    def cols_of(t):
        return pl.ds(pl.multiple_of(t * block, block), block)

    def a_cols(h, r):
        return pl.ds(pl.multiple_of((h * 4 + r * 2) * depth, depth), 2 * depth)

    def a_half(h):
        return pl.ds(h * 2 * depth, 2 * depth)

    def own_a(h):
        return pltpu.make_async_copy(a_ref.at[:, a_cols(h, row)], a_buf.at[0, :, a_half(h)], a_own_sem.at[h])

    def send_a(m, h):
        return pltpu.make_async_remote_copy(
            src_ref=a_ref.at[rows_of(m), a_cols(h, 1 - row)], dst_ref=a_buf.at[1, rows_of(m), a_half(h)],
            send_sem=a_send.at[m, h], recv_sem=a_recv.at[m, h], device_id=partner, device_id_type=MESH)

    def send_b(way, t):
        return pltpu.make_async_remote_copy(
            src_ref=b_got.at[0, t] if way == 2 else b_ref.at[:, cols_of(t)], dst_ref=b_got.at[way, t],
            send_sem=b_send.at[way, lax.rem(t, RING)], recv_sem=b_recv.at[way, lax.rem(t, RING)],
            device_id=neighbour if way == 0 else sibling, device_id_type=MESH)

    def load_b(t, slot):
        places = (core * 2 + col, core * 2 + 1 - col, (1 - core) * 2 + col, (1 - core) * 2 + 1 - col)
        return [
            pltpu.make_async_copy(
                b_ref.at[:, cols_of(t)] if i == 0 else b_got.at[i - 1, t],
                b_buf.at[slot, pl.ds(pl.multiple_of(place * depth, depth), depth), :], b_load_sem.at[slot, i])
            for i, place in enumerate(places)
        ]

    def send_first(m):
        return pltpu.make_async_remote_copy(
            src_ref=p_buf.at[0, rows_of(m)], dst_ref=r_got.at[0, rows_of(m)],
            send_sem=first_send.at[m], recv_sem=first_recv.at[m], device_id=partner, device_id_type=MESH)

    def send_block(s):
        return pltpu.make_async_remote_copy(
            src_ref=p_buf.at[lax.rem(s, SLOTS)], dst_ref=r_got.at[s],
            send_sem=p_send.at[lax.rem(s, SLOTS)], recv_sem=r_recv.at[lax.rem(s, RING)], device_id=partner, device_id_type=MESH)

    slab, rest = pl.ds(0, SLAB[0]), pl.ds(SLAB[0], p_buf.shape[1] - SLAB[0])
    wide = SLAB[1] * block // 4
    side, corner = pl.ds(0, wide), pl.ds(wide, block - wide)

    def at(c, r):
        return jnp.logical_and(core == 1, jnp.logical_and(col == c, row == r))

    def send_rest():
        return [
            pltpu.make_async_remote_copy(
                src_ref=p_buf.at[ROUND % SLOTS, *part], dst_ref=r_got.at[ROUND, *part],
                send_sem=send, recv_sem=recv, device_id=partner, device_id_type=MESH)
            for part, send, recv in (
                ((rest, slice(None)), p_send.at[ROUND % SLOTS], r_recv.at[ROUND % RING]),
                ((slab, corner), hop_send.at[3], hop_recv.at[3]),
            )
        ]

    def hop(i):
        sources = (p_buf.at[ROUND % SLOTS, slab, side], relay.at[0], relay.at[1])
        targets = (relay.at[0], relay.at[1], r_got.at[ROUND, slab, side])
        return pltpu.make_async_remote_copy(
            src_ref=sources[i], dst_ref=targets[i], send_sem=hop_send.at[i], recv_sem=hop_recv.at[i],
            device_id=partner if i == 1 else neighbour, device_id_type=MESH)

    def load_r(q):
        return pltpu.make_async_copy(r_got.at[q], r_buf, r_load_sem)

    def store_c(q):
        return pltpu.make_async_copy(c_buf, c_ref.at[:, cols_of(q)], c_sem)

    unit = p_buf.shape[1] // sum(PARTS)
    parts = [pl.ds(sum(PARTS[:i]) * unit, n * unit) for i, n in enumerate(PARTS)]

    def store_q():
        return [
            pltpu.make_async_copy(q_buf.at[1, part], out, q_sem.at[i])
            for i, (part, out) in enumerate(zip(parts, q_parts))
        ]

    def store_p():
        return [
            pltpu.make_async_copy(p_buf.at[last % SLOTS, part], out, last_sem.at[i])
            for i, (part, out) in enumerate(zip(parts, p_parts))
        ]

    def product(whose, m, slot):
        return jnp.dot(a_buf[whose, rows_of(m), :], b_buf[slot], preferred_element_type=jnp.float32)

    def pass_on(t):
        @pl.when(t >= RING - AHEAD)
        def _():
            send_b(0, t + AHEAD - RING).wait_send()

        @pl.when(t >= RING)
        def _():
            send_b(1, t - RING).wait_send()
            send_b(2, t - RING).wait_send()

        send_b(0, t).wait_recv()
        send_b(2, t).start()
        send_b(1, t).start()

        @pl.when(t + AHEAD < n_blocks)
        def _():
            send_b(0, t + AHEAD).start()

    def start_load_first(t):
        send_b(1, t).wait_recv()
        send_b(2, t).wait_recv()
        for copy in load_b(t, 0):
            copy.start()

    def finish(q):
        load_r(q).wait()

        @pl.when(q > 0)
        def _():
            store_c(q - 1).wait()

        @pl.loop(0, TILES)
        def _(m):
            rows = rows_of(m)
            c_buf[rows, :] = (q_buf[0, rows, :] + r_buf[rows, :]).astype(c_buf.dtype)

        store_c(q).start()

    barrier = pltpu.get_barrier_semaphore()
    is_hub = jnp.logical_and(col == HUB[0], core == HUB[1])
    pl.semaphore_signal(barrier, inc=1, device_id=partner, device_id_type=MESH)

    @pl.when(jnp.logical_not(is_hub))
    def _():
        hub = {"col": HUB[0], "depth": HUB[1]}
        pl.semaphore_signal(barrier, inc=1, device_id=hub, device_id_type=MESH)
        pl.semaphore_wait(barrier, 1)

    @pl.when(is_hub)
    def _():
        pl.semaphore_wait(barrier, 4)
        for other in (neighbour, sibling, {**neighbour, **sibling}):
            pl.semaphore_signal(here_sem, inc=1, device_id=other, device_id_type=MESH)

    def start_a(tiles):
        for m in tiles:
            for h in range(2):
                send_a(m, h).start()

    early, late = range(2), range(2, TILES)
    start_a(early)

    @pl.when(jnp.logical_not(is_hub))
    def _():
        pl.semaphore_wait(here_sem, 1)

    for t in range(AHEAD):
        send_b(0, t).start()

    @pl.when(core == 0)
    def _():
        start_a(late)

    for h in range(2):
        own_a(h).start()
    pass_on(0)
    pass_on(1)
    start_load_first(0)

    @pl.loop(2, AHEAD)
    def _(t):
        pass_on(t)

    for h in range(2):
        own_a(h).wait()
    for copy in load_b(0, 0):
        copy.wait()

    @pl.loop(0, n_blocks + SLOTS)
    def _(s):
        @pl.when(s < n_blocks)
        def _():
            @pl.when(s > 0)
            def _():
                for copy in load_b(s, 0):
                    copy.wait()

            @pl.when(s == SLOTS)
            def _():
                for m in range(TILES):
                    send_first(m).wait_send()

            slab_sent = jnp.logical_and(s == ROUND + SLOTS, at(0, 1))

            @pl.when(jnp.logical_and(s > SLOTS, jnp.logical_not(slab_sent)))
            def _():
                send_block(s - SLOTS).wait_send()

            @pl.when(slab_sent)
            def _():
                for copy in (*send_rest(), hop(0)):
                    copy.wait_send()

            @pl.loop(0, TILES)
            def _(m):
                @pl.when(s == 0)
                def _():
                    for h in range(2):
                        send_a(m, h).wait_recv()

                p_buf[lax.rem(s, SLOTS), rows_of(m), :] = product(1, m, 0)

                held = jnp.logical_and(core == 1, m < len(early))

                @pl.when(jnp.logical_and(s == 0, jnp.logical_not(held)))
                def _():
                    send_first(m).start()

                @pl.when(jnp.logical_and(jnp.logical_and(s == 0, core == 1), m == len(early) - 1))
                def _():
                    start_a(late)
                    for first in early:
                        send_first(first).start()

            @pl.when(s == last)
            def _():
                for copy in store_p():
                    copy.start()

            slab_goes = jnp.logical_and(s == ROUND, at(0, 1))

            @pl.when(jnp.logical_and(jnp.logical_and(s > 0, s < last), jnp.logical_not(slab_goes)))
            def _():
                send_block(s).start()

            @pl.when(slab_goes)
            def _():
                for copy in (*send_rest(), hop(0)):
                    copy.start()

            for i, place in ((1, (1, 1)), (2, (1, 0))):
                @pl.when(jnp.logical_and(s == ROUND + i, at(*place)))
                def _():
                    hop(i - 1).wait_recv()
                    hop(i).start()

            @pl.when(s + AHEAD < n_blocks)
            def _():
                pass_on(s + AHEAD)

            @pl.when(s + 1 < n_blocks)
            def _():
                start_load_first(s + 1)

        @pl.when(s >= SLOTS)
        def _():
            q = s - SLOTS

            @pl.when(q == 0)
            def _():
                for m in range(TILES):
                    send_first(m).wait_recv()

            slab_comes = jnp.logical_and(q == ROUND, at(0, 0))

            @pl.when(jnp.logical_and(jnp.logical_and(q > 0, q < last - 1), jnp.logical_not(slab_comes)))
            def _():
                send_block(q).wait_recv()

            @pl.when(slab_comes)
            def _():
                for copy in (*send_rest(), hop(2)):
                    copy.wait_recv()

            @pl.when(q < last - 1)
            def _():
                load_r(q).start()

            for copy in load_b(q, 1):
                copy.wait()

            mine = jnp.where(q == last, 1, 0)

            @pl.loop(0, TILES)
            def _(m):
                q_buf[mine, rows_of(m), :] = product(0, m, 1)

            @pl.when(q == last)
            def _():
                for copy in store_q():
                    copy.start()

            @pl.when(q + 1 < n_blocks)
            def _():
                for copy in load_b(q + 1, 1):
                    copy.start()

            @pl.when(q < last - 1)
            def _():
                finish(q)

        @pl.when(s == SLOTS - 1)
        def _():
            for copy in load_b(0, 1):
                copy.start()

    @pl.loop(n_blocks - RING, n_blocks)
    def _(t):
        send_b(1, t).wait_send()
        send_b(2, t).wait_send()

        @pl.when(t >= n_blocks - RING + AHEAD)
        def _():
            send_b(0, t).wait_send()

    for i, place in ((1, (1, 1)), (2, (1, 0))):
        @pl.when(at(*place))
        def _():
            hop(i).wait_send()

    for copy in store_q() + store_p():
        copy.wait()
    for m in range(TILES):
        for h in range(2):
            send_a(m, h).wait_send()

    @pl.loop(n_blocks - SLOTS, last)
    def _(s):
        send_block(s).wait_send()

    send_block(last - 1).wait_recv()
    load_r(last - 1).start()
    finish(last - 1)
    store_c(last - 1).wait()


def write_out(c_ref, out_ref, c_buf, load_sem, store_sem):
    done = pl.ds(0, c_buf.shape[1])
    load = pltpu.make_async_copy(c_ref.at[:, done], c_buf, load_sem)
    store = pltpu.make_async_copy(c_buf, out_ref.at[:, done], store_sem)
    load.start()
    load.wait()
    store.start()
    store.wait()


def device_product(block, a_rows, b_rows):
    rows, _ = a_rows.shape
    depth, n_cols = b_rows.shape
    n_blocks, tile, unit = n_cols // block, rows // TILES, rows // sum(PARTS)
    last = n_blocks - 1
    anywhere = pl.BlockSpec(memory_space=pl.ANY)
    dma = pltpu.SemaphoreType.DMA
    parts = [jax.ShapeDtypeStruct((n * unit, block), jnp.float32) for n in PARTS]
    c_main, _, _, _, *split = pl.pallas_call(
        functools.partial(kernel, n_blocks, tile),
        out_shape=(
            jax.ShapeDtypeStruct((rows, n_cols), jnp.bfloat16),
            jax.ShapeDtypeStruct((last, rows, block), jnp.float32),
            jax.ShapeDtypeStruct((3, n_blocks, depth, block), jnp.bfloat16),
            jax.ShapeDtypeStruct((2, SLAB[0], SLAB[1] * block // 4), jnp.float32),
            *parts,
            *parts,
        ),
        in_specs=[anywhere] * 2,
        out_specs=(anywhere,) * (4 + 2 * len(PARTS)),
        scratch_shapes=[
            pltpu.VMEM((2, rows, 4 * depth), jnp.bfloat16),
            pltpu.VMEM((2, 4 * depth, block), jnp.bfloat16),
            pltpu.VMEM((SLOTS, rows, block), jnp.float32),
            pltpu.VMEM((2, rows, block), jnp.float32),
            pltpu.VMEM((rows, block), jnp.float32),
            pltpu.VMEM((rows, block), jnp.bfloat16),
            dma((2,)),
            dma((TILES, 2)),
            dma((TILES, 2)),
            dma((3, RING)),
            dma((3, RING)),
            dma((2, 4)),
            dma((TILES,)),
            dma((TILES,)),
            dma((SLOTS,)),
            dma((RING,)),
            dma,
            dma,
            dma((len(PARTS),)),
            dma((len(PARTS),)),
            pltpu.SemaphoreType.REGULAR,
            dma((4,)),
            dma((4,)),
        ],
        compiler_params=pltpu.CompilerParams(
            collective_id=0, has_side_effects=True, vmem_limit_bytes=66_000_000
        ),
        name="split_sum_product",
    )(a_rows, b_rows)

    p_parts, q_parts = split[: len(PARTS)], split[len(PARTS) :]
    got = []
    for part in p_parts:
        got.append(lax.ppermute(part, "row", [(0, 1), (1, 0)]))
    out = pl.pallas_call(
        write_out,
        out_shape=jax.ShapeDtypeStruct((rows, n_cols), jnp.bfloat16),
        in_specs=[anywhere],
        out_specs=anywhere,
        scratch_shapes=[pltpu.VMEM((rows, last * block), jnp.bfloat16), dma, dma],
        compiler_params=pltpu.CompilerParams(vmem_limit_bytes=50_000_000),
        cost_estimate=pl.CostEstimate(flops=20_000_000_000, bytes_accessed=4 * rows * n_cols, transcendentals=0),
        name="write_out",
    )(c_main)
    for i, (own, part) in enumerate(zip(q_parts, got)):
        start = sum(PARTS[:i]) * unit
        out = lax.dynamic_update_slice(out, (own + part).astype(out.dtype), (start, last * block))
    return out


def solution(mesh, block=BLOCK):
    all_axes = ("depth", "row", "col")
    return jax.shard_map(
        functools.partial(device_product, block),
        mesh=mesh,
        in_specs=(P(all_axes, None), P(all_axes, None)),
        out_specs=P(all_axes, None),
        check_vma=False,
    )
```

```python
import functools

import jax
import jax.numpy as jnp
from jax import lax
from jax.experimental import pallas as pl
from jax.experimental.pallas import tpu as pltpu
from jax.sharding import PartitionSpec as P


MESH = pl.DeviceIdType.MESH
BLOCK = 512
TILES = 4
AHEAD = 4
SLOTS = 3
PARTS = (27, 4, 1)
HUB = (1, 0)
SLAB = (56, 1)
ROUND = 8
RING = 2 * (SLOTS + 1)


def kernel(
    n_blocks, tile, a_ref, b_ref, c_ref, r_got, b_got, relay, *others,
):
    p_parts, q_parts, scratch = others[: len(PARTS)], others[len(PARTS) : 2 * len(PARTS)], others[2 * len(PARTS) :]
    (
        a_buf, b_buf, p_buf, q_buf, r_buf, c_buf,
        a_own_sem, a_send, a_recv, b_send, b_recv, b_load_sem, first_send, first_recv, p_send, r_recv,
        r_load_sem, c_sem, q_sem, last_sem, here_sem, hop_send, hop_recv,
    ) = scratch
    last = n_blocks - 1
    col, row, core = lax.axis_index("col"), lax.axis_index("row"), lax.axis_index("depth")
    neighbour, partner, sibling = {"col": 1 - col}, {"row": 1 - row}, {"depth": 1 - core}
    depth, block = b_ref.shape[0], b_buf.shape[2]

    def rows_of(m):
        return pl.ds(pl.multiple_of(m * tile, tile), tile)

    def cols_of(t):
        return pl.ds(pl.multiple_of(t * block, block), block)

    def a_cols(h, r):
        return pl.ds(pl.multiple_of((h * 4 + r * 2) * depth, depth), 2 * depth)

    def a_half(h):
        return pl.ds(h * 2 * depth, 2 * depth)

    def own_a(h):
        return pltpu.make_async_copy(a_ref.at[:, a_cols(h, row)], a_buf.at[0, :, a_half(h)], a_own_sem.at[h])

    def send_a(m, h):
        return pltpu.make_async_remote_copy(
            src_ref=a_ref.at[rows_of(m), a_cols(h, 1 - row)], dst_ref=a_buf.at[1, rows_of(m), a_half(h)],
            send_sem=a_send.at[m, h], recv_sem=a_recv.at[m, h], device_id=partner, device_id_type=MESH)

    def send_b(way, t):
        return pltpu.make_async_remote_copy(
            src_ref=b_got.at[0, t] if way == 2 else b_ref.at[:, cols_of(t)], dst_ref=b_got.at[way, t],
            send_sem=b_send.at[way, lax.rem(t, RING)], recv_sem=b_recv.at[way, lax.rem(t, RING)],
            device_id=neighbour if way == 0 else sibling, device_id_type=MESH)

    def load_b(t, slot):
        places = (core * 2 + col, core * 2 + 1 - col, (1 - core) * 2 + col, (1 - core) * 2 + 1 - col)
        return [
            pltpu.make_async_copy(
                b_ref.at[:, cols_of(t)] if i == 0 else b_got.at[i - 1, t],
                b_buf.at[slot, pl.ds(pl.multiple_of(place * depth, depth), depth), :], b_load_sem.at[slot, i])
            for i, place in enumerate(places)
        ]

    def send_first(m):
        return pltpu.make_async_remote_copy(
            src_ref=p_buf.at[0, rows_of(m)], dst_ref=r_got.at[0, rows_of(m)],
            send_sem=first_send.at[m], recv_sem=first_recv.at[m], device_id=partner, device_id_type=MESH)

    def send_block(s):
        return pltpu.make_async_remote_copy(
            src_ref=p_buf.at[lax.rem(s, SLOTS)], dst_ref=r_got.at[s],
            send_sem=p_send.at[lax.rem(s, SLOTS)], recv_sem=r_recv.at[lax.rem(s, RING)], device_id=partner, device_id_type=MESH)

    slab, rest = pl.ds(0, SLAB[0]), pl.ds(SLAB[0], p_buf.shape[1] - SLAB[0])
    wide = SLAB[1] * block // 4
    side, corner = pl.ds(0, wide), pl.ds(wide, block - wide)

    def at(c, r):
        return jnp.logical_and(core == 1, jnp.logical_and(col == c, row == r))

    def send_rest():
        return [
            pltpu.make_async_remote_copy(
                src_ref=p_buf.at[ROUND % SLOTS, *part], dst_ref=r_got.at[ROUND, *part],
                send_sem=send, recv_sem=recv, device_id=partner, device_id_type=MESH)
            for part, send, recv in (
                ((rest, slice(None)), p_send.at[ROUND % SLOTS], r_recv.at[ROUND % RING]),
                ((slab, corner), hop_send.at[3], hop_recv.at[3]),
            )
        ]

    def hop(i):
        sources = (p_buf.at[ROUND % SLOTS, slab, side], relay.at[0], relay.at[1])
        targets = (relay.at[0], relay.at[1], r_got.at[ROUND, slab, side])
        return pltpu.make_async_remote_copy(
            src_ref=sources[i], dst_ref=targets[i], send_sem=hop_send.at[i], recv_sem=hop_recv.at[i],
            device_id=partner if i == 1 else neighbour, device_id_type=MESH)

    def load_r(q):
        return pltpu.make_async_copy(r_got.at[q], r_buf, r_load_sem)

    def store_c(q):
        return pltpu.make_async_copy(c_buf, c_ref.at[:, cols_of(q)], c_sem)

    unit = p_buf.shape[1] // sum(PARTS)
    parts = [pl.ds(sum(PARTS[:i]) * unit, n * unit) for i, n in enumerate(PARTS)]

    def store_q():
        return [
            pltpu.make_async_copy(q_buf.at[1, part], out, q_sem.at[i])
            for i, (part, out) in enumerate(zip(parts, q_parts))
        ]

    def store_p():
        return [
            pltpu.make_async_copy(p_buf.at[last % SLOTS, part], out, last_sem.at[i])
            for i, (part, out) in enumerate(zip(parts, p_parts))
        ]

    def product(whose, m, slot):
        return jnp.dot(a_buf[whose, rows_of(m), :], b_buf[slot], preferred_element_type=jnp.float32)

    def pass_on(t):
        @pl.when(t >= RING - AHEAD)
        def _():
            send_b(0, t + AHEAD - RING).wait_send()

        @pl.when(t >= RING)
        def _():
            send_b(1, t - RING).wait_send()
            send_b(2, t - RING).wait_send()

        send_b(0, t).wait_recv()
        send_b(2, t).start()
        send_b(1, t).start()

        @pl.when(t + AHEAD < n_blocks)
        def _():
            send_b(0, t + AHEAD).start()

    def start_load_first(t):
        send_b(1, t).wait_recv()
        send_b(2, t).wait_recv()
        for copy in load_b(t, 0):
            copy.start()

    def finish(q):
        load_r(q).wait()

        @pl.when(q > 0)
        def _():
            store_c(q - 1).wait()

        @pl.loop(0, TILES)
        def _(m):
            rows = rows_of(m)
            c_buf[rows, :] = (q_buf[0, rows, :] + r_buf[rows, :]).astype(c_buf.dtype)

        store_c(q).start()

    def start_a(tiles):
        for m in tiles:
            for h in range(2):
                send_a(m, h).start()

    early, late = range(2), range(2, TILES)
    barrier = pltpu.get_barrier_semaphore()
    pl.semaphore_signal(barrier, inc=1, device_id=partner, device_id_type=MESH)
    is_hub = jnp.logical_and(col == HUB[0], core == HUB[1])

    @pl.when(is_hub)
    def _():
        pl.semaphore_wait(barrier, 4)

    @pl.when(jnp.logical_not(is_hub))
    def _():
        pl.semaphore_wait(barrier, 1)

    start_a(early)

    @pl.when(is_hub)
    def _():
        for other in (neighbour, sibling, {**neighbour, **sibling}):
            pl.semaphore_signal(here_sem, inc=1, device_id=other, device_id_type=MESH)

    @pl.when(jnp.logical_not(is_hub))
    def _():
        hub = {"col": HUB[0], "depth": HUB[1]}
        pl.semaphore_signal(barrier, inc=1, device_id=hub, device_id_type=MESH)
        pl.semaphore_wait(here_sem, 1)

    for t in range(AHEAD):
        send_b(0, t).start()

    @pl.when(core == 0)
    def _():
        start_a(late)

    for h in range(2):
        own_a(h).start()
    pass_on(0)
    pass_on(1)
    start_load_first(0)

    @pl.loop(2, AHEAD)
    def _(t):
        pass_on(t)

    for h in range(2):
        own_a(h).wait()
    for copy in load_b(0, 0):
        copy.wait()

    @pl.loop(0, n_blocks + SLOTS)
    def _(s):
        @pl.when(s < n_blocks)
        def _():
            @pl.when(s > 0)
            def _():
                for copy in load_b(s, 0):
                    copy.wait()

            @pl.when(s == SLOTS)
            def _():
                for m in range(TILES):
                    send_first(m).wait_send()

            slab_sent = jnp.logical_and(s == ROUND + SLOTS, at(0, 1))

            @pl.when(jnp.logical_and(s > SLOTS, jnp.logical_not(slab_sent)))
            def _():
                send_block(s - SLOTS).wait_send()

            @pl.when(slab_sent)
            def _():
                for copy in (*send_rest(), hop(0)):
                    copy.wait_send()

            @pl.loop(0, TILES)
            def _(m):
                @pl.when(s == 0)
                def _():
                    for h in range(2):
                        send_a(m, h).wait_recv()

                p_buf[lax.rem(s, SLOTS), rows_of(m), :] = product(1, m, 0)

                held = jnp.logical_and(core == 1, m < len(early))

                @pl.when(jnp.logical_and(s == 0, jnp.logical_not(held)))
                def _():
                    send_first(m).start()

                @pl.when(jnp.logical_and(jnp.logical_and(s == 0, core == 1), m == len(early) - 1))
                def _():
                    start_a(late)
                    for first in early:
                        send_first(first).start()

            @pl.when(s == last)
            def _():
                for copy in store_p():
                    copy.start()

            slab_goes = jnp.logical_and(s == ROUND, at(0, 1))

            @pl.when(jnp.logical_and(jnp.logical_and(s > 0, s < last), jnp.logical_not(slab_goes)))
            def _():
                send_block(s).start()

            @pl.when(slab_goes)
            def _():
                for copy in (*send_rest(), hop(0)):
                    copy.start()

            for i, place in ((1, (1, 1)), (2, (1, 0))):
                @pl.when(jnp.logical_and(s == ROUND + i, at(*place)))
                def _():
                    hop(i - 1).wait_recv()
                    hop(i).start()

            @pl.when(s + AHEAD < n_blocks)
            def _():
                pass_on(s + AHEAD)

            @pl.when(s + 1 < n_blocks)
            def _():
                start_load_first(s + 1)

        @pl.when(s >= SLOTS)
        def _():
            q = s - SLOTS

            @pl.when(q == 0)
            def _():
                for m in range(TILES):
                    send_first(m).wait_recv()

            slab_comes = jnp.logical_and(q == ROUND, at(0, 0))

            @pl.when(jnp.logical_and(jnp.logical_and(q > 0, q < last - 1), jnp.logical_not(slab_comes)))
            def _():
                send_block(q).wait_recv()

            @pl.when(slab_comes)
            def _():
                for copy in (*send_rest(), hop(2)):
                    copy.wait_recv()

            @pl.when(q < last - 1)
            def _():
                load_r(q).start()

            for copy in load_b(q, 1):
                copy.wait()

            mine = jnp.where(q == last, 1, 0)

            @pl.loop(0, TILES)
            def _(m):
                q_buf[mine, rows_of(m), :] = product(0, m, 1)

            @pl.when(q == last)
            def _():
                for copy in store_q():
                    copy.start()

            @pl.when(q + 1 < n_blocks)
            def _():
                for copy in load_b(q + 1, 1):
                    copy.start()

            @pl.when(q < last - 1)
            def _():
                finish(q)

        @pl.when(s == SLOTS - 1)
        def _():
            for copy in load_b(0, 1):
                copy.start()

    @pl.loop(n_blocks - RING, n_blocks)
    def _(t):
        send_b(1, t).wait_send()
        send_b(2, t).wait_send()

        @pl.when(t >= n_blocks - RING + AHEAD)
        def _():
            send_b(0, t).wait_send()

    for i, place in ((1, (1, 1)), (2, (1, 0))):
        @pl.when(at(*place))
        def _():
            hop(i).wait_send()

    for copy in store_q() + store_p():
        copy.wait()
    for m in range(TILES):
        for h in range(2):
            send_a(m, h).wait_send()

    @pl.loop(n_blocks - SLOTS, last)
    def _(s):
        send_block(s).wait_send()

    send_block(last - 1).wait_recv()
    load_r(last - 1).start()
    finish(last - 1)
    store_c(last - 1).wait()


def write_out(c_ref, out_ref, c_buf, load_sem, store_sem):
    done = pl.ds(0, c_buf.shape[1])
    load = pltpu.make_async_copy(c_ref.at[:, done], c_buf, load_sem)
    store = pltpu.make_async_copy(c_buf, out_ref.at[:, done], store_sem)
    load.start()
    load.wait()
    store.start()
    store.wait()


def device_product(block, a_rows, b_rows):
    rows, _ = a_rows.shape
    depth, n_cols = b_rows.shape
    n_blocks, tile, unit = n_cols // block, rows // TILES, rows // sum(PARTS)
    last = n_blocks - 1
    anywhere = pl.BlockSpec(memory_space=pl.ANY)
    dma = pltpu.SemaphoreType.DMA
    parts = [jax.ShapeDtypeStruct((n * unit, block), jnp.float32) for n in PARTS]
    c_main, _, _, _, *split = pl.pallas_call(
        functools.partial(kernel, n_blocks, tile),
        out_shape=(
            jax.ShapeDtypeStruct((rows, n_cols), jnp.bfloat16),
            jax.ShapeDtypeStruct((last, rows, block), jnp.float32),
            jax.ShapeDtypeStruct((3, n_blocks, depth, block), jnp.bfloat16),
            jax.ShapeDtypeStruct((2, SLAB[0], SLAB[1] * block // 4), jnp.float32),
            *parts,
            *parts,
        ),
        in_specs=[anywhere] * 2,
        out_specs=(anywhere,) * (4 + 2 * len(PARTS)),
        scratch_shapes=[
            pltpu.VMEM((2, rows, 4 * depth), jnp.bfloat16),
            pltpu.VMEM((2, 4 * depth, block), jnp.bfloat16),
            pltpu.VMEM((SLOTS, rows, block), jnp.float32),
            pltpu.VMEM((2, rows, block), jnp.float32),
            pltpu.VMEM((rows, block), jnp.float32),
            pltpu.VMEM((rows, block), jnp.bfloat16),
            dma((2,)),
            dma((TILES, 2)),
            dma((TILES, 2)),
            dma((3, RING)),
            dma((3, RING)),
            dma((2, 4)),
            dma((TILES,)),
            dma((TILES,)),
            dma((SLOTS,)),
            dma((RING,)),
            dma,
            dma,
            dma((len(PARTS),)),
            dma((len(PARTS),)),
            pltpu.SemaphoreType.REGULAR,
            dma((4,)),
            dma((4,)),
        ],
        compiler_params=pltpu.CompilerParams(
            collective_id=0, has_side_effects=True, vmem_limit_bytes=66_000_000
        ),
        name="split_sum_product",
    )(a_rows, b_rows)

    p_parts, q_parts = split[: len(PARTS)], split[len(PARTS) :]
    got = []
    for part in p_parts:
        got.append(lax.ppermute(part, "row", [(0, 1), (1, 0)]))
    out = pl.pallas_call(
        write_out,
        out_shape=jax.ShapeDtypeStruct((rows, n_cols), jnp.bfloat16),
        in_specs=[anywhere],
        out_specs=anywhere,
        scratch_shapes=[pltpu.VMEM((rows, last * block), jnp.bfloat16), dma, dma],
        compiler_params=pltpu.CompilerParams(vmem_limit_bytes=50_000_000),
        cost_estimate=pl.CostEstimate(flops=20_000_000_000, bytes_accessed=4 * rows * n_cols, transcendentals=0),
        name="write_out",
    )(c_main)
    for i, (own, part) in enumerate(zip(q_parts, got)):
        start = sum(PARTS[:i]) * unit
        out = lax.dynamic_update_slice(out, (own + part).astype(out.dtype), (start, last * block))
    return out


def solution(mesh, block=BLOCK):
    all_axes = ("depth", "row", "col")
    return jax.shard_map(
        functools.partial(device_product, block),
        mesh=mesh,
        in_specs=(P(all_axes, None), P(all_axes, None)),
        out_specs=P(all_axes, None),
        check_vma=False,
    )
```
